128 devices in a mesh: row: 8 (over y, z_hi), col: 16 (over z_lo, x, core).
Axes of the slice: x: 4, y: 4, z: 4 (z_hi: 2, z_lo: 2; z = z_hi * 2 + z_lo), core: 2. Of those that a mesh axis runs over, the one named last changes fastest.
Arguments:
- pair: float32 [512, 512, 128], P('row', 'col'), may hold values from -6 to 6
- valid_length: int32 [1], replicated, may hold values from 128 to 511
- tri_in: bfloat16 [128, 512], replicated, may hold values from -0.5 to 0.5
- tri_gate: bfloat16 [128, 128], replicated, may hold values from -0.5 to 0.5
- tri_out: bfloat16 [128, 128], replicated, may hold values from -0.5 to 0.5
- att_in: bfloat16 [128, 512], replicated, may hold values from -16.9705627 to 16.9705627
- att_bias: bfloat16 [128, 4], replicated, may hold values from -0.5 to 0.5
- att_out: bfloat16 [128, 128], replicated, may hold values from -0.5 to 0.5
Outputs:
- pair_out: float32 [512, 512, 128], P('row', 'col')
The draws below stay inside these ranges and needn't reach their ends.
Inputs may be any that keep to these rules, and one draw needn't show every extreme that they name: Tokens at positions below valid_length[0] are real, the rest are padding.
All inputs are finite; a program needn't handle non-finite values.
Results may differ from the reference program's by a relative error of at most 0.025.
Values may be sent and summed in bfloat16 or wider, within the bound.
A program may use at most 128 MiB of HBM per device.

```python
import jax
import jax.numpy as jnp
from jax import lax

C = 128
CH = 128
H = 4
DH = 32
N = 512


def draw_att_in(key, part):
    raw = jax.random.truncated_normal(key, -4.0, 4.0, (C, 4 * C), jnp.float32) * C ** (-0.5)
    return raw.astype(jnp.bfloat16)


def shard_levels(stream_key, dims, shards, least, largest):
    factor_of, own = 1.0, jax.random.fold_in(stream_key, 6)
    for dim, shards_of in shards:
        heights = jnp.exp(jax.random.uniform(jax.random.fold_in(own, dim), (shards_of,), jnp.float32, least / len(shards), largest / len(shards)))
        factor_of = factor_of * jnp.repeat(heights, dims[dim] // shards_of).reshape([-1 if axis == dim else 1 for axis in range(len(dims))])
    return factor_of


def noise(key, extent, width, most, shards=(), held_as=jnp.bfloat16):
    array = width * jax.random.normal(key, extent, jnp.float32)
    if shards:
        array = array * shard_levels(key, extent, shards, -0.22, 0.18)
    return jnp.clip(array, -most, most).astype(held_as)


def setup_inputs(seed: int = 0) -> dict:
    splits = jax.random.split(jax.random.key(seed), 9)
    return {
        "pair": noise(splits[0], (N, N, C), 1.0, 6.0, ((0, 8), (1, 16)), jnp.float32),
        "valid_length": jax.random.randint(splits[1], (1,), N // 4, N).astype(jnp.int32),
        "tri_in": noise(splits[2], (C, 4 * CH), C ** -0.5, 0.5),
        "tri_gate": noise(splits[3], (C, C), C ** -0.5, 0.5),
        "tri_out": noise(splits[4], (CH, C), CH ** -0.5, 0.5),
        "att_in": draw_att_in(jax.random.fold_in(splits[8], 71), 0),
        "att_bias": noise(splits[6], (C, H), C ** -0.5, 0.5),
        "att_out": noise(splits[7], (C, C), C ** -0.5, 0.5),
    }


def layer_norm(values):
    center = values - lax.optimization_barrier(jnp.mean(values, axis=-1, keepdims=True))
    return center * lax.rsqrt(lax.optimization_barrier(jnp.mean(center * center, axis=-1, keepdims=True)) + 1e-05)

def reference(pair, valid_length, tri_in, tri_gate, tri_out, att_in, att_bias, att_out):
    tokens = jnp.arange(N).astype(jnp.int32)
    keep = (tokens < valid_length[0]).astype(jnp.float32)
    blocks = N // 8
    normed_pair = layer_norm(pair).astype(jnp.bfloat16)

    def edges(packed):
        rows, row_keep = packed
        projected = jnp.dot(rows, tri_in, preferred_element_type=jnp.float32)
        weight = (row_keep[:, None] * keep[None, :])[:, :, None]
        left = jax.nn.sigmoid(projected[..., :CH]) * projected[..., CH:2 * CH] * weight
        right = jax.nn.sigmoid(projected[..., 2 * CH:3 * CH]) * projected[..., 3 * CH:] * weight
        return (left.astype(jnp.bfloat16), right.astype(jnp.bfloat16))
    left_edges, right_edges = lax.map(edges, (normed_pair.reshape(blocks, 8, N, C), keep.reshape(blocks, 8)))
    left_edges = left_edges.reshape(N, N, CH)
    right_edges = right_edges.reshape(N, N, CH)
    products = jnp.einsum('ikc,jkc->ijc', left_edges.astype(jnp.float32), right_edges.astype(jnp.float32))
    normed_products = layer_norm(products).astype(jnp.bfloat16)
    update = jax.nn.sigmoid(jnp.dot(normed_pair, tri_gate, preferred_element_type=jnp.float32)) * jnp.dot(normed_products, tri_out, preferred_element_type=jnp.float32)
    middle = pair + update
    normed_mid = layer_norm(middle).astype(jnp.bfloat16)
    bias_all = jnp.dot(normed_mid, att_bias, preferred_element_type=jnp.float32).astype(jnp.bfloat16)
    bias_heads = jnp.transpose(bias_all.astype(jnp.float32), (2, 0, 1))
    mask_bias = jnp.where(tokens < valid_length[0], 0.0, -1000000000.0).astype(jnp.float32)

    def attend(packed):
        block_mid, block_norm = packed
        projected = jnp.dot(block_norm, att_in, preferred_element_type=jnp.float32)
        query = (projected[..., :C] * DH ** (-0.5)).astype(jnp.bfloat16).reshape(8, N, H, DH)
        keys = projected[..., C:2 * C].astype(jnp.bfloat16).reshape(8, N, H, DH)
        values = projected[..., 2 * C:3 * C].astype(jnp.bfloat16).reshape(8, N, H, DH)
        gate = jax.nn.sigmoid(projected[..., 3 * C:])
        scores = jnp.einsum('ijhd,ikhd->ihjk', query.astype(jnp.float32), keys.astype(jnp.float32))
        scores = scores + bias_heads[None] + mask_bias[None, None, None, :]
        weights = jax.nn.softmax(scores, axis=-1)
        attended = jnp.einsum('ihjk,ikhd->ijhd', weights, values.astype(jnp.float32)).reshape(8, N, C)
        gated = (gate * attended).astype(jnp.bfloat16)
        return block_mid + jnp.dot(gated, att_out, preferred_element_type=jnp.float32)
    result = lax.map(attend, (middle.reshape(blocks, 8, N, C), normed_mid.reshape(blocks, 8, N, C)))
    return result.reshape(N, N, C)
```

```python
import functools

import jax
import jax.numpy as jnp
from jax import lax
from jax.experimental import pallas as pl
from jax.experimental.pallas import tpu as pltpu
from jax.sharding import PartitionSpec as P

MESH = pl.DeviceIdType.MESH
F32 = jnp.float32
BF16 = jnp.bfloat16
NT = (((1,), (1,)), ((), ()))
TN = (((0,), (0,)), ((), ()))
NN = (((1,), (0,)), ((), ()))


def dot(a, b, dims=NN):
    return lax.dot_general(a, b, dims, preferred_element_type=F32)


def norm_last(x):
    c = x - jnp.mean(x, axis=-1, keepdims=True)
    return c * lax.rsqrt(jnp.mean(c * c, axis=-1, keepdims=True) + 1e-5)


def turned(w):
    return w.astype(F32).T.astype(BF16)


def swap16():
    p = lax.broadcasted_iota(jnp.int32, (256, 256), 0)
    q = lax.broadcasted_iota(jnp.int32, (256, 256), 1)
    return (q == (p % 16) * 16 + p // 16).astype(F32).astype(BF16)


def block_turn(tiles):
    return [
        jnp.concatenate([t[:, 32 * b : 32 * b + 32] for t in tiles], axis=1) for b in range(4)
    ]


def tile_of(x_ref, s):
    return jnp.concatenate([x_ref[16 * b + s] for b in range(4)], axis=0)


def edges_body(x_ref, len_ref, tri_in_ref, e_ref, n_ref, wt, y):
    wt[...] = turned(tri_in_ref[...])
    row = lax.axis_index("row") * 64
    col = lax.axis_index("col") * 32
    lane = lax.broadcasted_iota(jnp.int32, (1, 128), 1)
    length = len_ref[0]
    keep_k = (col + lane % 32) < length

    def one(s, _):
        nb = norm_last(tile_of(x_ref, s)).astype(BF16)
        n_ref[s] = nb
        pt = dot(wt[...], nb, NT)
        w = jnp.where(keep_k & ((row + (lane // 32) * 16 + s) < length), 1.0, 0.0)
        for side in range(2):
            g = pt[256 * side : 256 * side + 128]
            v = pt[256 * side + 128 : 256 * side + 256]
            edge = (jax.nn.sigmoid(g) * v * w).astype(BF16)
            y[:, pl.ds(pl.multiple_of(16 * s, 16), 16), 128 * side : 128 * side + 128] = (
                edge.reshape(8, 16, 128)
            )
        return 0

    lax.fori_loop(0, 16, one, 0)
    perm = swap16()

    def group(g, _):
        z = dot(perm, y[g]).astype(BF16)
        at = pl.ds(pl.multiple_of(16 * g, 16), 16)
        e_ref[at, 0] = z[:, :128].reshape(16, 16, 128)
        e_ref[at, 1] = z[:, 128:].reshape(16, 16, 128)
        return 0

    lax.fori_loop(0, 8, group, 0)


def triangle_body(rx_ref, o_ref, lm, rm):
    def gather(r, _):
        for side, m in ((0, lm), (1, rm)):
            for cg in range(4):
                tiles = [rx_ref[16 * r + 4 * cg + c, side] for c in range(4)]
                for b, t in enumerate(block_turn(tiles)):
                    at = pl.ds(pl.multiple_of(64 * r + 16 * b, 16), 16)
                    m[at, 128 * cg : 128 * cg + 128] = t
        return 0

    lax.fori_loop(0, 8, gather, 0)

    def rows(r, _):
        p = dot(lm[pl.ds(pl.multiple_of(64 * r, 64), 64), :], rm[...], NT).astype(BF16)
        for cg in range(4):
            tiles = [p[16 * b : 16 * b + 16, 128 * cg : 128 * cg + 128] for b in range(4)]
            for c, t in enumerate(block_turn(tiles)):
                o_ref[16 * r + 4 * cg + c] = t
        return 0

    lax.fori_loop(0, 8, rows, 0)


def middle_body(x_ref, n_ref, px_ref, gate_ref, out_ref, bias_ref, mid_ref, nm_ref, bm_ref, np_, yb):
    total = lax.fori_loop(
        0, 128, lambda c, a: a + px_ref[c].astype(F32), jnp.zeros((16, 128), F32), unroll=8
    )
    mean = total * (1.0 / 128)

    def square(c, a):
        d = px_ref[c].astype(F32) - mean
        return a + d * d

    var = lax.fori_loop(0, 128, square, jnp.zeros((16, 128), F32), unroll=8) * (1.0 / 128)
    scale = lax.rsqrt(var + 1e-5)
    perm = swap16()

    def group(g, _):
        at = pl.ds(pl.multiple_of(16 * g, 16), 16)
        z = ((px_ref[at].astype(F32) - mean[None]) * scale[None]).astype(BF16)
        z = dot(perm, z.reshape(256, 128)).astype(BF16)
        np_[:, at, :] = z.reshape(16, 16, 128)
        return 0

    lax.fori_loop(0, 8, group, 0)
    wb = bias_ref[...]

    def one(s, _):
        tri = dot(np_[s], out_ref[...], TN)
        gate = jax.nn.sigmoid(dot(n_ref[s], gate_ref[...]))
        mid = tile_of(x_ref, s) + gate * tri
        mid_ref[s] = mid
        nm = norm_last(mid).astype(BF16)
        nm_ref[s] = nm
        yb[pl.ds(s, 8, stride=16), :] = dot(wb, nm, NT)
        return 0

    lax.fori_loop(0, 16, one, 0)
    yt = yb[...].T
    bm_ref[...] = jnp.concatenate([yt[32 * b : 32 * b + 32, :64] for b in range(4)], axis=1).astype(
        BF16
    )


def attend_body(nx_ref, bx_ref, len_ref, att_in_ref, go_ref, qs, ks, vt, gt, bias, tile):
    wvt = turned(att_in_ref[:, 256:384])
    wgt = turned(att_in_ref[:, 384:512])
    lane128 = lax.broadcasted_iota(jnp.int32, (1, 128), 1)
    kk = lax.broadcasted_iota(jnp.int32, (512, 256), 0)
    mask = jnp.where(kk < len_ref[0], 0.0, -1e9).astype(F32).reshape(8, 2, 32, 256)

    def project(c, _):
        nx = nx_ref[c]
        qk = dot(nx, att_in_ref[:, :256])
        qs[c] = (qk[:, :128] * 32 ** (-0.5)).astype(BF16)
        ks[c] = qk[:, 128:].astype(BF16)
        gt[c] = jax.nn.sigmoid(dot(wgt, nx, NT))
        return 0

    lax.fori_loop(0, 16, project, 0)
    for b in range(4):
        rows = nx_ref[:, 32 * b : 32 * b + 32, :].reshape(512, 128)
        vt[b, :128] = dot(wvt, rows, NT).astype(BF16)
        vt[b, 128:] = jnp.ones((16, 512), BF16)

    def block(r, _):
        for core in range(2):
            got = bx_ref[core, pl.ds(pl.multiple_of(8 * r, 8), 8)].astype(F32)
            bias[:, core] = got + mask[:, core]
        for b in range(4):
            q = qs[pl.ds(2 * r, 2), 32 * b : 32 * b + 32, :].reshape(4, 1, 16, 128)
            hd = lax.broadcasted_iota(jnp.int32, (4, 4, 16, 128), 1)
            ln = lax.broadcasted_iota(jnp.int32, (4, 4, 16, 128), 3)
            qm = jnp.where(
                hd == ln // 32, jnp.broadcast_to(q, (4, 4, 16, 128)).astype(F32), 0.0
            ).astype(BF16)
            keys = ks[:, 32 * b : 32 * b + 32, :].reshape(512, 128)
            st = dot(keys, qm.reshape(256, 128), NT) + bias[...].reshape(512, 256)
            p = jnp.exp(st - jnp.max(st, axis=0, keepdims=True)).astype(BF16)
            ot = dot(vt[b], p)
            ot = ot[:128] / ot[128:129]
            for h in range(4):
                part = ot[32 * h : 32 * h + 32]
                for j in range(4):
                    at = 64 * (j % 2) + 16 * h
                    to = 32 * b + 16 * (j % 2)
                    moved = part[:, 128 * (j // 2) : 128 * (j // 2) + 128]
                    if (to - at) % 128:
                        moved = pltpu.roll(moved, (to - at) % 128, 1)
                    here = (lane128 >= to) & (lane128 < to + 16)
                    rows = slice(32 * h, 32 * h + 32)
                    tile[j // 2, rows] = jnp.where(here, moved, tile[j // 2, rows])
        for c in range(2):
            go_ref[2 * r + c] = (tile[c] * gt[2 * r + c]).astype(BF16)
        return 0

    tile[...] = jnp.zeros((2, 128, 128), F32)
    lax.fori_loop(0, 8, block, 0)


def final_body(gx_ref, mid_ref, att_out_ref, y_ref):
    def one(s, _):
        y = mid_ref[s] + dot(gx_ref[s], att_out_ref[...], TN)
        for b in range(4):
            y_ref[16 * b + s] = y[32 * b : 32 * b + 32]
        return 0

    lax.fori_loop(0, 16, one, 0)


VMEM = pl.BlockSpec(memory_space=pltpu.VMEM)
SMEM = pl.BlockSpec(memory_space=pltpu.SMEM)
LIMIT = 60 * 1024 * 1024


def call(body, outs, ins, scratch=(), smem=(), **params):
    many = isinstance(outs, list)
    return pl.pallas_call(
        body,
        out_shape=[jax.ShapeDtypeStruct(*o) for o in outs] if many else jax.ShapeDtypeStruct(*outs),
        in_specs=[SMEM if n in smem else VMEM for n in range(len(ins))],
        out_specs=[VMEM] * len(outs) if many else VMEM,
        scratch_shapes=list(scratch),
        compiler_params=pltpu.CompilerParams(vmem_limit_bytes=LIMIT, **params),
    )(*ins)


def spread_body(x_ref, o_ref, send_sem, near_sem, far_sem):
    r, c = lax.axis_index("row"), lax.axis_index("col")
    core = c % 2
    mate = c + 1 - 2 * core
    bar = pltpu.get_barrier_semaphore()

    def peer(k):
        return (lax.rem(r + k // 8, 8), 2 * lax.rem(c // 2 + k % 8, 8) + core)

    def greet(k, _):
        pl.semaphore_signal(bar, inc=1, device_id=peer(k), device_id_type=MESH)
        return 0

    lax.fori_loop(1, 64, greet, 0)
    pl.semaphore_signal(bar, inc=1, device_id=(r, mate), device_id_type=MESH)
    pl.semaphore_wait(bar, 64)

    def send(k, _):
        pltpu.make_async_remote_copy(
            x_ref, o_ref.at[core, 8 * r + c // 2], send_sem, near_sem, peer(k), MESH
        ).start()
        return 0

    lax.fori_loop(1, 64, send, 0)
    o_ref[core, 8 * r + c // 2] = x_ref[...]
    most = o_ref.at[0, pl.ds(0, 63)]
    pltpu.make_async_copy(most, most, near_sem).wait()
    pltpu.make_async_copy(most, most, send_sem).wait()
    mine = o_ref.at[core]
    copy = pltpu.make_async_remote_copy(mine, mine, send_sem, far_sem, (r, mate), MESH)
    copy.start()
    copy.wait()


def per_device(pair, valid_length, tri_in, tri_gate, tri_out, att_in, att_bias, att_out):
    both = ("row", "col")
    bias8 = jnp.pad(att_bias.T, ((0, 4), (0, 0)))
    edges, normed = call(
        edges_body,
        [((128, 2, 16, 128), BF16), ((16, 128, 128), BF16)],
        (pair, valid_length, tri_in),
        [pltpu.VMEM((512, 128), BF16), pltpu.VMEM((8, 256, 256), BF16)],
        smem=(1,),
    )
    got = lax.all_to_all(edges, both, 0, 0, tiled=True)
    products = call(
        triangle_body,
        ((128, 16, 128), BF16),
        (got,),
        [pltpu.VMEM((512, 512), BF16), pltpu.VMEM((512, 512), BF16)],
    )
    home = lax.all_to_all(products, both, 0, 0, tiled=True)
    middle, mid_norm, bias = call(
        middle_body,
        [((16, 128, 128), F32), ((16, 128, 128), BF16), ((32, 256), BF16)],
        (pair, normed, home, tri_gate, tri_out, bias8),
        [pltpu.VMEM((16, 128, 128), BF16), pltpu.VMEM((128, 128), F32)],
    )
    rows = lax.all_to_all(mid_norm, "col", 0, 0, tiled=True)
    bias_all = call(
        spread_body,
        ((2, 64, 32, 256), BF16),
        (bias,),
        [pltpu.SemaphoreType.DMA] * 3,
        collective_id=1,
        has_side_effects=True,
    )
    gated = call(
        attend_body,
        ((16, 128, 128), BF16),
        (rows, bias_all, valid_length, att_in),
        [
            pltpu.VMEM((16, 128, 128), BF16),
            pltpu.VMEM((16, 128, 128), BF16),
            pltpu.VMEM((4, 144, 512), BF16),
            pltpu.VMEM((16, 128, 128), F32),
            pltpu.VMEM((8, 2, 32, 256), F32),
            pltpu.VMEM((2, 128, 128), F32),
        ],
        smem=(2,),
    )
    back = lax.all_to_all(gated, "col", 0, 0, tiled=True)
    return call(final_body, ((64, 32, 128), F32), (back, middle, att_out))


def solution(mesh):
    placed = (P("row", "col", None), P(), P(), P(), P(), P(), P(), P())
    return jax.shard_map(
        per_device, mesh=mesh, in_specs=placed, out_specs=P("row", "col", None), check_vma=False
    )
```

```python
import jax
import jax.numpy as jnp
from jax import lax
from jax.experimental import pallas as pl
from jax.experimental.pallas import tpu as pltpu
from jax.sharding import PartitionSpec as P

MESH = pl.DeviceIdType.MESH
F32 = jnp.float32
BF16 = jnp.bfloat16
NT = (((1,), (1,)), ((), ()))
TN = (((0,), (0,)), ((), ()))
NN = (((1,), (0,)), ((), ()))


def dot(a, b, dims=NN):
    return lax.dot_general(a, b, dims, preferred_element_type=F32)


def norm_last(x):
    c = x - jnp.mean(x, axis=-1, keepdims=True)
    return c * lax.rsqrt(jnp.mean(c * c, axis=-1, keepdims=True) + 1e-5)


def turned(w):
    return w.astype(F32).T.astype(BF16)


def swap16():
    p = lax.broadcasted_iota(jnp.int32, (256, 256), 0)
    q = lax.broadcasted_iota(jnp.int32, (256, 256), 1)
    return (q == (p % 16) * 16 + p // 16).astype(F32).astype(BF16)


def block_turn(tiles):
    return [
        jnp.concatenate([t[:, 32 * b : 32 * b + 32] for t in tiles], axis=1) for b in range(4)
    ]


def tile_of(x_ref, s):
    return jnp.concatenate([x_ref[16 * b + s] for b in range(4)], axis=0)


def rows16(start):
    return pl.ds(pl.multiple_of(16 * start, 16), 16)


def loop(low, high, body, unroll=1):
    def step(n, carry):
        body(n)
        return carry

    lax.fori_loop(low, high, step, 0, unroll=unroll)


def push(src, dst, send_sem, recv_sem, row, col):
    pltpu.make_async_remote_copy(src, dst, send_sem, recv_sem, (row, col), MESH).start()


def take(ref, sem):
    pltpu.make_async_copy(ref, ref, sem).wait()


def kernel(
    x_ref, len_ref, tri_in_ref, tri_gate_ref, tri_out_ref, bias_ref, att_in_ref, att_out_ref, y_ref,
    wt, wvt, wgt, y, e, rx, n, lm, rm, po, px, gate, np_, yb, mid, nm, nx, bm, bx,
    qs, ks, vt, gt, bias, tile, go, gx,
    edge_send, edge_recv, prod_send, prod_recv, norm_send, norm_recv,
    near_send, near, far_send, far, back_send, back_recv,
):
    row, col = lax.axis_index("row"), lax.axis_index("col")
    me = 16 * row + col
    chip, core = col // 2, col % 2
    mate = col + 1 - 2 * core
    bar = pltpu.get_barrier_semaphore()

    def greet(k):
        t = lax.rem(me + k, 128)
        pl.semaphore_signal(bar, inc=1, device_id=(t // 16, t % 16), device_id_type=MESH)

    loop(1, 128, greet)

    wt[...] = turned(tri_in_ref[...])
    perm = swap16()
    lane128 = lax.broadcasted_iota(jnp.int32, (1, 128), 1)
    length = len_ref[0]
    keep_k = (32 * col + lane128 % 32) < length
    for side in range(2):

        def edge(s):
            if side == 0:
                nb = norm_last(tile_of(x_ref, s)).astype(BF16)
                n[s] = nb
            else:
                nb = n[s]
            pt = dot(wt[256 * side : 256 * side + 256], nb, NT)
            w = jnp.where(keep_k & ((64 * row + (lane128 // 32) * 16 + s) < length), 1.0, 0.0)
            v = (jax.nn.sigmoid(pt[:128]) * pt[128:] * w).astype(BF16)
            for g in range(8):
                at = slice(128 * (g % 2), 128 * (g % 2) + 128)
                y[g // 2, rows16(s), at] = v[16 * g : 16 * g + 16]

        loop(0, 16, edge, 4)

        def order(g):
            z = dot(perm, y[g]).astype(BF16)
            e[side, rows16(2 * g)] = z[:, :128].reshape(16, 16, 128)
            e[side, rows16(2 * g + 1)] = z[:, 128:].reshape(16, 16, 128)

        loop(0, 4, order, 4)
        if side == 0:
            pl.semaphore_wait(bar, 127)

        def send_edge(k):
            t = lax.rem(me + k, 128)
            push(
                e.at[side, t], rx.at[side, me], edge_send.at[side], edge_recv.at[side], t // 16, t % 16
            )

        loop(1, 128, send_edge)
        rx[side, me] = e[side, me]

    def make_gate(s):
        gate[s] = jax.nn.sigmoid(dot(n[s], tri_gate_ref[...]))

    loop(0, 16, make_gate, 4)
    wvt[...] = turned(att_in_ref[:, 256:384])
    wgt[...] = turned(att_in_ref[:, 384:512])

    for side, m in ((0, lm), (1, rm)):
        take(rx.at[side, pl.ds(0, 127)], edge_recv.at[side])

        def gather(r):
            for cg in range(4):
                tiles = [rx[side, 16 * r + 4 * cg + c] for c in range(4)]
                for b, t in enumerate(block_turn(tiles)):
                    m[rows16(4 * r + b), 128 * cg : 128 * cg + 128] = t

        loop(0, 8, gather, 4)

    def product(o):
        r = lax.rem(row + o, 8)
        p = dot(lm[pl.ds(pl.multiple_of(64 * r, 64), 64), :], rm[...], NT).astype(BF16)
        for cg in range(4):
            tiles = [p[16 * b : 16 * b + 16, 128 * cg : 128 * cg + 128] for b in range(4)]
            for c, t in enumerate(block_turn(tiles)):
                po[16 * r + 4 * cg + c] = t

        def send_product(k):
            c = lax.rem(col + k, 16)
            push(po.at[16 * r + c], px.at[me], prod_send, prod_recv, r, c)

        loop(jnp.where(o == 0, 1, 0), 16, send_product)

    loop(0, 8, product)
    px[me] = po[me]
    take(px.at[pl.ds(0, 127)], prod_recv)

    zero = jnp.zeros((16, 128), F32)
    total = lax.fori_loop(0, 128, lambda c, a: a + px[c].astype(F32), zero, unroll=16)
    mean = total * (1.0 / 128)

    def square(c, a):
        d = px[c].astype(F32) - mean
        return a + d * d

    scale = lax.rsqrt(lax.fori_loop(0, 128, square, zero, unroll=16) * (1.0 / 128) + 1e-5)

    def normed(g):
        z = ((px[rows16(g)].astype(F32) - mean[None]) * scale[None]).astype(BF16)
        z = dot(perm, z.reshape(256, 128)).astype(BF16)
        np_[:, rows16(g), :] = z.reshape(16, 16, 128)

    loop(0, 8, normed, 4)
    wb = bias_ref[...]

    def middle(q):
        for s in [4 * q + k for k in range(4)]:
            m = tile_of(x_ref, s) + gate[s] * dot(np_[s], tri_out_ref[...], TN)
            mid[s] = m
            nb = norm_last(m).astype(BF16)
            nm[s] = nb
            yb[pl.ds(s, 8, stride=16), :] = dot(wb, nb, NT)
        for k in range(4):
            s = 4 * q + k

            @pl.when(s != col)
            def _():
                push(nm.at[s], nx.at[col], norm_send, norm_recv, row, s)

    loop(0, 4, middle)
    nx[col] = nm[col]
    yt = yb[...].T
    bm[...] = jnp.concatenate([yt[32 * b : 32 * b + 32, :64] for b in range(4)], axis=1).astype(BF16)
    mine = 64 * core + 8 * row + chip

    def send_bias(o):
        to = lax.rem(row - o + 8, 8)

        def one(k):
            r = lax.rem(row + k, 8)

            @pl.when((k > 0) | (to != chip))
            def _():
                push(bm, bx.at[mine], near_send, near.at[o], r, 2 * to + core)

            @pl.when(o == 0)
            def _():
                push(bm, bx.at[mine], near_send, near.at[o], r, 2 * to + 1 - core)

        loop(0, 8, one)

    loop(0, 8, send_bias)
    bx[mine] = bm[...]

    kk = lax.broadcasted_iota(jnp.int32, (512, 256), 0)
    mask = jnp.where(kk < length, 0.0, -1e9).astype(F32).reshape(8, 2, 32, 256)
    own_step = lax.rem(row - chip + 8, 8)
    take(nx.at[pl.ds(0, 15)], norm_recv)

    def project(c):
        nb = nx[c]
        qk = dot(nb, att_in_ref[:, :256])
        qs[c] = (qk[:, :128] * 32 ** (-0.5)).astype(BF16)
        ks[c] = qk[:, 128:].astype(BF16)
        gt[c] = jax.nn.sigmoid(dot(wgt[...], nb, NT))

    loop(0, 16, project, 4)
    for b in range(4):
        vt[b, :128] = dot(wvt[...], nx[:, 32 * b : 32 * b + 32, :].reshape(512, 128), NT).astype(BF16)
        vt[b, 128:] = jnp.ones((16, 512), BF16)
    tile[...] = jnp.zeros((2, 128, 128), F32)

    def await_near(o, count):
        @pl.when(o == own_step)
        def _():
            take(bx.at[pl.ds(0, count - 1)], near.at[o])

        @pl.when(o != own_step)
        def _():
            take(bx.at[pl.ds(0, count)], near.at[o])

    def block(o):
        r = lax.rem(chip + o, 8)

        @pl.when(o == 0)
        def _():
            await_near(0, 16)

        @pl.when(o > 0)
        def _():
            take(bx.at[pl.ds(0, 8)], far.at[o])

        for k in range(2):
            got = bx[pl.ds(pl.multiple_of(64 * k + 8 * r, 8), 8)].astype(F32)
            bias[:, k] = got + mask[:, k]
        for b in range(4):
            if b == 2:

                @pl.when(o < 7)
                def _():
                    await_near(o + 1, 8)
                    ahead = bx.at[pl.ds(64 * core + 8 * lax.rem(r + 1, 8), 8)]
                    push(ahead, ahead, far_send, far.at[o + 1], row, mate)

            q = qs[pl.ds(2 * r, 2), 32 * b : 32 * b + 32, :].reshape(4, 1, 16, 128)
            hd = lax.broadcasted_iota(jnp.int32, (4, 4, 16, 128), 1)
            ln = lax.broadcasted_iota(jnp.int32, (4, 4, 16, 128), 3)
            qm = jnp.where(
                hd == ln // 32, jnp.broadcast_to(q, (4, 4, 16, 128)).astype(F32), 0.0
            ).astype(BF16)
            keys = ks[:, 32 * b : 32 * b + 32, :].reshape(512, 128)
            st = dot(keys, qm.reshape(256, 128), NT) + bias[...].reshape(512, 256)
            p = jnp.exp(st - jnp.max(st, axis=0, keepdims=True)).astype(BF16)
            ot = dot(vt[b], p)
            ot = ot[:128] / ot[128:129]
            for h in range(4):
                part = ot[32 * h : 32 * h + 32]
                for j in range(4):
                    at = 64 * (j % 2) + 16 * h
                    to = 32 * b + 16 * (j % 2)
                    moved = part[:, 128 * (j // 2) : 128 * (j // 2) + 128]
                    if (to - at) % 128:
                        moved = pltpu.roll(moved, (to - at) % 128, 1)
                    here = (lane128 >= to) & (lane128 < to + 16)
                    rows = slice(32 * h, 32 * h + 32)
                    tile[j // 2, rows] = jnp.where(here, moved, tile[j // 2, rows])
        for k in range(2):
            c = 2 * r + k
            go[c] = (tile[k] * gt[c]).astype(BF16)
        for k in range(2):
            c = 2 * r + k

            @pl.when(c != col)
            def _():
                push(go.at[c], gx.at[col], back_send, back_recv, row, c)

    loop(0, 8, block)
    gx[col] = go[col]
    take(gx.at[pl.ds(0, 15)], back_recv)

    def final(s):
        out = mid[s] + dot(gx[s], att_out_ref[...], TN)
        for b in range(4):
            y_ref[16 * b + s] = out[32 * b : 32 * b + 32]

    loop(0, 16, final, 4)
    for side in range(2):
        take(e.at[side, pl.ds(0, 127)], edge_send.at[side])
    take(px.at[pl.ds(0, 127)], prod_send)
    take(nx.at[pl.ds(0, 15)], norm_send)
    take(bx.at[pl.ds(0, 71)], near_send)
    take(bx.at[pl.ds(0, 56)], far_send)
    take(gx.at[pl.ds(0, 15)], back_send)


SCRATCH = [
    ((512, 128), BF16),
    ((128, 128), BF16),
    ((128, 128), BF16),
    ((4, 256, 256), BF16),
    ((2, 128, 16, 128), BF16),
    ((2, 128, 16, 128), BF16),
    ((16, 128, 128), BF16),
    ((512, 512), BF16),
    ((512, 512), BF16),
    ((128, 16, 128), BF16),
    ((128, 16, 128), BF16),
    ((16, 128, 128), F32),
    ((16, 128, 128), BF16),
    ((128, 128), F32),
    ((16, 128, 128), F32),
    ((16, 128, 128), BF16),
    ((16, 128, 128), BF16),
    ((32, 256), BF16),
    ((128, 32, 256), BF16),
    ((16, 128, 128), BF16),
    ((16, 128, 128), BF16),
    ((4, 144, 512), BF16),
    ((16, 128, 128), F32),
    ((8, 2, 32, 256), F32),
    ((2, 128, 128), F32),
    ((16, 128, 128), BF16),
    ((16, 128, 128), BF16),
]
SEMAPHORES = [(2,), (2,), (), (), (), (), (), (8,), (), (8,), (), ()]


def per_device(pair, valid_length, tri_in, tri_gate, tri_out, att_in, att_bias, att_out):
    bias8 = jnp.pad(att_bias.T, ((0, 4), (0, 0)))
    vmem = pl.BlockSpec(memory_space=pltpu.VMEM)
    smem = pl.BlockSpec(memory_space=pltpu.SMEM)
    return pl.pallas_call(
        kernel,
        out_shape=jax.ShapeDtypeStruct((64, 32, 128), F32),
        in_specs=[vmem, smem] + [vmem] * 6,
        out_specs=vmem,
        scratch_shapes=[pltpu.VMEM(*s) for s in SCRATCH]
        + [pltpu.SemaphoreType.DMA(s) for s in SEMAPHORES],
        compiler_params=pltpu.CompilerParams(
            collective_id=0, has_side_effects=True, vmem_limit_bytes=56 * 1024 * 1024
        ),
    )(pair, valid_length, tri_in, tri_gate, tri_out, bias8, att_in, att_out)


def solution(mesh):
    placed = (P("row", "col", None), P(), P(), P(), P(), P(), P(), P())
    return jax.shard_map(
        per_device, mesh=mesh, in_specs=placed, out_specs=P("row", "col", None), check_vma=False
    )
```

```python
import jax
import jax.numpy as jnp
from jax import lax
from jax.experimental import pallas as pl
from jax.experimental.pallas import tpu as pltpu
from jax.sharding import PartitionSpec as P

MESH = pl.DeviceIdType.MESH
F32 = jnp.float32
BF16 = jnp.bfloat16
NT = (((1,), (1,)), ((), ()))
TN = (((0,), (0,)), ((), ()))
NN = (((1,), (0,)), ((), ()))


def dot(a, b, dims=NN):
    return lax.dot_general(a, b, dims, preferred_element_type=F32)


def norm_last(x):
    c = x - jnp.mean(x, axis=-1, keepdims=True)
    return c * lax.rsqrt(jnp.mean(c * c, axis=-1, keepdims=True) + 1e-5)


def turned(w):
    return w.astype(F32).T.astype(BF16)


def swap16():
    p = lax.broadcasted_iota(jnp.int32, (256, 256), 0)
    q = lax.broadcasted_iota(jnp.int32, (256, 256), 1)
    return (q == (p % 16) * 16 + p // 16).astype(F32).astype(BF16)


def block_turn(tiles):
    return [
        jnp.concatenate([t[:, 32 * b : 32 * b + 32] for t in tiles], axis=1) for b in range(4)
    ]


def tile_of(x_ref, s):
    return jnp.concatenate([x_ref[16 * b + s] for b in range(4)], axis=0)


def rows16(start):
    return pl.ds(pl.multiple_of(16 * start, 16), 16)


def loop(low, high, body, unroll=1):
    def step(n, carry):
        body(n)
        return carry

    lax.fori_loop(low, high, step, 0, unroll=unroll)


def push(src, dst, send_sem, recv_sem, row, col):
    pltpu.make_async_remote_copy(src, dst, send_sem, recv_sem, (row, col), MESH).start()


def take(ref, sem):
    pltpu.make_async_copy(ref, ref, sem).wait()


def kernel(
    x_hbm, len_ref, tri_in_ref, tri_gate_ref, tri_out_ref, bias_ref, att_in_ref, mid, gx,
    x_ref, wt, wvt, wgt, y, e, rx, n, lm, rm, po, px, gate, np_, yb, nm, nx, bm, bx,
    qs, ks, vt, gt, bias, tile, go,
    load, right_send, right_recv, left_send, left_recv, prod_send, prod_recv, norm_send, norm_recv,
    line_send, line, near_send, near, far_send, far, back_send, back_recv,
):
    row, col = lax.axis_index("row"), lax.axis_index("col")
    me = 16 * row + col
    chip, core = col // 2, col % 2
    z_lo, x_at = chip // 4, chip % 4
    mate = col + 1 - 2 * core
    bar = pltpu.get_barrier_semaphore()
    fetch = pltpu.make_async_copy(x_hbm, x_ref, load)
    fetch.start()

    def greet(r, first=0):
        for k in range(first, 16):
            c = lax.rem(col + k, 16)
            pl.semaphore_signal(bar, inc=1, device_id=(r, c), device_id_type=MESH)

    greet(row, 1)
    loop(1, 8, lambda a: greet(lax.rem(row + a, 8)))
    wt[...] = turned(tri_in_ref[...])
    perm = swap16()
    lane128 = lax.broadcasted_iota(jnp.int32, (1, 128), 1)
    length = len_ref[0]
    keep_k = (32 * col + lane128 % 32) < length
    fetch.wait()

    def edge(side, s, nb):
        pt = dot(wt[256 * side : 256 * side + 256], nb, NT)
        w = jnp.where(keep_k & ((64 * row + (lane128 // 32) * 16 + s) < length), 1.0, 0.0)
        v = (jax.nn.sigmoid(pt[:128]) * pt[128:] * w).astype(BF16)
        for g in range(8):
            at = slice(128 * (g % 2), 128 * (g % 2) + 128)
            y[g // 2, rows16(s), at] = v[16 * g : 16 * g + 16]

    def order(side):
        for g in range(4):
            z = dot(perm, y[g]).astype(BF16)
            e[side, 32 * g : 32 * g + 16] = z[:, :128].reshape(16, 16, 128)
            e[side, 32 * g + 16 : 32 * g + 32] = z[:, 128:].reshape(16, 16, 128)

    def first_edge(s):
        nb = norm_last(tile_of(x_ref, s)).astype(BF16)
        n[s] = nb
        edge(1, s, nb)

    def send_right(a):
        r = lax.rem(row + a, 8)
        for k in range(1 if a == 0 else 0, 16):
            c = lax.rem(col + k, 16)
            push(e.at[1, 16 * r + c], rx.at[1, me], right_send, right_recv, r, c)

    def send_left(a):
        r = lax.rem(row + 8 - a, 8)
        for k in range(1 if a == 0 else 0, 16):
            c = lax.rem(col + k, 16)
            push(e.at[0, 16 * r + c], rx.at[0, me], left_send, left_recv.at[a], r, c)

    loop(0, 16, first_edge, 4)
    order(1)
    pl.semaphore_wait(bar, 127)
    for q in range(4):
        send_right(2 * q)
        send_right(2 * q + 1)
        for s in range(4 * q, 4 * q + 4):
            edge(0, s, n[s])
    rx[1, me] = e[1, me]
    order(0)
    for q in range(4):
        send_left(2 * q)
        send_left(2 * q + 1)
        for s in range(4 * q, 4 * q + 4):
            gate[s] = jax.nn.sigmoid(dot(n[s], tri_gate_ref[...]))
    rx[0, me] = e[0, me]
    wvt[...] = turned(att_in_ref[:, 256:384])
    wgt[...] = turned(att_in_ref[:, 384:512])

    def assemble(side, r, m, at):
        for cg in range(4):
            tiles = [rx[side, 16 * r + 4 * cg + c] for c in range(4)]
            for b, t in enumerate(block_turn(tiles)):
                m[rows16(at + b), 128 * cg : 128 * cg + 128] = t

    take(rx.at[1, pl.ds(0, 127)], right_recv)
    loop(0, 8, lambda r: assemble(1, r, rm, 4 * r), 4)

    def product(o, first=0):
        r = lax.rem(row + o, 8)
        take(rx.at[0, pl.ds(0, 16 - first)], left_recv.at[o])
        assemble(0, r, lm, 0)
        p = dot(lm[...], rm[...], NT).astype(BF16)
        for cg in range(4):
            tiles = [p[16 * b : 16 * b + 16, 128 * cg : 128 * cg + 128] for b in range(4)]
            for c, t in enumerate(block_turn(tiles)):
                po[16 * r + 4 * cg + c] = t
        for k in range(first, 16):
            c = lax.rem(col + k, 16)
            push(po.at[16 * r + c], px.at[me], prod_send, prod_recv, r, c)

    product(0, 1)
    loop(1, 8, product)
    px[me] = po[me]
    take(px.at[pl.ds(0, 127)], prod_recv)

    zero = jnp.zeros((16, 128), F32)
    total = lax.fori_loop(0, 128, lambda c, a: a + px[c].astype(F32), zero, unroll=16)
    mean = total * (1.0 / 128)

    def square(c, a):
        d = px[c].astype(F32) - mean
        return a + d * d

    scale = lax.rsqrt(lax.fori_loop(0, 128, square, zero, unroll=16) * (1.0 / 128) + 1e-5)

    def normed(g):
        z = ((px[rows16(g)].astype(F32) - mean[None]) * scale[None]).astype(BF16)
        z = dot(perm, z.reshape(256, 128)).astype(BF16)
        np_[:, rows16(g), :] = z.reshape(16, 16, 128)

    loop(0, 8, normed, 4)
    wb = bias_ref[...]

    def send_norm(s):
        @pl.when(s != col)
        def _():
            push(nm.at[s], nx.at[col], norm_send, norm_recv, row, s)

    def middle(q):
        for s in [4 * q + k for k in range(4)]:
            m = tile_of(x_ref, s) + gate[s] * dot(np_[s], tri_out_ref[...], TN)
            mid[s] = m
            nb = norm_last(m).astype(BF16)
            nm[s] = nb
            yb[pl.ds(s, 4, stride=16), :] = dot(wb, nb, NT)

        @pl.when(q < 2)
        def _():
            for k in range(4):
                send_norm(4 * q + k)

    loop(0, 4, middle)
    yt = yb[...].T
    bm[...] = jnp.concatenate([yt[32 * b : 32 * b + 32] for b in range(4)], axis=1).astype(BF16)
    line_of = 64 * core + 8 * row + 4 * z_lo
    mine = line_of + x_at
    for k in range(1, 4):
        c = 8 * z_lo + 2 * lax.rem(x_at + k, 4) + core
        push(bm, bx.at[mine], line_send, line, row, c)
    loop(8, 16, send_norm)
    nx[col] = nm[col]
    bx[mine] = bm[...]
    take(bx.at[pl.ds(0, 3)], line)
    own_step = lax.rem(8 - chip, 8)

    def send_bias(o):
        group = bx.at[pl.ds(line_of, 4)]
        for z in range(2):
            r = lax.rem(row - x_at - 4 * z - o + 16, 8)
            c = 8 * z + 2 * x_at

            @pl.when((r != row) | (z_lo != z))
            def _():
                push(group, group, near_send, near.at[o], r, c + core)

            @pl.when(o == 0)
            def _():
                push(group, group, near_send, near.at[o], r, c + 1 - core)

    loop(0, 8, send_bias)

    kk = lax.broadcasted_iota(jnp.int32, (512, 256), 0)
    mask = jnp.where(kk < length, 0.0, -1e9).astype(F32).reshape(8, 2, 32, 256)
    take(nx.at[pl.ds(0, 15)], norm_recv)

    def project(c):
        nb = nx[c]
        qk = dot(nb, att_in_ref[:, :256])
        qs[c] = (qk[:, :128] * 32 ** (-0.5)).astype(BF16)
        ks[c] = qk[:, 128:].astype(BF16)
        gt[c] = jax.nn.sigmoid(dot(wgt[...], nb, NT))

    loop(0, 16, project, 4)
    for b in range(4):
        vt[b, :128] = dot(wvt[...], nx[:, 32 * b : 32 * b + 32, :].reshape(512, 128), NT).astype(BF16)
        vt[b, 128:] = jnp.ones((16, 512), BF16)
    tile[...] = jnp.zeros((2, 128, 128), F32)

    def await_near(o, count):
        @pl.when(o == own_step)
        def _():
            take(bx.at[pl.ds(0, count - 4)], near.at[o])

        @pl.when(o != own_step)
        def _():
            take(bx.at[pl.ds(0, count)], near.at[o])

    def block(o):
        r = lax.rem(chip + row + o, 8)

        @pl.when(o == 0)
        def _():
            await_near(0, 16)

        @pl.when(o > 0)
        def _():
            take(bx.at[pl.ds(0, 8)], far.at[o])

        for k in range(2):
            got = bx[pl.ds(pl.multiple_of(64 * k + 8 * r, 8), 8)].astype(F32)
            bias[:, k] = got + mask[:, k]
        for b in range(4):
            if b == 2:

                @pl.when(o < 7)
                def _():
                    await_near(o + 1, 8)
                    ahead = bx.at[pl.ds(64 * core + 8 * lax.rem(r + 1, 8), 8)]
                    push(ahead, ahead, far_send, far.at[o + 1], row, mate)

            q = qs[pl.ds(2 * r, 2), 32 * b : 32 * b + 32, :].reshape(4, 1, 16, 128)
            hd = lax.broadcasted_iota(jnp.int32, (4, 4, 16, 128), 1)
            ln = lax.broadcasted_iota(jnp.int32, (4, 4, 16, 128), 3)
            qm = jnp.where(
                hd == ln // 32, jnp.broadcast_to(q, (4, 4, 16, 128)).astype(F32), 0.0
            ).astype(BF16)
            keys = ks[:, 32 * b : 32 * b + 32, :].reshape(512, 128)
            st = dot(keys, qm.reshape(256, 128), NT) + bias[...].reshape(512, 256)
            p = jnp.exp(st - jnp.max(st, axis=0, keepdims=True)).astype(BF16)
            ot = dot(vt[b], p)
            ot = ot[:128] / ot[128:129]
            for h in range(4):
                part = ot[32 * h : 32 * h + 32]
                for j in range(4):
                    at = 64 * (j % 2) + 16 * h
                    to = 32 * b + 16 * (j % 2)
                    moved = part[:, 128 * (j // 2) : 128 * (j // 2) + 128]
                    if (to - at) % 128:
                        moved = pltpu.roll(moved, (to - at) % 128, 1)
                    here = (lane128 >= to) & (lane128 < to + 16)
                    rows = slice(32 * h, 32 * h + 32)
                    tile[j // 2, rows] = jnp.where(here, moved, tile[j // 2, rows])
        for k in range(2):
            c = 2 * r + k
            go[c] = (tile[k] * gt[c]).astype(BF16)
        for k in range(2):
            c = 2 * r + k

            @pl.when(c != col)
            def _():
                push(go.at[c], gx.at[col], back_send, back_recv, row, c)

    loop(0, 8, block)
    gx[col] = go[col]
    take(rx.at[0, pl.ds(0, 127)], right_send)
    take(rx.at[0, pl.ds(0, 127)], left_send)
    take(px.at[pl.ds(0, 127)], prod_send)
    take(nx.at[pl.ds(0, 15)], norm_send)
    take(bx.at[pl.ds(0, 3)], line_send)
    take(bx.at[pl.ds(0, 68)], near_send)
    take(bx.at[pl.ds(0, 56)], far_send)
    take(gx.at[pl.ds(0, 15)], back_send)
    take(gx.at[pl.ds(0, 15)], back_recv)


def final(gx_ref, mid_ref, att_out_ref, y_ref):
    for s in range(4):
        out = mid_ref[s] + dot(gx_ref[s], att_out_ref[...], TN)
        for b in range(4):
            y_ref[b, s] = out[32 * b : 32 * b + 32]


SCRATCH = [
    ((64, 32, 128), F32),
    ((512, 128), BF16),
    ((128, 128), BF16),
    ((128, 128), BF16),
    ((4, 256, 256), BF16),
    ((2, 128, 16, 128), BF16),
    ((2, 128, 16, 128), BF16),
    ((16, 128, 128), BF16),
    ((64, 512), BF16),
    ((512, 512), BF16),
    ((128, 16, 128), BF16),
    ((128, 16, 128), BF16),
    ((16, 128, 128), F32),
    ((16, 128, 128), BF16),
    ((64, 128), F32),
    ((16, 128, 128), BF16),
    ((16, 128, 128), BF16),
    ((32, 256), BF16),
    ((128, 32, 256), BF16),
    ((16, 128, 128), BF16),
    ((16, 128, 128), BF16),
    ((4, 144, 512), BF16),
    ((16, 128, 128), F32),
    ((8, 2, 32, 256), F32),
    ((2, 128, 128), F32),
    ((16, 128, 128), BF16),
]
SEMAPHORES = [(), (), (), (), (8,), (), (), (), (), (), (), (), (8,), (), (8,), (), ()]


def per_device(pair, valid_length, tri_in, tri_gate, tri_out, att_in, att_bias, att_out):
    vmem = pl.BlockSpec(memory_space=pltpu.VMEM)
    smem = pl.BlockSpec(memory_space=pltpu.SMEM)
    middle, back = pl.pallas_call(
        kernel,
        out_shape=[
            jax.ShapeDtypeStruct((16, 128, 128), F32),
            jax.ShapeDtypeStruct((16, 128, 128), BF16),
        ],
        in_specs=[pl.BlockSpec(memory_space=pl.ANY), smem] + [vmem] * 5,
        out_specs=[vmem, vmem],
        scratch_shapes=[pltpu.VMEM(*s) for s in SCRATCH]
        + [pltpu.SemaphoreType.DMA(s) for s in SEMAPHORES],
        compiler_params=pltpu.CompilerParams(
            collective_id=0, has_side_effects=True, vmem_limit_bytes=56 * 1024 * 1024
        ),
    )(pair, valid_length, tri_in, tri_gate, tri_out, att_bias.T, att_in)
    tiles = pl.BlockSpec((4, 128, 128), lambda s: (s, 0, 0))
    out = pl.pallas_call(
        final,
        grid=(4,),
        out_shape=jax.ShapeDtypeStruct((4, 16, 32, 128), F32),
        in_specs=[tiles, tiles, pl.BlockSpec((128, 128), lambda s: (0, 0))],
        out_specs=pl.BlockSpec((4, 4, 32, 128), lambda s: (0, s, 0, 0)),
    )(back, middle, att_out)
    return out.reshape(64, 32, 128)


def solution(mesh):
    placed = (P("row", "col", None), P(), P(), P(), P(), P(), P(), P())
    return jax.shard_map(
        per_device, mesh=mesh, in_specs=placed, out_specs=P("row", "col", None), check_vma=False
    )
```

```python
import jax
import jax.numpy as jnp
from jax import lax
from jax.experimental import pallas as pl
from jax.experimental.pallas import tpu as pltpu
from jax.sharding import PartitionSpec as P

MESH = pl.DeviceIdType.MESH
F32 = jnp.float32
BF16 = jnp.bfloat16
NT = (((1,), (1,)), ((), ()))
TN = (((0,), (0,)), ((), ()))
NN = (((1,), (0,)), ((), ()))


def dot(a, b, dims=NN):
    return lax.dot_general(a, b, dims, preferred_element_type=F32)


def norm_last(x):
    c = x - jnp.mean(x, axis=-1, keepdims=True)
    return c * lax.rsqrt(jnp.mean(c * c, axis=-1, keepdims=True) + 1e-5)


def turned(w):
    return w.astype(F32).T.astype(BF16)


def swap16():
    p = lax.broadcasted_iota(jnp.int32, (256, 256), 0)
    q = lax.broadcasted_iota(jnp.int32, (256, 256), 1)
    return (q == (p % 16) * 16 + p // 16).astype(F32).astype(BF16)


def block_turn(tiles):
    return [
        jnp.concatenate([t[:, 32 * b : 32 * b + 32] for t in tiles], axis=1) for b in range(4)
    ]


def tile_of(x_ref, s):
    return jnp.concatenate([x_ref[16 * b + s] for b in range(4)], axis=0)


def rows16(start):
    return pl.ds(pl.multiple_of(16 * start, 16), 16)


def loop(low, high, body, unroll=1):
    def step(n, carry):
        body(n)
        return carry

    lax.fori_loop(low, high, step, 0, unroll=unroll)


def push(src, dst, send_sem, recv_sem, row, col):
    pltpu.make_async_remote_copy(src, dst, send_sem, recv_sem, (row, col), MESH).start()


def take(ref, sem):
    pltpu.make_async_copy(ref, ref, sem).wait()


def kernel(
    x_hbm, len_ref, tri_in_ref, tri_gate_ref, tri_out_ref, bias_ref, att_in_ref, mid_hbm, gx,
    x_ref, mid, wt, wvt, wgt, y, e, rx, n, lm, rm, po, px, gate, np_, yb, nm, nx, bm, bx,
    qs, ks, vt, gt, bias, tile, go,
    load, right_send, right_recv, left_send, left_recv, prod_send, prod_recv, norm_send, norm_recv,
    line_send, line, plane_send, plane, near_send, near, far_send, far, back_send, back_recv, keep,
):
    row, col = lax.axis_index("row"), lax.axis_index("col")
    me = 16 * row + col
    chip, core = col // 2, col % 2
    z_lo, x_at = chip // 4, chip % 4
    y_at, z_at = row // 2, 2 * (row % 2) + z_lo
    mate = col + 1 - 2 * core
    bar = pltpu.get_barrier_semaphore()
    fetch = pltpu.make_async_copy(x_hbm, x_ref, load)
    fetch.start()

    def greet(r, first=0):
        for k in range(first, 16):
            c = lax.rem(col + k, 16)
            pl.semaphore_signal(bar, inc=1, device_id=(r, c), device_id_type=MESH)

    greet(row, 1)
    loop(1, 8, lambda a: greet(lax.rem(row + a, 8)))
    wt[...] = turned(tri_in_ref[...])
    perm = swap16()
    lane128 = lax.broadcasted_iota(jnp.int32, (1, 128), 1)
    length = len_ref[0]
    keep_k = (32 * col + lane128 % 32) < length
    fetch.wait()

    def edge(side, s, nb):
        pt = dot(wt[256 * side : 256 * side + 256], nb, NT)
        w = jnp.where(keep_k & ((64 * row + (lane128 // 32) * 16 + s) < length), 1.0, 0.0)
        v = (jax.nn.sigmoid(pt[:128]) * pt[128:] * w).astype(BF16)
        for g in range(8):
            at = slice(128 * (g % 2), 128 * (g % 2) + 128)
            y[g // 2, rows16(s), at] = v[16 * g : 16 * g + 16]

    def order(side):
        for g in range(4):
            z = dot(perm, y[g]).astype(BF16)
            e[side, 32 * g : 32 * g + 16] = z[:, :128].reshape(16, 16, 128)
            e[side, 32 * g + 16 : 32 * g + 32] = z[:, 128:].reshape(16, 16, 128)

    def first_edge(s):
        nb = norm_last(tile_of(x_ref, s)).astype(BF16)
        n[s] = nb
        edge(1, s, nb)

    def send_right(a):
        r = lax.rem(row + a, 8)
        for k in range(1 if a == 0 else 0, 16):
            c = lax.rem(col + k, 16)
            push(e.at[1, 16 * r + c], rx.at[1, me], right_send, right_recv, r, c)

    def send_left(a):
        r = lax.rem(row + 8 - a, 8)
        for k in range(1 if a == 0 else 0, 16):
            c = lax.rem(col + k, 16)
            push(e.at[0, 16 * r + c], rx.at[0, me], left_send, left_recv.at[a], r, c)

    loop(0, 16, first_edge, 4)
    order(1)
    pl.semaphore_wait(bar, 127)
    for q in range(4):
        send_right(2 * q)
        send_right(2 * q + 1)
        for s in range(4 * q, 4 * q + 4):
            edge(0, s, n[s])
    rx[1, me] = e[1, me]
    order(0)
    for q in range(4):
        send_left(2 * q)
        send_left(2 * q + 1)
        for s in range(4 * q, 4 * q + 4):
            gate[s] = jax.nn.sigmoid(dot(n[s], tri_gate_ref[...]))
    rx[0, me] = e[0, me]
    wvt[...] = turned(att_in_ref[:, 256:384])
    wgt[...] = turned(att_in_ref[:, 384:512])

    def assemble(side, r, m, at):
        for cg in range(4):
            tiles = [rx[side, 16 * r + 4 * cg + c] for c in range(4)]
            for b, t in enumerate(block_turn(tiles)):
                m[rows16(at + b), 128 * cg : 128 * cg + 128] = t

    take(rx.at[1, pl.ds(0, 127)], right_recv)
    loop(0, 8, lambda r: assemble(1, r, rm, 4 * r), 4)

    def product(o, first=0):
        r = lax.rem(row + o, 8)
        take(rx.at[0, pl.ds(0, 16 - first)], left_recv.at[o])
        assemble(0, r, lm, 0)
        p = dot(lm[...], rm[...], NT).astype(BF16)
        for cg in range(4):
            tiles = [p[16 * b : 16 * b + 16, 128 * cg : 128 * cg + 128] for b in range(4)]
            for c, t in enumerate(block_turn(tiles)):
                po[16 * r + 4 * cg + c] = t
        for k in range(first, 16):
            c = lax.rem(col + k, 16)
            push(po.at[16 * r + c], px.at[me], prod_send, prod_recv, r, c)

    product(0, 1)
    loop(1, 8, product)
    px[me] = po[me]
    take(px.at[pl.ds(0, 127)], prod_recv)

    zero = jnp.zeros((16, 128), F32)
    total = lax.fori_loop(0, 128, lambda c, a: a + px[c].astype(F32), zero, unroll=16)
    mean = total * (1.0 / 128)

    def square(c, a):
        d = px[c].astype(F32) - mean
        return a + d * d

    scale = lax.rsqrt(lax.fori_loop(0, 128, square, zero, unroll=16) * (1.0 / 128) + 1e-5)

    def normed(g):
        z = ((px[rows16(g)].astype(F32) - mean[None]) * scale[None]).astype(BF16)
        z = dot(perm, z.reshape(256, 128)).astype(BF16)
        np_[:, rows16(g), :] = z.reshape(16, 16, 128)

    loop(0, 8, normed, 4)
    wb = bias_ref[...]

    def send_norm(s):
        @pl.when(s != col)
        def _():
            push(nm.at[s], nx.at[col], norm_send, norm_recv, row, s)

    def middle(q):
        first = 4 * lax.rem(q + 2 - 2 * z_lo, 4)
        for s in [first + k for k in range(4)]:
            m = tile_of(x_ref, s) + gate[s] * dot(np_[s], tri_out_ref[...], TN)
            mid[s] = m
            nb = norm_last(m).astype(BF16)
            nm[s] = nb
            yb[pl.ds(s, 4, stride=16), :] = dot(wb, nb, NT)

        @pl.when(q < 2)
        def _():
            for k in range(4):
                s = first + k
                push(nm.at[s], nx.at[col], norm_send, norm_recv, row, s)

    loop(0, 4, middle)
    yt = yb[...].T
    bm[...] = jnp.concatenate([yt[32 * b : 32 * b + 32] for b in range(4)], axis=1).astype(BF16)
    line_of = 64 * core + 8 * row + 4 * z_lo
    mine = line_of + x_at
    for k in range(1, 4):
        c = 8 * z_lo + 2 * lax.rem(x_at + k, 4) + core
        push(bm, bx.at[mine], line_send, line, row, c)
    loop(8 * z_lo, 8 * z_lo + 8, send_norm)
    nx[col] = nm[col]
    bx[mine] = bm[...]
    saved = pltpu.make_async_copy(mid, mid_hbm, keep.at[0])
    saved.start()
    take(bx.at[pl.ds(0, 3)], line)
    group = bx.at[pl.ds(line_of, 4)]
    for k in range(1, 4):
        z = lax.rem(z_at + k, 4)
        push(group, group, plane_send, plane, 2 * y_at + z // 2, 8 * (z % 2) + 2 * x_at + core)

    def rows_of(o):
        turn = 2 * (x_at % 2)
        back = jnp.where(o < 2, 0, jnp.where(o < 4, 1 + turn, jnp.where(o < 6, 3 - turn, 2)))
        half = lax.rem(o + x_at, 2)
        return 2 * lax.rem(y_at - back + 4, 4) + half, 2 * back + half

    def bias_rows(r):
        return bx.at[pl.ds(64 * core + 8 * r, 8)]

    take(bx.at[pl.ds(0, 12)], plane)
    for o in range(2):
        mine_ = bias_rows(rows_of(o)[0])
        push(mine_, mine_, far_send, far.at[o], row, mate)
    for k in (1, 3, 2):
        for half in range(2):
            mine_ = bias_rows(2 * y_at + half)
            r = 2 * lax.rem(y_at + k, 4) + row % 2
            push(mine_, mine_, near_send, near.at[2 * k + half], r, col)

    kk = lax.broadcasted_iota(jnp.int32, (512, 256), 0)
    mask = jnp.where(kk < length, 0.0, -1e9).astype(F32).reshape(8, 2, 32, 256)
    take(nx.at[pl.ds(0, 15)], norm_recv)

    def project(c):
        nb = nx[c]
        qk = dot(nb, att_in_ref[:, :256])
        qs[c] = (qk[:, :128] * 32 ** (-0.5)).astype(BF16)
        ks[c] = qk[:, 128:].astype(BF16)
        gt[c] = jax.nn.sigmoid(dot(wgt[...], nb, NT))

    loop(0, 16, project, 4)
    for b in range(4):
        vt[b, :128] = dot(wvt[...], nx[:, 32 * b : 32 * b + 32, :].reshape(512, 128), NT).astype(BF16)
        vt[b, 128:] = jnp.ones((16, 512), BF16)
    tile[...] = jnp.zeros((2, 128, 128), F32)

    def block(o):
        r = rows_of(o)[0]
        take(bx.at[pl.ds(0, 8)], far.at[o])
        for k in range(2):
            got = bx[pl.ds(pl.multiple_of(64 * k + 8 * r, 8), 8)].astype(F32)
            bias[:, k] = got + mask[:, k]
        for b in range(4):
            if b == 2:

                @pl.when((o > 0) & (o < 7))
                def _():
                    later, slot = rows_of(o + 1)
                    take(bx.at[pl.ds(0, 8)], near.at[slot])
                    push(bias_rows(later), bias_rows(later), far_send, far.at[o + 1], row, mate)

            q = qs[pl.ds(2 * r, 2), 32 * b : 32 * b + 32, :].reshape(4, 1, 16, 128)
            hd = lax.broadcasted_iota(jnp.int32, (4, 4, 16, 128), 1)
            ln = lax.broadcasted_iota(jnp.int32, (4, 4, 16, 128), 3)
            qm = jnp.where(
                hd == ln // 32, jnp.broadcast_to(q, (4, 4, 16, 128)).astype(F32), 0.0
            ).astype(BF16)
            keys = ks[:, 32 * b : 32 * b + 32, :].reshape(512, 128)
            st = dot(keys, qm.reshape(256, 128), NT) + bias[...].reshape(512, 256)
            p = jnp.exp(st - jnp.max(st, axis=0, keepdims=True)).astype(BF16)
            ot = dot(vt[b], p)
            ot = ot[:128] / ot[128:129]
            for h in range(4):
                part = ot[32 * h : 32 * h + 32]
                for j in range(4):
                    at = 64 * (j % 2) + 16 * h
                    to = 32 * b + 16 * (j % 2)
                    moved = part[:, 128 * (j // 2) : 128 * (j // 2) + 128]
                    if (to - at) % 128:
                        moved = pltpu.roll(moved, (to - at) % 128, 1)
                    here = (lane128 >= to) & (lane128 < to + 16)
                    rows = slice(32 * h, 32 * h + 32)
                    tile[j // 2, rows] = jnp.where(here, moved, tile[j // 2, rows])
        for k in range(2):
            c = 2 * r + k
            go[c] = (tile[k] * gt[c]).astype(BF16)
        for k in range(2):
            c = 2 * r + k

            @pl.when(c != col)
            def _():
                push(go.at[c], gx.at[col], back_send, back_recv, row, c)

    loop(0, 8, block)
    own = pltpu.make_async_copy(go.at[col], gx.at[col], keep.at[1])
    own.start()
    take(rx.at[0, pl.ds(0, 127)], right_send)
    take(rx.at[0, pl.ds(0, 127)], left_send)
    take(px.at[pl.ds(0, 127)], prod_send)
    take(nx.at[pl.ds(0, 15)], norm_send)
    take(bx.at[pl.ds(0, 3)], line_send)
    take(bx.at[pl.ds(0, 12)], plane_send)
    take(bx.at[pl.ds(0, 48)], near_send)
    take(bx.at[pl.ds(0, 64)], far_send)
    saved.wait()
    own.wait()
    take(go.at[pl.ds(0, 15)], back_send)
    take(go.at[pl.ds(0, 15)], back_recv)


def final(gx_hbm, mid_hbm, att_out_ref, y_hbm, gx, mid, y, gx_sem, mid_sem, y_sem):
    def fetch(g):
        at = pl.ds(4 * g, 4)
        return (
            pltpu.make_async_copy(gx_hbm.at[at], gx.at[at], gx_sem.at[g]),
            pltpu.make_async_copy(mid_hbm.at[at], mid.at[at], mid_sem.at[g]),
        )

    def store(g):
        at = pl.ds(4 * g, 4)
        return pltpu.make_async_copy(y.at[:, at], y_hbm.at[:, at], y_sem.at[g])

    for g in range(4):
        for copy in fetch(g):
            copy.start()
    for g in range(4):
        for copy in fetch(g):
            copy.wait()
        for s in range(4 * g, 4 * g + 4):
            out = mid[s] + dot(gx[s], att_out_ref[...], TN)
            for b in range(4):
                y[b, s] = out[32 * b : 32 * b + 32]
        store(g).start()
    for g in range(4):
        store(g).wait()


SCRATCH = [
    ((64, 32, 128), F32),
    ((16, 128, 128), F32),
    ((512, 128), BF16),
    ((128, 128), BF16),
    ((128, 128), BF16),
    ((4, 256, 256), BF16),
    ((2, 128, 16, 128), BF16),
    ((2, 128, 16, 128), BF16),
    ((16, 128, 128), BF16),
    ((64, 512), BF16),
    ((512, 512), BF16),
    ((128, 16, 128), BF16),
    ((128, 16, 128), BF16),
    ((16, 128, 128), F32),
    ((16, 128, 128), BF16),
    ((64, 128), F32),
    ((16, 128, 128), BF16),
    ((16, 128, 128), BF16),
    ((32, 256), BF16),
    ((128, 32, 256), BF16),
    ((16, 128, 128), BF16),
    ((16, 128, 128), BF16),
    ((4, 144, 512), BF16),
    ((16, 128, 128), F32),
    ((8, 2, 32, 256), F32),
    ((2, 128, 128), F32),
    ((16, 128, 128), BF16),
]
SEMAPHORES = [(), (), (), (), (8,), (), (), (), (), (), (), (), (), (), (8,), (), (8,), (), (), (2,)]


def per_device(pair, valid_length, tri_in, tri_gate, tri_out, att_in, att_bias, att_out):
    vmem = pl.BlockSpec(memory_space=pltpu.VMEM)
    smem = pl.BlockSpec(memory_space=pltpu.SMEM)
    anywhere = pl.BlockSpec(memory_space=pl.ANY)
    middle, back = pl.pallas_call(
        kernel,
        out_shape=[
            jax.ShapeDtypeStruct((16, 128, 128), F32),
            jax.ShapeDtypeStruct((16, 128, 128), BF16),
        ],
        in_specs=[anywhere, smem] + [vmem] * 5,
        out_specs=[anywhere, anywhere],
        scratch_shapes=[pltpu.VMEM(*s) for s in SCRATCH]
        + [pltpu.SemaphoreType.DMA(s) for s in SEMAPHORES],
        compiler_params=pltpu.CompilerParams(
            collective_id=0, has_side_effects=True, vmem_limit_bytes=60 * 1024 * 1024
        ),
    )(pair, valid_length, tri_in, tri_gate, tri_out, att_bias.T, att_in)
    out = pl.pallas_call(
        final,
        out_shape=jax.ShapeDtypeStruct((4, 16, 32, 128), F32),
        in_specs=[anywhere, anywhere, vmem],
        out_specs=anywhere,
        scratch_shapes=[
            pltpu.VMEM((16, 128, 128), BF16),
            pltpu.VMEM((16, 128, 128), F32),
            pltpu.VMEM((4, 16, 32, 128), F32),
        ]
        + [pltpu.SemaphoreType.DMA((4,))] * 3,
        compiler_params=pltpu.CompilerParams(vmem_limit_bytes=60 * 1024 * 1024),
    )(back, middle, att_out)
    return out.reshape(64, 32, 128)


def solution(mesh):
    placed = (P("row", "col", None), P(), P(), P(), P(), P(), P(), P())
    return jax.shard_map(
        per_device, mesh=mesh, in_specs=placed, out_specs=P("row", "col", None), check_vma=False
    )
```

```python
import jax
import jax.numpy as jnp
from jax import lax
from jax.experimental import pallas as pl
from jax.experimental.pallas import tpu as pltpu
from jax.sharding import PartitionSpec as P

MESH = pl.DeviceIdType.MESH
LOG2E = 1.4426950408889634
F32 = jnp.float32
BF16 = jnp.bfloat16
NT = (((1,), (1,)), ((), ()))
TN = (((0,), (0,)), ((), ()))
NN = (((1,), (0,)), ((), ()))


def dot(a, b, dims=NN):
    return lax.dot_general(a, b, dims, preferred_element_type=F32)


def norm_last(x):
    c = x - jnp.mean(x, axis=-1, keepdims=True)
    return c * lax.rsqrt(jnp.mean(c * c, axis=-1, keepdims=True) + 1e-5)


def turned(w):
    return w.astype(F32).T.astype(BF16)


def swap16():
    p = lax.broadcasted_iota(jnp.int32, (256, 256), 0)
    q = lax.broadcasted_iota(jnp.int32, (256, 256), 1)
    return (q == (p % 16) * 16 + p // 16).astype(F32).astype(BF16)


def block_turn(tiles):
    return [
        jnp.concatenate([t[:, 32 * b : 32 * b + 32] for t in tiles], axis=1) for b in range(4)
    ]


def tile_of(x_ref, s):
    return jnp.concatenate([x_ref[16 * b + s] for b in range(4)], axis=0)


def rows16(start):
    return pl.ds(pl.multiple_of(16 * start, 16), 16)


def loop(low, high, body, unroll=1):
    def step(n, carry):
        body(n)
        return carry

    lax.fori_loop(low, high, step, 0, unroll=unroll)


def push(src, dst, send_sem, recv_sem, row, col):
    pltpu.make_async_remote_copy(src, dst, send_sem, recv_sem, (row, col), MESH).start()


def take(ref, sem):
    pltpu.make_async_copy(ref, ref, sem).wait()


def kernel(
    x_hbm, len_ref, tri_in_ref, tri_gate_ref, tri_out_ref, bias_ref, att_in_ref, att_out_ref, out_hbm,
    x_ref, gx, out, update, wt, wvt, wgt, y, e, rx, n, lm, rm, po, px, gate, np_, yb, nm, nx, bm, bx,
    qs, ks, vt, gt, bias, scores, tile, go,
    load, right_send, right_recv, left_send, left_recv, prod_send, prod_recv, norm_send, norm_recv,
    line_send, line, plane_send, plane, near_send, near, far_send, far, back_send, back_recv, keep,
):
    row, col = lax.axis_index("row"), lax.axis_index("col")
    me = 16 * row + col
    chip, core = col // 2, col % 2
    z_lo, x_at = chip // 4, chip % 4
    y_at, z_at = row // 2, 2 * (row % 2) + z_lo
    mate = col + 1 - 2 * core
    bar = pltpu.get_barrier_semaphore()
    fetch = pltpu.make_async_copy(x_hbm, x_ref, load)
    fetch.start()

    def greet(r, first=0):
        for k in range(first, 16):
            c = lax.rem(col + k, 16)
            pl.semaphore_signal(bar, inc=1, device_id=(r, c), device_id_type=MESH)

    greet(row, 1)
    loop(1, 8, lambda a: greet(lax.rem(row + a, 8)))
    wt[...] = turned(tri_in_ref[...])
    perm = swap16()
    lane128 = lax.broadcasted_iota(jnp.int32, (1, 128), 1)
    length = len_ref[0]
    keep_k = (32 * col + lane128 % 32) < length
    fetch.wait()

    def edge(side, s, nb):
        pt = dot(wt[256 * side : 256 * side + 256], nb, NT)
        w = jnp.where(keep_k & ((64 * row + (lane128 // 32) * 16 + s) < length), 1.0, 0.0)
        v = (jax.nn.sigmoid(pt[:128]) * pt[128:] * w).astype(BF16)
        for g in range(8):
            at = slice(128 * (g % 2), 128 * (g % 2) + 128)
            y[g // 2, rows16(s), at] = v[16 * g : 16 * g + 16]

    def order(side):
        for g in range(4):
            z = dot(perm, y[g]).astype(BF16)
            e[side, 32 * g : 32 * g + 16] = z[:, :128].reshape(16, 16, 128)
            e[side, 32 * g + 16 : 32 * g + 32] = z[:, 128:].reshape(16, 16, 128)

    def first_edge(s):
        nb = norm_last(tile_of(x_ref, s)).astype(BF16)
        n[s] = nb
        edge(1, s, nb)

    def send_right(a):
        r = lax.rem(row + a, 8)
        for k in range(1 if a == 0 else 0, 16):
            c = lax.rem(col + k, 16)
            push(e.at[1, 16 * r + c], rx.at[1, me], right_send, right_recv, r, c)

    def send_left(a):
        r = lax.rem(row + 8 - a, 8)
        for k in range(1 if a == 0 else 0, 16):
            c = lax.rem(col + k, 16)
            push(e.at[0, 16 * r + c], rx.at[0, me], left_send, left_recv.at[a], r, c)

    loop(0, 16, first_edge, 4)
    order(1)
    pl.semaphore_wait(bar, 127)
    for q in range(4):
        send_right(2 * q)
        send_right(2 * q + 1)
        for s in range(4 * q, 4 * q + 4):
            edge(0, s, n[s])
    rx[1, me] = e[1, me]
    order(0)
    for q in range(4):
        send_left(2 * q)
        send_left(2 * q + 1)
        for s in range(4 * q, 4 * q + 4):
            gate[s] = jax.nn.sigmoid(dot(n[s], tri_gate_ref[...]))
    rx[0, me] = e[0, me]
    wvt[...] = turned(att_in_ref[:, 256:384])
    wgt[...] = turned(att_in_ref[:, 384:512])

    def assemble(side, r, m, at):
        for cg in range(4):
            tiles = [rx[side, 16 * r + 4 * cg + c] for c in range(4)]
            for b, t in enumerate(block_turn(tiles)):
                m[rows16(at + b), 128 * cg : 128 * cg + 128] = t

    take(rx.at[1, pl.ds(0, 127)], right_recv)
    loop(0, 8, lambda r: assemble(1, r, rm, 4 * r), 4)

    def product(o, first=0):
        r = lax.rem(row + o, 8)
        take(rx.at[0, pl.ds(0, 16 - first)], left_recv.at[o])
        assemble(0, r, lm, 0)
        p = dot(lm[...], rm[...], NT).astype(BF16)
        for cg in range(4):
            tiles = [p[16 * b : 16 * b + 16, 128 * cg : 128 * cg + 128] for b in range(4)]
            for c, t in enumerate(block_turn(tiles)):
                po[16 * r + 4 * cg + c] = t
        for k in range(first, 16):
            c = lax.rem(col + k, 16)
            push(po.at[16 * r + c], px.at[me], prod_send, prod_recv, r, c)

    product(0, 1)
    loop(1, 8, product)
    px[me] = po[me]
    take(px.at[pl.ds(0, 127)], prod_recv)

    zero = jnp.zeros((16, 128), F32)
    total = lax.fori_loop(0, 128, lambda c, a: a + px[c].astype(F32), zero, unroll=16)
    mean = total * (1.0 / 128)

    def square(c, a):
        d = px[c].astype(F32) - mean
        return a + d * d

    scale = lax.rsqrt(lax.fori_loop(0, 128, square, zero, unroll=16) * (1.0 / 128) + 1e-5)

    def normed(g):
        z = ((px[rows16(g)].astype(F32) - mean[None]) * scale[None]).astype(BF16)
        z = dot(perm, z.reshape(256, 128)).astype(BF16)
        np_[:, rows16(g), :] = z.reshape(16, 16, 128)

    loop(0, 8, normed, 4)
    wb = bias_ref[...]

    def send_norm(s):
        @pl.when(s != col)
        def _():
            push(nm.at[s], nx.at[col], norm_send, norm_recv, row, s)

    def middle(q):
        first = 4 * lax.rem(q + 2 - 2 * z_lo, 4)
        for s in [first + k for k in range(4)]:
            u = gate[s] * dot(np_[s], tri_out_ref[...], TN)
            update[s] = u
            nb = norm_last(tile_of(x_ref, s) + u).astype(BF16)
            nm[s] = nb
            yb[pl.ds(s, 4, stride=16), :] = dot(wb, nb, NT)

        @pl.when(q < 2)
        def _():
            for k in range(4):
                s = first + k
                push(nm.at[s], nx.at[col], norm_send, norm_recv, row, s)

    loop(0, 4, middle)
    yt = yb[...].T
    bm[...] = jnp.concatenate([yt[32 * b : 32 * b + 32] for b in range(4)], axis=1).astype(BF16)
    line_of = 64 * core + 8 * row + 4 * z_lo
    mine = line_of + x_at
    for k in range(1, 4):
        c = 8 * z_lo + 2 * lax.rem(x_at + k, 4) + core
        push(bm, bx.at[mine], line_send, line, row, c)
    loop(8 * z_lo, 8 * z_lo + 8, send_norm)
    nx[col] = nm[col]
    bx[mine] = bm[...]
    take(bx.at[pl.ds(0, 3)], line)
    group = bx.at[pl.ds(line_of, 4)]
    for k in range(1, 4):
        z = lax.rem(z_at + k, 4)
        push(group, group, plane_send, plane, 2 * y_at + z // 2, 8 * (z % 2) + 2 * x_at + core)

    def rows_of(o):
        turn = 2 * (x_at % 2)
        back = jnp.where(o < 2, 0, jnp.where(o < 4, 1 + turn, jnp.where(o < 6, 3 - turn, 2)))
        half = lax.rem(o + x_at, 2)
        return 2 * lax.rem(y_at - back + 4, 4) + half, 2 * back + half

    def bias_rows(r):
        return bx.at[pl.ds(64 * core + 8 * r, 8)]

    take(bx.at[pl.ds(0, 12)], plane)
    for o in range(2):
        mine_ = bias_rows(rows_of(o)[0])
        push(mine_, mine_, far_send, far.at[o], row, mate)
    for half in range(2):
        for k in (1, 3):
            mine_ = bias_rows(2 * y_at + half)
            r = 2 * lax.rem(y_at + k, 4) + row % 2
            push(mine_, mine_, near_send, near.at[2 * k + half], r, col)

    kk = lax.broadcasted_iota(jnp.int32, (512, 256), 0)
    mask = jnp.where(kk < length, 0.0, -1e9).astype(F32).reshape(8, 2, 32, 256)
    take(nx.at[pl.ds(0, 15)], norm_recv)

    def project(c):
        nb = nx[c]
        qk = dot(nb, att_in_ref[:, :256])
        qs[c] = (qk[:, :128] * 32 ** (-0.5)).astype(BF16)
        ks[c] = qk[:, 128:].astype(BF16)
        gt[c] = jax.nn.sigmoid(dot(wgt[...], nb, NT))

    loop(0, 16, project, 4)
    for b in range(4):
        vt[b, :128] = dot(wvt[...], nx[:, 32 * b : 32 * b + 32, :].reshape(512, 128), NT).astype(BF16)
        vt[b, 128:] = jnp.ones((16, 512), BF16)
    tile[...] = jnp.zeros((2, 128, 128), F32)

    def block(o):
        r = rows_of(o)[0]

        @pl.when((o > 0) & (o < 7))
        def _():
            later, slot = rows_of(o + 1)
            rows = bias_rows(later)
            take(bx.at[pl.ds(0, 8)], near.at[slot])
            push(rows, rows, far_send, far.at[o + 1], row, mate)
            for k, half in ((1, 0), (3, 1)):

                @pl.when(slot == 2 * k + half)
                def _():
                    to = 2 * lax.rem(y_at + k, 4) + row % 2
                    push(rows, rows, near_send, near.at[4 + half], to, col)

        take(bx.at[pl.ds(0, 8)], far.at[o])
        for k in range(2):
            got = bx[pl.ds(pl.multiple_of(64 * k + 8 * r, 8), 8)].astype(F32)
            bias[:, k] = (got + mask[:, k]) * LOG2E

        def score(b):
            q = qs[pl.ds(2 * r, 2), 32 * b : 32 * b + 32, :].reshape(4, 1, 16, 128)
            hd = lax.broadcasted_iota(jnp.int32, (4, 4, 16, 128), 1)
            ln = lax.broadcasted_iota(jnp.int32, (4, 4, 16, 128), 3)
            qm = jnp.where(
                hd == ln // 32, jnp.broadcast_to(q, (4, 4, 16, 128)).astype(F32), 0.0
            ).astype(BF16)
            keys = ks[:, 32 * b : 32 * b + 32, :].reshape(512, 128)
            st = dot(keys, qm.reshape(256, 128), NT) * LOG2E + bias[...].reshape(512, 256)
            scores[b] = st
            return jnp.max(st, axis=0, keepdims=True)

        top = score(0)
        for b in range(4):
            later_top = score(b + 1) if b < 3 else None
            ot = dot(vt[b], jnp.exp2(scores[b] - top).astype(BF16))
            ot = ot[:128] * (1.0 / ot[128:129])
            for h in range(4):
                part = ot[32 * h : 32 * h + 32]
                for j in range(4):
                    at = 64 * (j % 2) + 16 * h
                    to = 32 * b + 16 * (j % 2)
                    moved = part[:, 128 * (j // 2) : 128 * (j // 2) + 128]
                    if (to - at) % 128:
                        moved = pltpu.roll(moved, (to - at) % 128, 1)
                    here = (lane128 >= to) & (lane128 < to + 16)
                    rows = slice(32 * h, 32 * h + 32)
                    tile[j // 2, rows] = jnp.where(here, moved, tile[j // 2, rows])
            top = later_top
        for k in range(2):
            c = 2 * r + k
            go[c] = (tile[k] * gt[c]).astype(BF16)
        for k in range(2):
            c = 2 * r + k

            @pl.when(c != col)
            def _():
                push(go.at[c], gx.at[col], back_send, back_recv, row, c)

    loop(0, 8, block)
    gx[col] = go[col]
    take(gx.at[pl.ds(0, 15)], back_recv)

    def store(g):
        at = pl.ds(4 * g, 4)
        return pltpu.make_async_copy(out.at[:, at], out_hbm.at[:, at], keep.at[g])

    for g in range(4):
        for s in range(4 * g, 4 * g + 4):
            t = update[s] + dot(gx[s], att_out_ref[...], TN)
            for b in range(4):
                out[b, s] = t[32 * b : 32 * b + 32]
        store(g).start()
    take(rx.at[0, pl.ds(0, 127)], right_send)
    take(rx.at[0, pl.ds(0, 127)], left_send)
    take(px.at[pl.ds(0, 127)], prod_send)
    take(nx.at[pl.ds(0, 15)], norm_send)
    take(bx.at[pl.ds(0, 3)], line_send)
    take(bx.at[pl.ds(0, 12)], plane_send)
    take(bx.at[pl.ds(0, 48)], near_send)
    take(bx.at[pl.ds(0, 64)], far_send)
    take(go.at[pl.ds(0, 15)], back_send)
    for g in range(4):
        store(g).wait()


SCRATCH = [
    ((64, 32, 128), F32),
    ((16, 128, 128), BF16),
    ((4, 16, 32, 128), F32),
    ((16, 128, 128), F32),
    ((512, 128), BF16),
    ((128, 128), BF16),
    ((128, 128), BF16),
    ((4, 256, 256), BF16),
    ((2, 128, 16, 128), BF16),
    ((2, 128, 16, 128), BF16),
    ((16, 128, 128), BF16),
    ((64, 512), BF16),
    ((512, 512), BF16),
    ((128, 16, 128), BF16),
    ((128, 16, 128), BF16),
    ((16, 128, 128), F32),
    ((16, 128, 128), BF16),
    ((64, 128), F32),
    ((16, 128, 128), BF16),
    ((16, 128, 128), BF16),
    ((32, 256), BF16),
    ((128, 32, 256), BF16),
    ((16, 128, 128), BF16),
    ((16, 128, 128), BF16),
    ((4, 144, 512), BF16),
    ((16, 128, 128), F32),
    ((8, 2, 32, 256), F32),
    ((4, 512, 256), F32),
    ((2, 128, 128), F32),
    ((16, 128, 128), BF16),
]
SEMAPHORES = [(), (), (), (), (8,), (), (), (), (), (), (), (), (), (), (8,), (), (8,), (), (), (4,)]


def per_device(pair, valid_length, tri_in, tri_gate, tri_out, att_in, att_bias, att_out):
    vmem = pl.BlockSpec(memory_space=pltpu.VMEM)
    smem = pl.BlockSpec(memory_space=pltpu.SMEM)
    anywhere = pl.BlockSpec(memory_space=pl.ANY)
    change = pl.pallas_call(
        kernel,
        out_shape=jax.ShapeDtypeStruct((4, 16, 32, 128), F32),
        in_specs=[anywhere, smem] + [vmem] * 6,
        out_specs=anywhere,
        scratch_shapes=[pltpu.VMEM(*s) for s in SCRATCH]
        + [pltpu.SemaphoreType.DMA(s) for s in SEMAPHORES],
        compiler_params=pltpu.CompilerParams(
            collective_id=0, has_side_effects=True, vmem_limit_bytes=60 * 1024 * 1024
        ),
    )(pair, valid_length, tri_in, tri_gate, tri_out, att_bias.T, att_in, att_out)
    return pair + change.reshape(64, 32, 128)


def solution(mesh):
    placed = (P("row", "col", None), P(), P(), P(), P(), P(), P(), P())
    return jax.shard_map(
        per_device, mesh=mesh, in_specs=placed, out_specs=P("row", "col", None), check_vma=False
    )
```

```python
import jax
import jax.numpy as jnp
from jax import lax
from jax.experimental import pallas as pl
from jax.experimental.pallas import tpu as pltpu
from jax.sharding import PartitionSpec as P

MESH = pl.DeviceIdType.MESH
LOG2E = 1.4426950408889634
F32 = jnp.float32
BF16 = jnp.bfloat16
NT = (((1,), (1,)), ((), ()))
TN = (((0,), (0,)), ((), ()))
NN = (((1,), (0,)), ((), ()))


def dot(a, b, dims=NN):
    return lax.dot_general(a, b, dims, preferred_element_type=F32)


def norm_last(x):
    c = x - jnp.mean(x, axis=-1, keepdims=True)
    return c * lax.rsqrt(jnp.mean(c * c, axis=-1, keepdims=True) + 1e-5)


def turned(w):
    return w.astype(F32).T.astype(BF16)


def swap16():
    p = lax.broadcasted_iota(jnp.int32, (256, 256), 0)
    q = lax.broadcasted_iota(jnp.int32, (256, 256), 1)
    return (q == (p % 16) * 16 + p // 16).astype(F32).astype(BF16)


def block_turn(tiles):
    return [
        jnp.concatenate([t[:, 32 * b : 32 * b + 32] for t in tiles], axis=1) for b in range(4)
    ]


def tile_of(x_ref, s):
    return jnp.concatenate([x_ref[16 * b + s] for b in range(4)], axis=0)


def rows16(start):
    return pl.ds(pl.multiple_of(16 * start, 16), 16)


def loop(low, high, body, unroll=1):
    def step(n, carry):
        body(n)
        return carry

    lax.fori_loop(low, high, step, 0, unroll=unroll)


def push(src, dst, send_sem, recv_sem, row, col):
    pltpu.make_async_remote_copy(src, dst, send_sem, recv_sem, (row, col), MESH).start()


def take(ref, sem):
    pltpu.make_async_copy(ref, ref, sem).wait()


def kernel(
    x_hbm, len_ref, tri_in_hbm, tri_gate_hbm, tri_out_hbm, bias_hbm, att_in_hbm, att_out_hbm, out,
    x_ref, tri_in_ref, tri_gate_ref, tri_out_ref, bias_ref, att_in_ref, att_out_ref, gx, update, wt, wvt, wgt, y, e, rx, n, lm, rm, po, px, gate, np_, yb, nm, nx, bm, bx,
    qs, ks, vt, gt, bias, scores, tile, go,
    load, right_send, right_recv, left_send, left_recv, prod_send, prod_recv, norm_send, norm_recv,
    line_send, line, plane_send, plane, near_send, near, far_send, far, back_send, back_recv,
):
    row, col = lax.axis_index("row"), lax.axis_index("col")
    me = 16 * row + col
    chip, core = col // 2, col % 2
    z_lo, x_at = chip // 4, chip % 4
    y_at, z_at = row // 2, 2 * (row % 2) + z_lo
    mate = col + 1 - 2 * core
    bar = pltpu.get_barrier_semaphore()
    pairs = (
        (tri_in_hbm, tri_in_ref), (x_hbm, x_ref), (tri_gate_hbm, tri_gate_ref), (att_in_hbm, att_in_ref),
        (tri_out_hbm, tri_out_ref), (bias_hbm, bias_ref), (att_out_hbm, att_out_ref),
    )
    fetch = [pltpu.make_async_copy(a, b, load.at[n]) for n, (a, b) in enumerate(pairs)]
    for copy in fetch:
        copy.start()

    def greet(r, first=0):
        for k in range(first, 16):
            c = lax.rem(col + k, 16)
            pl.semaphore_signal(bar, inc=1, device_id=(r, c), device_id_type=MESH)

    greet(row, 1)
    loop(1, 8, lambda a: greet(lax.rem(row + a, 8)))
    fetch[0].wait()
    wt[...] = turned(tri_in_ref[...])
    perm = swap16()
    lane128 = lax.broadcasted_iota(jnp.int32, (1, 128), 1)
    length = len_ref[0]
    keep_k = (32 * col + lane128 % 32) < length
    fetch[1].wait()

    def edge(side, s, nb):
        pt = dot(wt[256 * side : 256 * side + 256], nb, NT)
        w = jnp.where(keep_k & ((64 * row + (lane128 // 32) * 16 + s) < length), 1.0, 0.0)
        v = (jax.nn.sigmoid(pt[:128]) * pt[128:] * w).astype(BF16)
        for g in range(8):
            at = slice(128 * (g % 2), 128 * (g % 2) + 128)
            y[g // 2, rows16(s), at] = v[16 * g : 16 * g + 16]

    def order(side):
        for g in range(4):
            z = dot(perm, y[g]).astype(BF16)
            e[side, 32 * g : 32 * g + 16] = z[:, :128].reshape(16, 16, 128)
            e[side, 32 * g + 16 : 32 * g + 32] = z[:, 128:].reshape(16, 16, 128)

    def first_edge(s):
        nb = norm_last(tile_of(x_ref, s)).astype(BF16)
        n[s] = nb
        edge(1, s, nb)

    def send_right(a):
        r = lax.rem(row + a, 8)
        for k in range(1 if a == 0 else 0, 16):
            c = lax.rem(col + k, 16)
            push(e.at[1, 16 * r + c], rx.at[1, me], right_send, right_recv, r, c)

    def send_left(a):
        r = lax.rem(row + 8 - a, 8)
        for k in range(1 if a == 0 else 0, 16):
            c = lax.rem(col + k, 16)
            push(e.at[0, 16 * r + c], rx.at[0, me], left_send, left_recv.at[a], r, c)

    loop(0, 16, first_edge, 4)
    order(1)
    for copy in fetch[2:]:
        copy.wait()
    pl.semaphore_wait(bar, 127)
    for q in range(4):
        send_right(2 * q)
        send_right(2 * q + 1)
        for s in range(4 * q, 4 * q + 4):
            edge(0, s, n[s])
    rx[1, me] = e[1, me]
    order(0)
    for q in range(4):
        send_left(2 * q)
        send_left(2 * q + 1)
        for s in range(4 * q, 4 * q + 4):
            gate[s] = jax.nn.sigmoid(dot(n[s], tri_gate_ref[...]))
    rx[0, me] = e[0, me]
    wvt[...] = turned(att_in_ref[:, 256:384])
    wgt[...] = turned(att_in_ref[:, 384:512])

    def assemble(side, r, m, at):
        for cg in range(4):
            tiles = [rx[side, 16 * r + 4 * cg + c] for c in range(4)]
            for b, t in enumerate(block_turn(tiles)):
                m[rows16(at + b), 128 * cg : 128 * cg + 128] = t

    take(rx.at[1, pl.ds(0, 127)], right_recv)
    loop(0, 8, lambda r: assemble(1, r, rm, 4 * r), 4)

    def product(o, first=0):
        r = lax.rem(row + o, 8)
        take(rx.at[0, pl.ds(0, 16 - first)], left_recv.at[o])
        assemble(0, r, lm, 0)
        p = dot(lm[...], rm[...], NT).astype(BF16)
        for cg in range(4):
            tiles = [p[16 * b : 16 * b + 16, 128 * cg : 128 * cg + 128] for b in range(4)]
            for c, t in enumerate(block_turn(tiles)):
                po[16 * r + 4 * cg + c] = t
        for k in range(first, 16):
            c = lax.rem(col + k, 16)
            push(po.at[16 * r + c], px.at[me], prod_send, prod_recv, r, c)

    product(0, 1)
    loop(1, 8, product)
    px[me] = po[me]
    take(px.at[pl.ds(0, 127)], prod_recv)

    zero = jnp.zeros((16, 128), F32)
    total = lax.fori_loop(0, 128, lambda c, a: a + px[c].astype(F32), zero, unroll=16)
    mean = total * (1.0 / 128)

    def square(c, a):
        d = px[c].astype(F32) - mean
        return a + d * d

    scale = lax.rsqrt(lax.fori_loop(0, 128, square, zero, unroll=16) * (1.0 / 128) + 1e-5)

    def normed(g):
        z = ((px[rows16(g)].astype(F32) - mean[None]) * scale[None]).astype(BF16)
        z = dot(perm, z.reshape(256, 128)).astype(BF16)
        np_[:, rows16(g), :] = z.reshape(16, 16, 128)

    loop(0, 8, normed, 4)
    wb = bias_ref[...]

    def send_norm(s):
        @pl.when(s != col)
        def _():
            push(nm.at[s], nx.at[col], norm_send, norm_recv, row, s)

    def middle(q):
        first = 4 * lax.rem(q + 2 - 2 * z_lo, 4)
        for s in [first + k for k in range(4)]:
            u = gate[s] * dot(np_[s], tri_out_ref[...], TN)
            update[s] = u
            nb = norm_last(tile_of(x_ref, s) + u).astype(BF16)
            nm[s] = nb
            yb[pl.ds(s, 4, stride=16), :] = dot(wb, nb, NT)

        @pl.when(q < 2)
        def _():
            for k in range(4):
                s = first + k
                push(nm.at[s], nx.at[col], norm_send, norm_recv, row, s)

    loop(0, 4, middle)
    yt = yb[...].T
    bm[...] = jnp.concatenate([yt[32 * b : 32 * b + 32] for b in range(4)], axis=1).astype(BF16)
    line_of = 64 * core + 8 * row + 4 * z_lo
    mine = line_of + x_at
    for k in range(1, 4):
        c = 8 * z_lo + 2 * lax.rem(x_at + k, 4) + core
        push(bm, bx.at[mine], line_send, line, row, c)
    loop(8 * z_lo, 8 * z_lo + 8, send_norm)
    nx[col] = nm[col]
    bx[mine] = bm[...]
    take(bx.at[pl.ds(0, 3)], line)
    group = bx.at[pl.ds(line_of, 4)]
    for k in range(1, 4):
        z = lax.rem(z_at + k, 4)
        push(group, group, plane_send, plane, 2 * y_at + z // 2, 8 * (z % 2) + 2 * x_at + core)

    def rows_of(o):
        turn = 2 * (x_at % 2)
        back = jnp.where(o < 2, 0, jnp.where(o < 4, 1 + turn, jnp.where(o < 6, 3 - turn, 2)))
        half = lax.rem(o + x_at, 2)
        return 2 * lax.rem(y_at - back + 4, 4) + half, 2 * back + half

    def bias_rows(r):
        return bx.at[pl.ds(64 * core + 8 * r, 8)]

    take(bx.at[pl.ds(0, 12)], plane)
    for o in range(2):
        mine_ = bias_rows(rows_of(o)[0])
        push(mine_, mine_, far_send, far.at[o], row, mate)
    for half in range(2):
        for k in (1, 3):
            mine_ = bias_rows(2 * y_at + half)
            r = 2 * lax.rem(y_at + k, 4) + row % 2
            push(mine_, mine_, near_send, near.at[2 * k + half], r, col)

    kk = lax.broadcasted_iota(jnp.int32, (512, 256), 0)
    mask = jnp.where(kk < length, 0.0, -1e9).astype(F32).reshape(8, 2, 32, 256)
    take(nx.at[pl.ds(0, 15)], norm_recv)

    def project(c):
        nb = nx[c]
        qk = dot(nb, att_in_ref[:, :256])
        qs[c] = (qk[:, :128] * 32 ** (-0.5)).astype(BF16)
        ks[c] = qk[:, 128:].astype(BF16)
        gt[c] = jax.nn.sigmoid(dot(wgt[...], nb, NT))

    loop(0, 16, project, 4)
    for b in range(4):
        vt[b, :128] = dot(wvt[...], nx[:, 32 * b : 32 * b + 32, :].reshape(512, 128), NT).astype(BF16)
        vt[b, 128:] = jnp.ones((16, 512), BF16)
    tile[...] = jnp.zeros((2, 128, 128), F32)

    def block(o):
        r = rows_of(o)[0]

        @pl.when((o > 0) & (o < 7))
        def _():
            later, slot = rows_of(o + 1)
            rows = bias_rows(later)
            take(bx.at[pl.ds(0, 8)], near.at[slot])
            push(rows, rows, far_send, far.at[o + 1], row, mate)
            for k, half in ((1, 0), (3, 1)):

                @pl.when(slot == 2 * k + half)
                def _():
                    to = 2 * lax.rem(y_at + k, 4) + row % 2
                    push(rows, rows, near_send, near.at[4 + half], to, col)

        take(bx.at[pl.ds(0, 8)], far.at[o])
        for k in range(2):
            got = bx[pl.ds(pl.multiple_of(64 * k + 8 * r, 8), 8)].astype(F32)
            bias[:, k] = (got + mask[:, k]) * LOG2E

        def score(b):
            q = qs[pl.ds(2 * r, 2), 32 * b : 32 * b + 32, :].reshape(4, 1, 16, 128)
            hd = lax.broadcasted_iota(jnp.int32, (4, 4, 16, 128), 1)
            ln = lax.broadcasted_iota(jnp.int32, (4, 4, 16, 128), 3)
            qm = jnp.where(
                hd == ln // 32, jnp.broadcast_to(q, (4, 4, 16, 128)).astype(F32), 0.0
            ).astype(BF16)
            keys = ks[:, 32 * b : 32 * b + 32, :].reshape(512, 128)
            st = dot(keys, qm.reshape(256, 128), NT) * LOG2E + bias[...].reshape(512, 256)
            scores[b] = st
            return jnp.max(st, axis=0, keepdims=True)

        top = score(0)
        for b in range(4):
            later_top = score(b + 1) if b < 3 else None
            ot = dot(vt[b], jnp.exp2(scores[b] - top).astype(BF16))
            ot = ot[:128] * (1.0 / ot[128:129])
            for h in range(4):
                part = ot[32 * h : 32 * h + 32]
                for j in range(4):
                    at = 64 * (j % 2) + 16 * h
                    to = 32 * b + 16 * (j % 2)
                    moved = part[:, 128 * (j // 2) : 128 * (j // 2) + 128]
                    if (to - at) % 128:
                        moved = pltpu.roll(moved, (to - at) % 128, 1)
                    here = (lane128 >= to) & (lane128 < to + 16)
                    rows = slice(32 * h, 32 * h + 32)
                    tile[j // 2, rows] = jnp.where(here, moved, tile[j // 2, rows])
            top = later_top
        for k in range(2):
            c = 2 * r + k
            go[c] = (tile[k] * gt[c]).astype(BF16)
        for k in range(2):
            c = 2 * r + k

            @pl.when(c != col)
            def _():
                push(go.at[c], gx.at[col], back_send, back_recv, row, c)

    loop(0, 8, block)
    gx[col] = go[col]
    take(gx.at[pl.ds(0, 15)], back_recv)

    for g in range(4):
        for s in range(4 * g, 4 * g + 4):
            t = update[s] + dot(gx[s], att_out_ref[...], TN)
            for b in range(4):
                out[b, s] = t[32 * b : 32 * b + 32]
    take(rx.at[0, pl.ds(0, 127)], right_send)
    take(rx.at[0, pl.ds(0, 127)], left_send)
    take(px.at[pl.ds(0, 127)], prod_send)
    take(nx.at[pl.ds(0, 15)], norm_send)
    take(bx.at[pl.ds(0, 3)], line_send)
    take(bx.at[pl.ds(0, 12)], plane_send)
    take(bx.at[pl.ds(0, 48)], near_send)
    take(bx.at[pl.ds(0, 64)], far_send)
    take(go.at[pl.ds(0, 15)], back_send)


SCRATCH = [
    ((64, 32, 128), F32),
    ((128, 512), BF16),
    ((128, 128), BF16),
    ((128, 128), BF16),
    ((4, 128), BF16),
    ((128, 512), BF16),
    ((128, 128), BF16),
    ((16, 128, 128), BF16),
    ((16, 128, 128), F32),
    ((512, 128), BF16),
    ((128, 128), BF16),
    ((128, 128), BF16),
    ((4, 256, 256), BF16),
    ((2, 128, 16, 128), BF16),
    ((2, 128, 16, 128), BF16),
    ((16, 128, 128), BF16),
    ((64, 512), BF16),
    ((512, 512), BF16),
    ((128, 16, 128), BF16),
    ((128, 16, 128), BF16),
    ((16, 128, 128), F32),
    ((16, 128, 128), BF16),
    ((64, 128), F32),
    ((16, 128, 128), BF16),
    ((16, 128, 128), BF16),
    ((32, 256), BF16),
    ((128, 32, 256), BF16),
    ((16, 128, 128), BF16),
    ((16, 128, 128), BF16),
    ((4, 144, 512), BF16),
    ((16, 128, 128), F32),
    ((8, 2, 32, 256), F32),
    ((4, 512, 256), F32),
    ((2, 128, 128), F32),
    ((16, 128, 128), BF16),
]
SEMAPHORES = [(7,), (), (), (), (8,), (), (), (), (), (), (), (), (), (), (8,), (), (8,), (), ()]


def per_device(pair, valid_length, tri_in, tri_gate, tri_out, att_in, att_bias, att_out):
    vmem = pl.BlockSpec(memory_space=pltpu.VMEM)
    smem = pl.BlockSpec(memory_space=pltpu.SMEM)
    hbm = pl.BlockSpec(memory_space=pltpu.HBM)
    change = pl.pallas_call(
        kernel,
        out_shape=jax.ShapeDtypeStruct((4, 16, 32, 128), F32),
        in_specs=[hbm, smem] + [hbm] * 6,
        out_specs=vmem,
        scratch_shapes=[pltpu.VMEM(*s) for s in SCRATCH]
        + [pltpu.SemaphoreType.DMA(s) for s in SEMAPHORES],
        compiler_params=pltpu.CompilerParams(
            collective_id=0, has_side_effects=True, vmem_limit_bytes=40 * 1024 * 1024
        ),
    )(*[a if n == 1 else pltpu.with_memory_space_constraint(a, pltpu.HBM) for n, a in enumerate((pair, valid_length, tri_in, tri_gate, tri_out, att_bias.T, att_in, att_out))])
    return pair + change.reshape(64, 32, 128)


def solution(mesh):
    placed = (P("row", "col", None), P(), P(), P(), P(), P(), P(), P())
    return jax.shard_map(
        per_device, mesh=mesh, in_specs=placed, out_specs=P("row", "col", None), check_vma=False
    )
```

```python
import jax
import jax.numpy as jnp
from jax import lax
from jax.experimental import pallas as pl
from jax.experimental.pallas import tpu as pltpu
from jax.sharding import PartitionSpec as P

MESH = pl.DeviceIdType.MESH
LOG2E = 1.4426950408889634
F32 = jnp.float32
BF16 = jnp.bfloat16
NT = (((1,), (1,)), ((), ()))
TN = (((0,), (0,)), ((), ()))
NN = (((1,), (0,)), ((), ()))


def dot(a, b, dims=NN):
    return lax.dot_general(a, b, dims, preferred_element_type=F32)


def norm_last(x):
    c = x - jnp.mean(x, axis=-1, keepdims=True)
    return c * lax.rsqrt(jnp.mean(c * c, axis=-1, keepdims=True) + 1e-5)


def turned(w):
    return w.astype(F32).T.astype(BF16)


def swap16():
    p = lax.broadcasted_iota(jnp.int32, (256, 256), 0)
    q = lax.broadcasted_iota(jnp.int32, (256, 256), 1)
    return (q == (p % 16) * 16 + p // 16).astype(F32).astype(BF16)


def block_turn(tiles):
    return [
        jnp.concatenate([t[:, 32 * b : 32 * b + 32] for t in tiles], axis=1) for b in range(4)
    ]


def tile_of(x_ref, s):
    return jnp.concatenate([x_ref[16 * b + s] for b in range(4)], axis=0)


def rows16(start):
    return pl.ds(pl.multiple_of(16 * start, 16), 16)


def loop(low, high, body, unroll=1):
    def step(n, carry):
        body(n)
        return carry

    lax.fori_loop(low, high, step, 0, unroll=unroll)


def push(src, dst, send_sem, recv_sem, row, col):
    pltpu.make_async_remote_copy(src, dst, send_sem, recv_sem, (row, col), MESH).start()


def take(ref, sem):
    pltpu.make_async_copy(ref, ref, sem).wait()


def kernel(
    x_hbm, len_ref, tri_in_hbm, tri_gate_hbm, tri_out_hbm, bias_hbm, att_in_hbm, att_out_hbm, out,
    x_ref, tri_in_ref, tri_gate_ref, tri_out_ref, bias_ref, att_in_ref, att_out_ref, gx, update, wt, wvt, wgt, y, e, rx, n, lm, rm, po, px, gate, np_, yb, nm, nx, bm, bx,
    qs, ks, vt, gt, bias, scores, tile, go,
    load, right_send, right_recv, left_send, left_recv, prod_send, prod_recv, norm_send, norm_recv,
    line_send, line, plane_send, plane, early_send, early, near_send, near, far_send, far, back_send, back_recv,
):
    row, col = lax.axis_index("row"), lax.axis_index("col")
    me = 16 * row + col
    chip, core = col // 2, col % 2
    z_lo, x_at = chip // 4, chip % 4
    y_at, z_at = row // 2, 2 * (row % 2) + z_lo
    mate = col + 1 - 2 * core
    bar = pltpu.get_barrier_semaphore()
    pairs = (
        (tri_in_hbm, tri_in_ref), (x_hbm, x_ref), (tri_gate_hbm, tri_gate_ref), (att_in_hbm, att_in_ref),
        (tri_out_hbm, tri_out_ref), (bias_hbm, bias_ref), (att_out_hbm, att_out_ref),
    )
    fetch = [pltpu.make_async_copy(a, b, load.at[n]) for n, (a, b) in enumerate(pairs)]
    for copy in fetch:
        copy.start()

    def greet(r, first=0):
        for k in range(first, 16):
            c = lax.rem(col + k, 16)
            pl.semaphore_signal(bar, inc=1, device_id=(r, c), device_id_type=MESH)

    greet(row, 1)
    loop(1, 8, lambda a: greet(lax.rem(row + a, 8)))
    fetch[0].wait()
    wt[...] = turned(tri_in_ref[...])
    perm = swap16()
    lane128 = lax.broadcasted_iota(jnp.int32, (1, 128), 1)
    length = len_ref[0]
    keep_k = (32 * col + lane128 % 32) < length
    fetch[1].wait()

    def edge(side, s, nb):
        pt = dot(wt[256 * side : 256 * side + 256], nb, NT)
        w = jnp.where(keep_k & ((64 * row + (lane128 // 32) * 16 + s) < length), 1.0, 0.0)
        v = (jax.nn.sigmoid(pt[:128]) * pt[128:] * w).astype(BF16)
        for g in range(8):
            at = slice(128 * (g % 2), 128 * (g % 2) + 128)
            y[g // 2, rows16(s), at] = v[16 * g : 16 * g + 16]

    def order(side):
        for g in range(4):
            z = dot(perm, y[g]).astype(BF16)
            e[side, 32 * g : 32 * g + 16] = z[:, :128].reshape(16, 16, 128)
            e[side, 32 * g + 16 : 32 * g + 32] = z[:, 128:].reshape(16, 16, 128)

    def first_edge(s):
        edge(1, s, n[s])

    def send_right(a):
        r = lax.rem(row + a, 8)
        for k in range(1 if a == 0 else 0, 16):
            c = lax.rem(col + k, 16)
            push(e.at[1, 16 * r + c], rx.at[1, me], right_send, right_recv, r, c)

    def send_left(a):
        r = lax.rem(row + 8 - a, 8)
        for k in range(1 if a == 0 else 0, 16):
            c = lax.rem(col + k, 16)
            push(e.at[0, 16 * r + c], rx.at[0, me], left_send, left_recv.at[a], r, c)

    def first_norm(q):
        rows = jnp.concatenate([tile_of(x_ref, 4 * q + k) for k in range(4)], axis=0)
        n[pl.ds(pl.multiple_of(4 * q, 4), 4)] = norm_last(rows).astype(BF16).reshape(4, 128, 128)

    loop(0, 4, first_norm, 4)
    loop(0, 16, first_edge, 4)
    order(1)
    for copy in fetch[2:]:
        copy.wait()
    pl.semaphore_wait(bar, 127)
    for q in range(4):
        send_right(2 * q)
        send_right(2 * q + 1)
        for s in range(4 * q, 4 * q + 4):
            edge(0, s, n[s])
    rx[1, me] = e[1, me]
    order(0)
    for q in range(4):
        send_left(2 * q)
        send_left(2 * q + 1)
        for s in range(4 * q, 4 * q + 4):
            gate[s] = jax.nn.sigmoid(dot(n[s], tri_gate_ref[...]))
    rx[0, me] = e[0, me]
    wvt[...] = turned(att_in_ref[:, 256:384])
    wgt[...] = turned(att_in_ref[:, 384:512])

    def assemble(side, r, m, at):
        for cg in range(4):
            tiles = [rx[side, 16 * r + 4 * cg + c] for c in range(4)]
            for b, t in enumerate(block_turn(tiles)):
                m[rows16(at + b), 128 * cg : 128 * cg + 128] = t

    take(rx.at[1, pl.ds(0, 127)], right_recv)
    loop(0, 8, lambda r: assemble(1, r, rm, 4 * r), 4)

    def product(o, first=0):
        r = lax.rem(row + o, 8)
        take(rx.at[0, pl.ds(0, 16 - first)], left_recv.at[o])
        assemble(0, r, lm, 0)
        p = dot(lm[...], rm[...], NT).astype(BF16)
        for cg in range(4):
            tiles = [p[16 * b : 16 * b + 16, 128 * cg : 128 * cg + 128] for b in range(4)]
            for c, t in enumerate(block_turn(tiles)):
                po[16 * r + 4 * cg + c] = t
        for k in range(first, 16):
            c = lax.rem(col + k, 16)
            push(po.at[16 * r + c], px.at[me], prod_send, prod_recv, r, c)

    product(0, 1)
    loop(1, 8, product)
    px[me] = po[me]
    take(px.at[pl.ds(0, 127)], prod_recv)

    zero = jnp.zeros((16, 128), F32)
    total = lax.fori_loop(0, 128, lambda c, a: a + px[c].astype(F32), zero, unroll=16)
    mean = total * (1.0 / 128)

    def square(c, a):
        d = px[c].astype(F32) - mean
        return a + d * d

    scale = lax.rsqrt(lax.fori_loop(0, 128, square, zero, unroll=16) * (1.0 / 128) + 1e-5)

    def normed(g):
        z = ((px[rows16(g)].astype(F32) - mean[None]) * scale[None]).astype(BF16)
        z = dot(perm, z.reshape(256, 128)).astype(BF16)
        np_[:, rows16(g), :] = z.reshape(16, 16, 128)

    loop(0, 8, normed, 4)
    wb = bias_ref[...]

    def send_norm(s):
        @pl.when(s != col)
        def _():
            push(nm.at[s], nx.at[col], norm_send, norm_recv, row, s)

    for half in range(2):
        first = 8 * (lax.rem(z_lo + 1, 2) if half == 0 else z_lo)
        for s in [first + k for k in range(8)]:
            u = gate[s] * dot(np_[s], tri_out_ref[...], TN)
            update[s] = u
            gate[s] = tile_of(x_ref, s) + u
        for q in range(2):
            at = pl.ds(pl.multiple_of(first + 4 * q, 4), 4)
            nb = norm_last(gate[at].reshape(512, 128)).astype(BF16)
            nm[at] = nb.reshape(4, 128, 128)
            z = dot(wb, nb, NT)
            for k in range(4):
                yb[pl.ds(first + 4 * q + k, 4, stride=16), :] = z[:, 128 * k : 128 * k + 128]
        for s in [first + k for k in range(8 if half == 0 else 0)]:
            push(nm.at[s], nx.at[col], norm_send, norm_recv, row, s)

    yt = yb[...].T
    bm[...] = jnp.concatenate([yt[32 * b : 32 * b + 32] for b in range(4)], axis=1).astype(BF16)
    line_of = 64 * core + 8 * row + 4 * z_lo
    mine = line_of + x_at
    for k in range(1, 4):
        c = 8 * z_lo + 2 * lax.rem(x_at + k, 4) + core
        push(bm, bx.at[mine], line_send, line, row, c)
    loop(8 * z_lo, 8 * z_lo + 8, send_norm)
    nx[col] = nm[col]
    bx[mine] = bm[...]
    take(bx.at[pl.ds(0, 3)], line)
    z_hi = row % 2
    group = bx.at[pl.ds(line_of, 4)]
    for k in range(1, 4):
        z = lax.rem(z_at + k, 4)
        push(group, group, plane_send, plane, 2 * y_at + z // 2, 8 * (z % 2) + 2 * x_at + core)
    for k in (1, 3, 2):
        push(group, group, early_send, early.at[k], 2 * lax.rem(y_at + k, 4) + z_hi, col)

    def rows_of(o):
        turn = 2 * (x_at % 2)
        late = lax.rem(o + x_at // 2 + 2 * z_lo, 4)
        last = jnp.where(late < 2, 3 - turn, 2)
        back = jnp.where(o < 2, 0, jnp.where(o < 4, 1 + turn, last))
        half = lax.rem(z_hi + jnp.where(o < 4, o, late), 2)
        return 2 * lax.rem(y_at - back + 4, 4) + half, back, half == z_hi

    def bias_rows(r):
        return bx.at[pl.ds(64 * core + 8 * r, 8)]

    take(bx.at[pl.ds(0, 12)], plane)
    for o in range(2):
        mine_ = bias_rows(rows_of(o)[0])
        push(mine_, mine_, far_send, far.at[o], row, mate)
    rest = bx.at[pl.ds(64 * core + 8 * row + 4 - 4 * z_lo, 4)]
    whole = bias_rows(2 * y_at + 1 - z_hi)
    for part in ((1, 3), (2,)):
        for k in part:
            push(rest, rest, near_send, near.at[k], 2 * lax.rem(y_at + k, 4) + z_hi, col)
        for k in part:
            push(whole, whole, near_send, near.at[4 + k], 2 * lax.rem(y_at + k, 4) + z_hi, col)

    kk = lax.broadcasted_iota(jnp.int32, (512, 256), 0)
    mask = jnp.where(kk < length, 0.0, -1e9).astype(F32).reshape(8, 2, 32, 256)
    take(nx.at[pl.ds(0, 15)], norm_recv)

    def project(c):
        nb = nx[c]
        qk = dot(nb, att_in_ref[:, :256])
        qs[c] = (qk[:, :128] * 32 ** (-0.5)).astype(BF16)
        ks[c] = qk[:, 128:].astype(BF16)
        gt[c] = jax.nn.sigmoid(dot(wgt[...], nb, NT))

    loop(0, 16, project, 4)
    for b in range(4):
        vt[b, :128] = dot(wvt[...], nx[:, 32 * b : 32 * b + 32, :].reshape(512, 128), NT).astype(BF16)
        vt[b, 128:] = jnp.ones((16, 512), BF16)
    tile[...] = jnp.zeros((2, 128, 128), F32)

    def block(o):
        r = rows_of(o)[0]

        @pl.when((o > 0) & (o < 7))
        def _():
            later, back, own_half = rows_of(o + 1)
            rows = bias_rows(later)

            @pl.when(own_half)
            def _():
                take(bx.at[pl.ds(0, 4)], early.at[back])
                take(bx.at[pl.ds(0, 4)], near.at[back])

            @pl.when(jnp.logical_not(own_half))
            def _():
                take(bx.at[pl.ds(0, 8)], near.at[4 + back])

            push(rows, rows, far_send, far.at[o + 1], row, mate)

        take(bx.at[pl.ds(0, 8)], far.at[o])
        for k in range(2):
            got = bx[pl.ds(pl.multiple_of(64 * k + 8 * r, 8), 8)].astype(F32)
            bias[:, k] = (got + mask[:, k]) * LOG2E

        def score(b):
            q = qs[pl.ds(2 * r, 2), 32 * b : 32 * b + 32, :].reshape(4, 1, 16, 128)
            hd = lax.broadcasted_iota(jnp.int32, (4, 4, 16, 128), 1)
            ln = lax.broadcasted_iota(jnp.int32, (4, 4, 16, 128), 3)
            qm = jnp.where(
                hd == ln // 32, jnp.broadcast_to(q, (4, 4, 16, 128)).astype(F32), 0.0
            ).astype(BF16)
            keys = ks[:, 32 * b : 32 * b + 32, :].reshape(512, 128)
            st = dot(keys, qm.reshape(256, 128), NT) * LOG2E + bias[...].reshape(512, 256)
            scores[b] = st
            return jnp.max(st, axis=0, keepdims=True)

        top = score(0)
        for b in range(4):
            later_top = score(b + 1) if b < 3 else None
            ot = dot(vt[b], jnp.exp2(scores[b] - top).astype(BF16))
            ot = ot[:128] * (1.0 / ot[128:129])
            for h in range(4):
                part = ot[32 * h : 32 * h + 32]
                for j in range(4):
                    at = 64 * (j % 2) + 16 * h
                    to = 32 * b + 16 * (j % 2)
                    moved = part[:, 128 * (j // 2) : 128 * (j // 2) + 128]
                    if (to - at) % 128:
                        moved = pltpu.roll(moved, (to - at) % 128, 1)
                    here = (lane128 >= to) & (lane128 < to + 16)
                    rows = slice(32 * h, 32 * h + 32)
                    tile[j // 2, rows] = jnp.where(here, moved, tile[j // 2, rows])
            top = later_top
        for k in range(2):
            c = 2 * r + k
            go[c] = (tile[k] * gt[c]).astype(BF16)
        for k in range(2):
            c = 2 * r + k

            @pl.when(c != col)
            def _():
                push(go.at[c], gx.at[col], back_send, back_recv, row, c)

    loop(0, 8, block)
    gx[col] = go[col]
    take(gx.at[pl.ds(0, 15)], back_recv)

    for g in range(4):
        for s in range(4 * g, 4 * g + 4):
            t = update[s] + dot(gx[s], att_out_ref[...], TN)
            for b in range(4):
                out[b, s] = t[32 * b : 32 * b + 32]
    take(rx.at[0, pl.ds(0, 127)], right_send)
    take(rx.at[0, pl.ds(0, 127)], left_send)
    take(px.at[pl.ds(0, 127)], prod_send)
    take(nx.at[pl.ds(0, 15)], norm_send)
    take(bx.at[pl.ds(0, 3)], line_send)
    take(bx.at[pl.ds(0, 12)], plane_send)
    take(bx.at[pl.ds(0, 12)], early_send)
    take(bx.at[pl.ds(0, 36)], near_send)
    take(bx.at[pl.ds(0, 64)], far_send)
    take(go.at[pl.ds(0, 15)], back_send)


SCRATCH = [
    ((64, 32, 128), F32),
    ((128, 512), BF16),
    ((128, 128), BF16),
    ((128, 128), BF16),
    ((4, 128), BF16),
    ((128, 512), BF16),
    ((128, 128), BF16),
    ((16, 128, 128), BF16),
    ((16, 128, 128), F32),
    ((512, 128), BF16),
    ((128, 128), BF16),
    ((128, 128), BF16),
    ((4, 256, 256), BF16),
    ((2, 128, 16, 128), BF16),
    ((2, 128, 16, 128), BF16),
    ((16, 128, 128), BF16),
    ((64, 512), BF16),
    ((512, 512), BF16),
    ((128, 16, 128), BF16),
    ((128, 16, 128), BF16),
    ((16, 128, 128), F32),
    ((16, 128, 128), BF16),
    ((64, 128), F32),
    ((16, 128, 128), BF16),
    ((16, 128, 128), BF16),
    ((32, 256), BF16),
    ((128, 32, 256), BF16),
    ((16, 128, 128), BF16),
    ((16, 128, 128), BF16),
    ((4, 144, 512), BF16),
    ((16, 128, 128), F32),
    ((8, 2, 32, 256), F32),
    ((4, 512, 256), F32),
    ((2, 128, 128), F32),
    ((16, 128, 128), BF16),
]
SEMAPHORES = [
    (7,), (), (), (), (8,), (), (), (), (), (), (), (), (), (), (4,), (), (8,), (), (8,), (), (),
]


def per_device(pair, valid_length, tri_in, tri_gate, tri_out, att_in, att_bias, att_out):
    vmem = pl.BlockSpec(memory_space=pltpu.VMEM)
    smem = pl.BlockSpec(memory_space=pltpu.SMEM)
    hbm = pl.BlockSpec(memory_space=pltpu.HBM)
    change = pl.pallas_call(
        kernel,
        out_shape=jax.ShapeDtypeStruct((4, 16, 32, 128), F32),
        in_specs=[hbm, smem] + [hbm] * 6,
        out_specs=vmem,
        scratch_shapes=[pltpu.VMEM(*s) for s in SCRATCH]
        + [pltpu.SemaphoreType.DMA(s) for s in SEMAPHORES],
        compiler_params=pltpu.CompilerParams(
            collective_id=0, has_side_effects=True, vmem_limit_bytes=40 * 1024 * 1024
        ),
    )(*[a if n == 1 else pltpu.with_memory_space_constraint(a, pltpu.HBM) for n, a in enumerate((pair, valid_length, tri_in, tri_gate, tri_out, att_bias.T, att_in, att_out))])
    return pair + change.reshape(64, 32, 128)


def solution(mesh):
    placed = (P("row", "col", None), P(), P(), P(), P(), P(), P(), P())
    return jax.shard_map(
        per_device, mesh=mesh, in_specs=placed, out_specs=P("row", "col", None), check_vma=False
    )
```

```python
import jax
import jax.numpy as jnp
from jax import lax
from jax.experimental import pallas as pl
from jax.experimental.pallas import tpu as pltpu
from jax.sharding import PartitionSpec as P

MESH = pl.DeviceIdType.MESH
LOG2E = 1.4426950408889634
F32 = jnp.float32
BF16 = jnp.bfloat16
NT = (((1,), (1,)), ((), ()))
TN = (((0,), (0,)), ((), ()))
NN = (((1,), (0,)), ((), ()))


def dot(a, b, dims=NN):
    return lax.dot_general(a, b, dims, preferred_element_type=F32)


def norm_last(x):
    c = x - jnp.mean(x, axis=-1, keepdims=True)
    return c * lax.rsqrt(jnp.mean(c * c, axis=-1, keepdims=True) + 1e-5)


def turned(w):
    return w.astype(F32).T.astype(BF16)


def swap16():
    p = lax.broadcasted_iota(jnp.int32, (256, 256), 0)
    q = lax.broadcasted_iota(jnp.int32, (256, 256), 1)
    return (q == (p % 16) * 16 + p // 16).astype(F32).astype(BF16)


def block_turn(tiles):
    return [
        jnp.concatenate([t[:, 32 * b : 32 * b + 32] for t in tiles], axis=1) for b in range(4)
    ]


def tile_of(x_ref, s):
    return jnp.concatenate([x_ref[16 * b + s] for b in range(4)], axis=0)


def rows16(start):
    return pl.ds(pl.multiple_of(16 * start, 16), 16)


def loop(low, high, body, unroll=1):
    def step(n, carry):
        body(n)
        return carry

    lax.fori_loop(low, high, step, 0, unroll=unroll)


def push(src, dst, send_sem, recv_sem, row, col):
    pltpu.make_async_remote_copy(src, dst, send_sem, recv_sem, (row, col), MESH).start()


def take(ref, sem):
    pltpu.make_async_copy(ref, ref, sem).wait()


def kernel(
    x_hbm, len_ref, tri_in_hbm, tri_gate_hbm, tri_out_hbm, bias_hbm, att_in_hbm, att_out_hbm, out,
    x_ref, tri_in_ref, tri_gate_ref, tri_out_ref, bias_ref, att_in_ref, att_out_ref, gx, update, wt, wvt, wgt, y, e, rx, n, lm, rm, po, px, gate, np_, yb, nm, nx, bm, bx,
    qs, ks, vt, gt, bias, scores, tile, go,
    load, right_send, right_recv, left_send, left_recv, prod_send, prod_recv, norm_send, norm_recv,
    line_send, line, plane_send, plane, early_send, early, near_send, near, far_send, far, back_send, back_recv,
):
    row, col = lax.axis_index("row"), lax.axis_index("col")
    me = 16 * row + col
    chip, core = col // 2, col % 2
    z_lo, x_at = chip // 4, chip % 4
    y_at, z_at = row // 2, 2 * (row % 2) + z_lo
    mate = col + 1 - 2 * core
    bar = pltpu.get_barrier_semaphore()
    pairs = (
        (tri_in_hbm, tri_in_ref), (x_hbm, x_ref), (tri_gate_hbm, tri_gate_ref), (att_in_hbm, att_in_ref),
        (tri_out_hbm, tri_out_ref), (bias_hbm, bias_ref), (att_out_hbm, att_out_ref),
    )
    fetch = [pltpu.make_async_copy(a, b, load.at[n]) for n, (a, b) in enumerate(pairs)]
    for copy in fetch:
        copy.start()

    def greet(r, first=0):
        for k in range(first, 16):
            c = lax.rem(col + k, 16)
            pl.semaphore_signal(bar, inc=1, device_id=(r, c), device_id_type=MESH)

    greet(row, 1)
    loop(1, 8, lambda a: greet(lax.rem(row + a, 8)))
    fetch[0].wait()
    wt[...] = turned(tri_in_ref[...])
    perm = swap16()
    lane128 = lax.broadcasted_iota(jnp.int32, (1, 128), 1)
    length = len_ref[0]
    keep_k = (32 * col + lane128 % 32) < length
    fetch[1].wait()

    def edge(side, s, nb):
        pt = dot(wt[256 * side : 256 * side + 256], nb, NT)
        w = jnp.where(keep_k & ((64 * row + (lane128 // 32) * 16 + s) < length), 1.0, 0.0)
        v = (jax.nn.sigmoid(pt[:128]) * pt[128:] * w).astype(BF16)
        for g in range(8):
            at = slice(128 * (g % 2), 128 * (g % 2) + 128)
            y[g // 2, rows16(s), at] = v[16 * g : 16 * g + 16]

    def order(side):
        for g in range(4):
            z = dot(perm, y[g]).astype(BF16)
            e[side, 32 * g : 32 * g + 16] = z[:, :128].reshape(16, 16, 128)
            e[side, 32 * g + 16 : 32 * g + 32] = z[:, 128:].reshape(16, 16, 128)

    def first_edge(s):
        edge(1, s, n[s])

    def send_right(a):
        r = lax.rem(row + a, 8)
        for k in range(1 if a == 0 else 0, 16):
            c = lax.rem(col + k, 16)
            push(e.at[1, 16 * r + c], rx.at[1, me], right_send, right_recv, r, c)

    def send_left(a):
        r = lax.rem(row + 8 - a, 8)
        for k in range(1 if a == 0 else 0, 16):
            c = lax.rem(col + k, 16)
            push(e.at[0, 16 * r + c], rx.at[0, me], left_send, left_recv.at[a], r, c)

    def first_norm(q):
        rows = jnp.concatenate([tile_of(x_ref, 4 * q + k) for k in range(4)], axis=0)
        n[pl.ds(pl.multiple_of(4 * q, 4), 4)] = norm_last(rows).astype(BF16).reshape(4, 128, 128)

    loop(0, 4, first_norm, 4)
    loop(0, 16, first_edge, 4)
    order(1)
    for copy in fetch[2:]:
        copy.wait()
    pl.semaphore_wait(bar, 127)
    for q in range(4):
        send_right(2 * q)
        send_right(2 * q + 1)
        for s in range(4 * q, 4 * q + 4):
            edge(0, s, n[s])
    rx[1, me] = e[1, me]
    order(0)
    for q in range(4):
        send_left(2 * q)
        send_left(2 * q + 1)
        for s in range(4 * q, 4 * q + 4):
            gate[s] = jax.nn.sigmoid(dot(n[s], tri_gate_ref[...]))
    rx[0, me] = e[0, me]
    wvt[...] = turned(att_in_ref[:, 256:384])
    wgt[...] = turned(att_in_ref[:, 384:512])

    def assemble(side, r, m, at):
        for cg in range(4):
            tiles = [rx[side, 16 * r + 4 * cg + c] for c in range(4)]
            for b, t in enumerate(block_turn(tiles)):
                m[rows16(at + b), 128 * cg : 128 * cg + 128] = t

    take(rx.at[1, pl.ds(0, 127)], right_recv)
    loop(0, 8, lambda r: assemble(1, r, rm, 4 * r), 4)

    def product(o, first=0):
        r = lax.rem(row + o, 8)
        take(rx.at[0, pl.ds(0, 16 - first)], left_recv.at[o])
        assemble(0, r, lm, 0)
        p = dot(lm[...], rm[...], NT).astype(BF16)
        for cg in range(4):
            tiles = [p[16 * b : 16 * b + 16, 128 * cg : 128 * cg + 128] for b in range(4)]
            for c, t in enumerate(block_turn(tiles)):
                po[16 * r + 4 * cg + c] = t
        for k in range(first, 16):
            c = lax.rem(col + k, 16)
            push(po.at[16 * r + c], px.at[me], prod_send, prod_recv, r, c)

    product(0, 1)
    loop(1, 8, product)
    px[me] = po[me]
    take(px.at[pl.ds(0, 127)], prod_recv)

    zero = jnp.zeros((16, 128), F32)
    total = lax.fori_loop(0, 128, lambda c, a: a + px[c].astype(F32), zero, unroll=16)
    mean = total * (1.0 / 128)

    def square(c, a):
        d = px[c].astype(F32) - mean
        return a + d * d

    scale = lax.rsqrt(lax.fori_loop(0, 128, square, zero, unroll=16) * (1.0 / 128) + 1e-5)

    def normed(g):
        z = ((px[rows16(g)].astype(F32) - mean[None]) * scale[None]).astype(BF16)
        z = dot(perm, z.reshape(256, 128)).astype(BF16)
        np_[:, rows16(g), :] = z.reshape(16, 16, 128)

    loop(0, 8, normed, 4)
    wb = bias_ref[...]

    def send_norm(s):
        @pl.when(s != col)
        def _():
            push(nm.at[s], nx.at[col], norm_send, norm_recv, row, s)

    for half in range(2):
        first = 8 * (lax.rem(z_lo + 1, 2) if half == 0 else z_lo)
        for s in [first + k for k in range(8)]:
            u = gate[s] * dot(np_[s], tri_out_ref[...], TN)
            update[s] = u
            gate[s] = tile_of(x_ref, s) + u
        for q in range(2):
            at = pl.ds(pl.multiple_of(first + 4 * q, 4), 4)
            nb = norm_last(gate[at].reshape(512, 128)).astype(BF16)
            nm[at] = nb.reshape(4, 128, 128)
            z = dot(wb, nb, NT)
            for k in range(4):
                yb[pl.ds(first + 4 * q + k, 4, stride=16), :] = z[:, 128 * k : 128 * k + 128]
        for s in [first + k for k in range(8 if half == 0 else 0)]:
            push(nm.at[s], nx.at[col], norm_send, norm_recv, row, s)

    yt = yb[...].T
    own_keys = lax.broadcasted_iota(jnp.int32, (32, 256), 0) + 32 * col
    yt = jnp.concatenate([yt[32 * b : 32 * b + 32] for b in range(4)], axis=1)
    bm[...] = jnp.where(own_keys < length, yt, -1e9).astype(BF16)
    line_of = 64 * core + 8 * row + 4 * z_lo
    mine = line_of + x_at
    for k in range(1, 4):
        c = 8 * z_lo + 2 * lax.rem(x_at + k, 4) + core
        push(bm, bx.at[mine], line_send, line, row, c)
    loop(8 * z_lo, 8 * z_lo + 8, send_norm)
    nx[col] = nm[col]
    bx[mine] = bm[...]
    take(bx.at[pl.ds(0, 3)], line)
    z_hi = row % 2
    group = bx.at[pl.ds(line_of, 4)]
    for k in range(1, 4):
        z = lax.rem(z_at + k, 4)
        push(group, group, plane_send, plane.at[jnp.where(z // 2 == z_hi, 0, 1)], 2 * y_at + z // 2, 8 * (z % 2) + 2 * x_at + core)
    for k in (1, 3, 2):
        push(group, group, early_send, early.at[k], 2 * lax.rem(y_at + k, 4) + z_hi, col)

    turn = 2 * (x_at % 2)
    shift = x_at // 2 + 2 * z_lo

    def listed(o):
        late = lax.rem(o + shift, 4)
        last = jnp.where(late < 2, 3 - turn, 2)
        back = jnp.where(o < 2, 0, jnp.where(o < 4, 1 + turn, last))
        half = lax.rem(z_hi + jnp.where(o < 4, o, late), 2)
        return 2 * lax.rem(y_at - back + 4, 4) + half, back, half == z_hi

    put_off = jnp.where(chip // 2 == y_at, lax.rem(chip + 4, 8), chip)
    far_back = lax.rem(y_at - put_off // 2 + 4, 4)
    other = jnp.where(put_off % 2 == z_hi, 0, 1)
    place = jnp.where(
        far_back == 1 + turn,
        2 + other,
        4 + lax.rem(other + jnp.where(far_back == 2, 2, 0) - shift + 4, 4),
    )

    def rows_of(o):
        return listed(jnp.where(o == 7, place, o + jnp.where(o < place, 0, 1)))

    def bias_rows(r):
        return bx.at[pl.ds(64 * core + 8 * r, 8)]

    take(bx.at[pl.ds(0, 4)], plane.at[0])
    rest = bx.at[pl.ds(64 * core + 8 * row + 4 - 4 * z_lo, 4)]
    own_row, other_row = bias_rows(row), bias_rows(2 * y_at + 1 - z_hi)
    push(own_row, own_row, far_send, far.at[0], row, mate)
    for k in (1, 3, 2):
        push(rest, rest, near_send, near.at[k], 2 * lax.rem(y_at + k, 4) + z_hi, col)

    take(bx.at[pl.ds(0, 8)], plane.at[1])
    push(other_row, other_row, far_send, far.at[1], row, mate)
    for k in (1, 3, 2):
        push(other_row, other_row, near_send, near.at[4 + k], 2 * lax.rem(y_at + k, 4) + z_hi, col)

    take(nx.at[pl.ds(0, 15)], norm_recv)

    def project(c):
        nb = nx[c]
        qk = dot(nb, att_in_ref[:, :256])
        qs[c] = (qk[:, :128] * 32 ** (-0.5)).astype(BF16)
        ks[c] = qk[:, 128:].astype(BF16)
        gt[c] = jax.nn.sigmoid(dot(wgt[...], nb, NT))

    loop(0, 16, project, 4)
    for b in range(4):
        vt[b, :128] = dot(wvt[...], nx[:, 32 * b : 32 * b + 32, :].reshape(512, 128), NT).astype(BF16)
        vt[b, 128:] = jnp.ones((16, 512), BF16)

    tile[...] = jnp.zeros((2, 128, 128), F32)

    def block(o):
        r = rows_of(o)[0]

        @pl.when((o > 0) & (o < 7))
        def _():
            later, back, own_half = rows_of(o + 1)
            rows = bias_rows(later)

            @pl.when(own_half)
            def _():
                take(bx.at[pl.ds(0, 4)], early.at[back])
                take(bx.at[pl.ds(0, 4)], near.at[back])

            @pl.when(jnp.logical_not(own_half))
            def _():
                take(bx.at[pl.ds(0, 8)], near.at[4 + back])

            push(rows, rows, far_send, far.at[o + 1], row, mate)

        take(bx.at[pl.ds(0, 8)], far.at[o])
        for k in range(2):
            got = bx[pl.ds(pl.multiple_of(64 * k + 8 * r, 8), 8)].astype(F32)
            bias[:, k] = got * LOG2E

        def score(b):
            q = qs[pl.ds(2 * r, 2), 32 * b : 32 * b + 32, :].reshape(4, 1, 16, 128)
            hd = lax.broadcasted_iota(jnp.int32, (4, 4, 16, 128), 1)
            ln = lax.broadcasted_iota(jnp.int32, (4, 4, 16, 128), 3)
            qm = jnp.where(
                hd == ln // 32, jnp.broadcast_to(q, (4, 4, 16, 128)).astype(F32), 0.0
            ).astype(BF16)
            keys = ks[:, 32 * b : 32 * b + 32, :].reshape(512, 128)
            st = dot(keys, qm.reshape(256, 128), NT) * LOG2E + bias[...].reshape(512, 256)
            scores[b] = st
            return jnp.max(st, axis=0, keepdims=True)

        top = score(0)
        for b in range(4):
            later_top = score(b + 1) if b < 3 else None
            ot = dot(vt[b], jnp.exp2(scores[b] - top).astype(BF16))
            ot = ot[:128] * (1.0 / ot[128:129])
            for h in range(4):
                part = ot[32 * h : 32 * h + 32]
                for j in range(4):
                    at = 64 * (j % 2) + 16 * h
                    to = 32 * b + 16 * (j % 2)
                    moved = part[:, 128 * (j // 2) : 128 * (j // 2) + 128]
                    if (to - at) % 128:
                        moved = pltpu.roll(moved, (to - at) % 128, 1)
                    here = (lane128 >= to) & (lane128 < to + 16)
                    rows = slice(32 * h, 32 * h + 32)
                    tile[j // 2, rows] = jnp.where(here, moved, tile[j // 2, rows])
            top = later_top
        for k in range(2):
            c = 2 * r + k
            go[c] = (tile[k] * gt[c]).astype(BF16)
        for k in range(2):
            c = 2 * r + k

            @pl.when(c != col)
            def _():
                push(go.at[c], gx.at[col], back_send, back_recv, row, c)

    loop(0, 8, block)
    gx[col] = go[col]
    take(gx.at[pl.ds(0, 15)], back_recv)

    for g in range(4):
        for s in range(4 * g, 4 * g + 4):
            t = update[s] + dot(gx[s], att_out_ref[...], TN)
            for b in range(4):
                out[b, s] = t[32 * b : 32 * b + 32]
    take(rx.at[0, pl.ds(0, 127)], right_send)
    take(rx.at[0, pl.ds(0, 127)], left_send)
    take(px.at[pl.ds(0, 127)], prod_send)
    take(nx.at[pl.ds(0, 15)], norm_send)
    take(bx.at[pl.ds(0, 3)], line_send)
    take(bx.at[pl.ds(0, 12)], plane_send)
    take(bx.at[pl.ds(0, 12)], early_send)
    take(bx.at[pl.ds(0, 36)], near_send)
    take(bx.at[pl.ds(0, 64)], far_send)
    take(go.at[pl.ds(0, 15)], back_send)


SCRATCH = [
    ((64, 32, 128), F32),
    ((128, 512), BF16),
    ((128, 128), BF16),
    ((128, 128), BF16),
    ((4, 128), BF16),
    ((128, 512), BF16),
    ((128, 128), BF16),
    ((16, 128, 128), BF16),
    ((16, 128, 128), F32),
    ((512, 128), BF16),
    ((128, 128), BF16),
    ((128, 128), BF16),
    ((4, 256, 256), BF16),
    ((2, 128, 16, 128), BF16),
    ((2, 128, 16, 128), BF16),
    ((16, 128, 128), BF16),
    ((64, 512), BF16),
    ((512, 512), BF16),
    ((128, 16, 128), BF16),
    ((128, 16, 128), BF16),
    ((16, 128, 128), F32),
    ((16, 128, 128), BF16),
    ((64, 128), F32),
    ((16, 128, 128), BF16),
    ((16, 128, 128), BF16),
    ((32, 256), BF16),
    ((128, 32, 256), BF16),
    ((16, 128, 128), BF16),
    ((16, 128, 128), BF16),
    ((4, 144, 512), BF16),
    ((16, 128, 128), F32),
    ((8, 2, 32, 256), F32),
    ((4, 512, 256), F32),
    ((2, 128, 128), F32),
    ((16, 128, 128), BF16),
]
SEMAPHORES = [
    (7,), (), (), (), (8,), (), (), (), (), (), (), (), (2,), (), (4,), (), (8,), (), (8,), (), (),
]


def per_device(pair, valid_length, tri_in, tri_gate, tri_out, att_in, att_bias, att_out):
    vmem = pl.BlockSpec(memory_space=pltpu.VMEM)
    smem = pl.BlockSpec(memory_space=pltpu.SMEM)
    hbm = pl.BlockSpec(memory_space=pltpu.HBM)
    change = pl.pallas_call(
        kernel,
        out_shape=jax.ShapeDtypeStruct((4, 16, 32, 128), F32),
        in_specs=[hbm, smem] + [hbm] * 6,
        out_specs=vmem,
        scratch_shapes=[pltpu.VMEM(*s) for s in SCRATCH]
        + [pltpu.SemaphoreType.DMA(s) for s in SEMAPHORES],
        compiler_params=pltpu.CompilerParams(
            collective_id=0, has_side_effects=True, vmem_limit_bytes=40 * 1024 * 1024
        ),
    )(*[a if n == 1 else pltpu.with_memory_space_constraint(a, pltpu.HBM) for n, a in enumerate((pair, valid_length, tri_in, tri_gate, tri_out, att_bias.T, att_in, att_out))])
    return pair + change.reshape(64, 32, 128)


def solution(mesh):
    placed = (P("row", "col", None), P(), P(), P(), P(), P(), P(), P())
    return jax.shard_map(
        per_device, mesh=mesh, in_specs=placed, out_specs=P("row", "col", None), check_vma=False
    )
```

```python
import jax
import jax.numpy as jnp
from jax import lax
from jax.experimental import pallas as pl
from jax.experimental.pallas import tpu as pltpu
from jax.sharding import PartitionSpec as P

MESH = pl.DeviceIdType.MESH
LOG2E = 1.4426950408889634
F32 = jnp.float32
BF16 = jnp.bfloat16
NT = (((1,), (1,)), ((), ()))
TN = (((0,), (0,)), ((), ()))
NN = (((1,), (0,)), ((), ()))


def dot(a, b, dims=NN):
    return lax.dot_general(a, b, dims, preferred_element_type=F32)


def norm_last(x):
    c = x - jnp.mean(x, axis=-1, keepdims=True)
    return c * lax.rsqrt(jnp.mean(c * c, axis=-1, keepdims=True) + 1e-5)


def turned(w):
    return w.astype(F32).T.astype(BF16)


def swap16():
    p = lax.broadcasted_iota(jnp.int32, (256, 256), 0)
    q = lax.broadcasted_iota(jnp.int32, (256, 256), 1)
    return (q == (p % 16) * 16 + p // 16).astype(F32).astype(BF16)


def block_turn(tiles):
    return [
        jnp.concatenate([t[:, 32 * b : 32 * b + 32] for t in tiles], axis=1) for b in range(4)
    ]


def tile_of(x_ref, s):
    return jnp.concatenate([x_ref[16 * b + s] for b in range(4)], axis=0)


def rows16(start):
    return pl.ds(pl.multiple_of(16 * start, 16), 16)


def loop(low, high, body, unroll=1):
    def step(n, carry):
        body(n)
        return carry

    lax.fori_loop(low, high, step, 0, unroll=unroll)


def push(src, dst, send_sem, recv_sem, row, col):
    pltpu.make_async_remote_copy(src, dst, send_sem, recv_sem, (row, col), MESH).start()


def take(ref, sem):
    pltpu.make_async_copy(ref, ref, sem).wait()


def kernel(
    x_hbm, len_ref, tri_in_hbm, tri_gate_hbm, tri_out_hbm, bias_hbm, att_in_hbm, att_out_hbm, out,
    x_ref, tri_in_ref, tri_gate_ref, tri_out_ref, bias_ref, att_in_ref, att_out_ref, gx, update, wt, wvt, wgt, y, e, rx, n, lm, rm, po, px, gate, np_, stats, yb, nm, nx, bm, bx,
    qs, ks, vt, gt, bias, scores, tile, go,
    load, right_send, right_recv, left_send, left_recv, prod_send, prod_recv, norm_send, norm_recv,
    line_send, line, plane_send, plane, early_send, early, near_send, near, far_send, far, back_send, back_recv,
):
    row, col = lax.axis_index("row"), lax.axis_index("col")
    me = 16 * row + col
    chip, core = col // 2, col % 2
    z_lo, x_at = chip // 4, chip % 4
    y_at, z_at = row // 2, 2 * (row % 2) + z_lo
    mate = col + 1 - 2 * core
    bar = pltpu.get_barrier_semaphore()
    pairs = (
        (tri_in_hbm, tri_in_ref), (x_hbm, x_ref), (tri_gate_hbm, tri_gate_ref), (att_in_hbm, att_in_ref),
        (tri_out_hbm, tri_out_ref), (bias_hbm, bias_ref), (att_out_hbm, att_out_ref),
    )
    fetch = [pltpu.make_async_copy(a, b, load.at[n]) for n, (a, b) in enumerate(pairs)]
    for copy in fetch:
        copy.start()

    def greet(r, first=0):
        for k in range(first, 16):
            c = lax.rem(col + k, 16)
            pl.semaphore_signal(bar, inc=1, device_id=(r, c), device_id_type=MESH)

    greet(row, 1)
    loop(1, 8, lambda a: greet(lax.rem(row + a, 8)))
    fetch[0].wait()
    wt[...] = turned(tri_in_ref[...])
    perm = swap16()
    lane128 = lax.broadcasted_iota(jnp.int32, (1, 128), 1)
    length = len_ref[0]
    keep_k = (32 * col + lane128 % 32) < length
    fetch[1].wait()

    def edge(side, s, nb):
        pt = dot(wt[256 * side : 256 * side + 256], nb, NT)
        w = jnp.where(keep_k & ((64 * row + (lane128 // 32) * 16 + s) < length), 1.0, 0.0)
        v = (jax.nn.sigmoid(pt[:128]) * pt[128:] * w).astype(BF16)
        for g in range(8):
            at = slice(128 * (g % 2), 128 * (g % 2) + 128)
            y[g // 2, rows16(s), at] = v[16 * g : 16 * g + 16]

    def order(side):
        for g in range(4):
            z = dot(perm, y[g]).astype(BF16)
            e[side, 32 * g : 32 * g + 16] = z[:, :128].reshape(16, 16, 128)
            e[side, 32 * g + 16 : 32 * g + 32] = z[:, 128:].reshape(16, 16, 128)

    def first_edge(s):
        edge(1, s, n[s])

    def send_right(k):
        c = lax.rem(col + k, 16)
        for a in range(1 if k == 0 else 0, 8):
            r = lax.rem(row + a, 8)
            push(e.at[1, 16 * r + c], rx.at[1, me], right_send, right_recv, r, c)

    def send_left(a):
        r = lax.rem(row + 8 - a, 8)
        for k in range(1 if a == 0 else 0, 16):
            c = lax.rem(col + k, 16)
            push(e.at[0, 16 * r + c], rx.at[0, me], left_send, left_recv.at[a], r, c)

    def first_norm(q):
        rows = jnp.concatenate([tile_of(x_ref, 4 * q + k) for k in range(4)], axis=0)
        n[pl.ds(pl.multiple_of(4 * q, 4), 4)] = norm_last(rows).astype(BF16).reshape(4, 128, 128)

    loop(0, 4, first_norm, 4)
    loop(0, 16, first_edge, 4)
    order(1)
    for copy in fetch[2:]:
        copy.wait()
    pl.semaphore_wait(bar, 127)
    for q in range(4):
        for k in range(4):
            send_right(4 * k + q)
        for s in range(4 * q, 4 * q + 4):
            edge(0, s, n[s])
    rx[1, me] = e[1, me]
    order(0)
    for q in range(4):
        send_left(2 * q)
        send_left(2 * q + 1)
        for s in range(4 * q, 4 * q + 4):
            gate[s] = jax.nn.sigmoid(dot(n[s], tri_gate_ref[...]))
    rx[0, me] = e[0, me]
    wvt[...] = turned(att_in_ref[:, 256:384])
    wgt[...] = turned(att_in_ref[:, 384:512])

    def assemble(side, r, m, at):
        for cg in range(4):
            tiles = [rx[side, 16 * r + 4 * cg + c] for c in range(4)]
            for b, t in enumerate(block_turn(tiles)):
                m[rows16(at + b), 128 * cg : 128 * cg + 128] = t

    take(rx.at[1, pl.ds(0, 127)], right_recv)
    loop(0, 8, lambda r: assemble(1, r, rm, 4 * r), 4)

    def product(o, first=0):
        r = lax.rem(row + o, 8)
        take(rx.at[0, pl.ds(0, 16 - first)], left_recv.at[o])
        assemble(0, r, lm, 0)
        p = dot(lm[...], rm[...], NT).astype(BF16)
        for cg in range(4):
            tiles = [p[16 * b : 16 * b + 16, 128 * cg : 128 * cg + 128] for b in range(4)]
            for c, t in enumerate(block_turn(tiles)):
                po[16 * r + 4 * cg + c] = t
        for k in range(first, 16):
            c = lax.rem(col + k, 16)
            push(po.at[16 * r + c], px.at[me], prod_send, prod_recv.at[o], r, c)

    product(0, 1)
    loop(1, 8, product)
    px[me] = po[me]

    for o in range(8):
        r = lax.rem(row - o + 8, 8)
        take(px.at[pl.ds(0, 15 if o == 0 else 16)], prod_recv.at[o])
        got = px[rows16(r)]
        np_[:, rows16(r), :] = dot(perm, got.reshape(256, 128)).astype(BF16).reshape(16, 16, 128)
        got = got.astype(F32)
        group_mean = jnp.sum(got, axis=0) * (1.0 / 16)
        got = got - group_mean[None]
        squares = jnp.sum(got * got, axis=0)
        if o == 0:
            mean, spread = group_mean, squares
        else:
            step = group_mean - mean
            mean = mean + step * (1.0 / (o + 1))
            spread = spread + squares + step * step * (16.0 * o / (o + 1))
    stats[0] = mean
    stats[1] = lax.rsqrt(spread * (1.0 / 128) + 1e-5)

    wb = bias_ref[...]

    def send_norm(s):
        @pl.when(s != col)
        def _():
            push(nm.at[s], nx.at[col], norm_send, norm_recv, row, s)

    for half in range(2):
        first = 8 * (lax.rem(z_lo + 1, 2) if half == 0 else z_lo)
        for s in [first + k for k in range(8)]:
            z = (np_[s].astype(F32) - stats[0, pl.ds(s, 1)]) * stats[1, pl.ds(s, 1)]
            u = gate[s] * dot(z.astype(BF16), tri_out_ref[...], TN)
            update[s] = u
            gate[s] = tile_of(x_ref, s) + u
        for q in range(2):
            at = pl.ds(pl.multiple_of(first + 4 * q, 4), 4)
            nb = norm_last(gate[at].reshape(512, 128)).astype(BF16)
            nm[at] = nb.reshape(4, 128, 128)
            z = dot(wb, nb, NT)
            for k in range(4):
                yb[pl.ds(first + 4 * q + k, 4, stride=16), :] = z[:, 128 * k : 128 * k + 128]
        for s in [first + k for k in range(8 if half == 0 else 0)]:
            push(nm.at[s], nx.at[col], norm_send, norm_recv, row, s)

    yt = yb[...].T
    own_keys = lax.broadcasted_iota(jnp.int32, (32, 256), 0) + 32 * col
    yt = jnp.concatenate([yt[32 * b : 32 * b + 32] for b in range(4)], axis=1)
    bm[...] = jnp.where(own_keys < length, yt, -1e9).astype(BF16)
    line_of = 64 * core + 8 * row + 4 * z_lo
    mine = line_of + x_at
    for k in range(1, 4):
        c = 8 * z_lo + 2 * lax.rem(x_at + k, 4) + core
        push(bm, bx.at[mine], line_send, line, row, c)
    loop(8 * z_lo, 8 * z_lo + 8, send_norm)
    nx[col] = nm[col]
    bx[mine] = bm[...]
    take(bx.at[pl.ds(0, 3)], line)
    z_hi = row % 2
    group = bx.at[pl.ds(line_of, 4)]
    for k in range(1, 4):
        z = lax.rem(z_at + k, 4)
        push(group, group, plane_send, plane.at[jnp.where(z // 2 == z_hi, 0, 1)], 2 * y_at + z // 2, 8 * (z % 2) + 2 * x_at + core)
    for k in (1, 3, 2):
        push(group, group, early_send, early.at[k], 2 * lax.rem(y_at + k, 4) + z_hi, col)

    turn = 2 * (x_at % 2)
    shift = x_at // 2 + 2 * z_lo

    def listed(o):
        late = lax.rem(o + shift, 4)
        last = jnp.where(late < 2, 3 - turn, 2)
        back = jnp.where(o < 2, 0, jnp.where(o < 4, 1 + turn, last))
        half = lax.rem(z_hi + jnp.where(o < 4, o, late), 2)
        return 2 * lax.rem(y_at - back + 4, 4) + half, back, half == z_hi

    put_off = jnp.where(chip // 2 == y_at, lax.rem(chip + 4, 8), chip)
    far_back = lax.rem(y_at - put_off // 2 + 4, 4)
    other = jnp.where(put_off % 2 == z_hi, 0, 1)
    place = jnp.where(
        far_back == 1 + turn,
        2 + other,
        4 + lax.rem(other + jnp.where(far_back == 2, 2, 0) - shift + 4, 4),
    )

    def rows_of(o):
        return listed(jnp.where(o == 7, place, o + jnp.where(o < place, 0, 1)))

    def bias_rows(r):
        return bx.at[pl.ds(64 * core + 8 * r, 8)]

    take(bx.at[pl.ds(0, 4)], plane.at[0])
    rest = bx.at[pl.ds(64 * core + 8 * row + 4 - 4 * z_lo, 4)]
    own_row, other_row = bias_rows(row), bias_rows(2 * y_at + 1 - z_hi)
    push(own_row, own_row, far_send, far.at[0], row, mate)
    for k in (1, 3, 2):
        push(rest, rest, near_send, near.at[k], 2 * lax.rem(y_at + k, 4) + z_hi, col)

    take(bx.at[pl.ds(0, 8)], plane.at[1])
    push(other_row, other_row, far_send, far.at[1], row, mate)
    for k in (1, 3, 2):
        push(other_row, other_row, near_send, near.at[4 + k], 2 * lax.rem(y_at + k, 4) + z_hi, col)

    take(nx.at[pl.ds(0, 15)], norm_recv)

    for q in range(4):
        at = slice(4 * q, 4 * q + 4)
        nb = nx[at].reshape(512, 128)
        qk = dot(nb, att_in_ref[:, :256])
        qs[at] = (qk[:, :128] * 32 ** (-0.5)).astype(BF16).reshape(4, 128, 128)
        ks[at] = qk[:, 128:].astype(BF16).reshape(4, 128, 128)
    for q in range(4):
        z = jax.nn.sigmoid(dot(wgt[...], nx[4 * q : 4 * q + 4].reshape(512, 128), NT))
        for k in range(4):
            gt[4 * q + k] = z[:, 128 * k : 128 * k + 128]
    for b in range(4):
        vt[b, :128] = dot(wvt[...], nx[:, 32 * b : 32 * b + 32, :].reshape(512, 128), NT).astype(BF16)
        vt[b, 128:] = jnp.ones((16, 512), BF16)

    tile[...] = jnp.zeros((2, 128, 128), F32)

    def block(o):
        r = rows_of(o)[0]

        @pl.when((o > 0) & (o < 7))
        def _():
            later, back, own_half = rows_of(o + 1)
            rows = bias_rows(later)

            @pl.when(own_half)
            def _():
                take(bx.at[pl.ds(0, 4)], early.at[back])
                take(bx.at[pl.ds(0, 4)], near.at[back])

            @pl.when(jnp.logical_not(own_half))
            def _():
                take(bx.at[pl.ds(0, 8)], near.at[4 + back])

            push(rows, rows, far_send, far.at[o + 1], row, mate)

        take(bx.at[pl.ds(0, 8)], far.at[o])
        for k in range(2):
            got = bx[pl.ds(pl.multiple_of(64 * k + 8 * r, 8), 8)].astype(F32)
            bias[:, k] = got * LOG2E

        def score(b):
            q = qs[pl.ds(2 * r, 2), 32 * b : 32 * b + 32, :].reshape(4, 1, 16, 128)
            hd = lax.broadcasted_iota(jnp.int32, (4, 4, 16, 128), 1)
            ln = lax.broadcasted_iota(jnp.int32, (4, 4, 16, 128), 3)
            qm = jnp.where(
                hd == ln // 32, jnp.broadcast_to(q, (4, 4, 16, 128)).astype(F32), 0.0
            ).astype(BF16)
            keys = ks[:, 32 * b : 32 * b + 32, :].reshape(512, 128)
            st = dot(keys, qm.reshape(256, 128), NT) * LOG2E + bias[...].reshape(512, 256)
            scores[b] = st
            return jnp.max(st, axis=0, keepdims=True)

        top = score(0)
        for b in range(4):
            later_top = score(b + 1) if b < 3 else None
            ot = dot(vt[b], jnp.exp2(scores[b] - top).astype(BF16))
            ot = ot[:128] * (1.0 / ot[128:129])
            for h in range(4):
                part = ot[32 * h : 32 * h + 32]
                for j in range(4):
                    at = 64 * (j % 2) + 16 * h
                    to = 32 * b + 16 * (j % 2)
                    moved = part[:, 128 * (j // 2) : 128 * (j // 2) + 128]
                    if (to - at) % 128:
                        moved = pltpu.roll(moved, (to - at) % 128, 1)
                    here = (lane128 >= to) & (lane128 < to + 16)
                    rows = slice(32 * h, 32 * h + 32)
                    tile[j // 2, rows] = jnp.where(here, moved, tile[j // 2, rows])
            top = later_top
        for k in range(2):
            c = 2 * r + k
            go[c] = (tile[k] * gt[c]).astype(BF16)
        for k in range(2):
            c = 2 * r + k

            @pl.when(c != col)
            def _():
                push(go.at[c], gx.at[col], back_send, back_recv, row, c)

    loop(0, 8, block)
    gx[col] = go[col]
    take(gx.at[pl.ds(0, 15)], back_recv)

    for g in range(4):
        for s in range(4 * g, 4 * g + 4):
            t = update[s] + dot(gx[s], att_out_ref[...], TN)
            for b in range(4):
                out[b, s] = t[32 * b : 32 * b + 32]
    take(rx.at[0, pl.ds(0, 127)], right_send)
    take(rx.at[0, pl.ds(0, 127)], left_send)
    take(px.at[pl.ds(0, 127)], prod_send)
    take(nx.at[pl.ds(0, 15)], norm_send)
    take(bx.at[pl.ds(0, 3)], line_send)
    take(bx.at[pl.ds(0, 12)], plane_send)
    take(bx.at[pl.ds(0, 12)], early_send)
    take(bx.at[pl.ds(0, 36)], near_send)
    take(bx.at[pl.ds(0, 64)], far_send)
    take(go.at[pl.ds(0, 15)], back_send)


SCRATCH = [
    ((64, 32, 128), F32),
    ((128, 512), BF16),
    ((128, 128), BF16),
    ((128, 128), BF16),
    ((4, 128), BF16),
    ((128, 512), BF16),
    ((128, 128), BF16),
    ((16, 128, 128), BF16),
    ((16, 128, 128), F32),
    ((512, 128), BF16),
    ((128, 128), BF16),
    ((128, 128), BF16),
    ((4, 256, 256), BF16),
    ((2, 128, 16, 128), BF16),
    ((2, 128, 16, 128), BF16),
    ((16, 128, 128), BF16),
    ((64, 512), BF16),
    ((512, 512), BF16),
    ((128, 16, 128), BF16),
    ((128, 16, 128), BF16),
    ((16, 128, 128), F32),
    ((16, 128, 128), BF16),
    ((2, 16, 128), F32),
    ((64, 128), F32),
    ((16, 128, 128), BF16),
    ((16, 128, 128), BF16),
    ((32, 256), BF16),
    ((128, 32, 256), BF16),
    ((16, 128, 128), BF16),
    ((16, 128, 128), BF16),
    ((4, 144, 512), BF16),
    ((16, 128, 128), F32),
    ((8, 2, 32, 256), F32),
    ((4, 512, 256), F32),
    ((2, 128, 128), F32),
    ((16, 128, 128), BF16),
]
SEMAPHORES = [
    (7,), (), (), (), (8,), (), (8,), (), (), (), (), (), (2,), (), (4,), (), (8,), (), (8,), (), (),
]


def per_device(pair, valid_length, tri_in, tri_gate, tri_out, att_in, att_bias, att_out):
    vmem = pl.BlockSpec(memory_space=pltpu.VMEM)
    smem = pl.BlockSpec(memory_space=pltpu.SMEM)
    hbm = pl.BlockSpec(memory_space=pltpu.HBM)
    change = pl.pallas_call(
        kernel,
        out_shape=jax.ShapeDtypeStruct((4, 16, 32, 128), F32),
        in_specs=[hbm, smem] + [hbm] * 6,
        out_specs=vmem,
        scratch_shapes=[pltpu.VMEM(*s) for s in SCRATCH]
        + [pltpu.SemaphoreType.DMA(s) for s in SEMAPHORES],
        compiler_params=pltpu.CompilerParams(
            collective_id=0, has_side_effects=True, vmem_limit_bytes=40 * 1024 * 1024
        ),
    )(*[a if n == 1 else pltpu.with_memory_space_constraint(a, pltpu.HBM) for n, a in enumerate((pair, valid_length, tri_in, tri_gate, tri_out, att_bias.T, att_in, att_out))])
    return pair + change.reshape(64, 32, 128)


def solution(mesh):
    placed = (P("row", "col", None), P(), P(), P(), P(), P(), P(), P())
    return jax.shard_map(
        per_device, mesh=mesh, in_specs=placed, out_specs=P("row", "col", None), check_vma=False
    )
```

```python
import jax
import jax.numpy as jnp
from jax import lax
from jax.experimental import pallas as pl
from jax.experimental.pallas import tpu as pltpu
from jax.sharding import PartitionSpec as P

MESH = pl.DeviceIdType.MESH
LOG2E = 1.4426950408889634
F32 = jnp.float32
BF16 = jnp.bfloat16
NT = (((1,), (1,)), ((), ()))
TN = (((0,), (0,)), ((), ()))
NN = (((1,), (0,)), ((), ()))


def dot(a, b, dims=NN):
    return lax.dot_general(a, b, dims, preferred_element_type=F32)


def norm_last(x):
    c = x - jnp.mean(x, axis=-1, keepdims=True)
    return c * lax.rsqrt(jnp.mean(c * c, axis=-1, keepdims=True) + 1e-5)


def turned(w):
    return w.astype(F32).T.astype(BF16)


def swap16():
    p = lax.broadcasted_iota(jnp.int32, (256, 256), 0)
    q = lax.broadcasted_iota(jnp.int32, (256, 256), 1)
    return (q == (p % 16) * 16 + p // 16).astype(F32).astype(BF16)


def block_turn(tiles):
    return [
        jnp.concatenate([t[:, 32 * b : 32 * b + 32] for t in tiles], axis=1) for b in range(4)
    ]


def tile_of(x_ref, s):
    return jnp.concatenate([x_ref[16 * b + s] for b in range(4)], axis=0)


def rows16(start):
    return pl.ds(pl.multiple_of(16 * start, 16), 16)


def loop(low, high, body, unroll=1):
    def step(n, carry):
        body(n)
        return carry

    lax.fori_loop(low, high, step, 0, unroll=unroll)


def push(src, dst, send_sem, recv_sem, row, col):
    pltpu.make_async_remote_copy(src, dst, send_sem, recv_sem, (row, col), MESH).start()


def take(ref, sem):
    pltpu.make_async_copy(ref, ref, sem).wait()


def kernel(
    x_hbm, len_ref, tri_in_hbm, tri_gate_hbm, tri_out_hbm, bias_hbm, att_in_hbm, att_out_hbm, out,
    x_ref, tri_in_ref, tri_gate_ref, tri_out_ref, bias_ref, att_in_ref, att_out_ref, gx, update, wt, wvt, wgt, y, e, rx, n, lm, rm, po, px, gate, np_, stats, yb, nm, nx, bm, bx,
    qs, ks, vt, gt, bias, scores, tile, go,
    load, right_send, right_recv, left_send, left_recv, prod_send, prod_recv, norm_send, norm_recv,
    line_send, line, plane_send, plane, early_send, early, near_send, near, far_send, far, back_send, back_recv,
):
    row, col = lax.axis_index("row"), lax.axis_index("col")
    me = 16 * row + col
    chip, core = col // 2, col % 2
    z_lo, x_at = chip // 4, chip % 4
    y_at, z_at = row // 2, 2 * (row % 2) + z_lo
    mate = col + 1 - 2 * core
    bar = pltpu.get_barrier_semaphore()
    pairs = (
        (tri_in_hbm, tri_in_ref), (x_hbm, x_ref), (tri_gate_hbm, tri_gate_ref), (att_in_hbm, att_in_ref),
        (tri_out_hbm, tri_out_ref), (bias_hbm, bias_ref), (att_out_hbm, att_out_ref),
    )
    fetch = [pltpu.make_async_copy(a, b, load.at[n]) for n, (a, b) in enumerate(pairs)]
    for copy in fetch:
        copy.start()

    def greet(r, first=0):
        for k in range(first, 16):
            c = lax.rem(col + k, 16)
            pl.semaphore_signal(bar, inc=1, device_id=(r, c), device_id_type=MESH)

    greet(row, 1)
    loop(1, 8, lambda a: greet(lax.rem(row + a, 8)))
    fetch[0].wait()
    wt[...] = turned(tri_in_ref[...])
    perm = swap16()
    lane128 = lax.broadcasted_iota(jnp.int32, (1, 128), 1)
    length = len_ref[0]
    keep_k = (32 * col + lane128 % 32) < length
    fetch[1].wait()

    def edge(side, s, nb):
        pt = dot(wt[256 * side : 256 * side + 256], nb, NT)
        w = jnp.where(keep_k & ((64 * row + (lane128 // 32) * 16 + s) < length), 1.0, 0.0)
        v = (jax.nn.sigmoid(pt[:128]) * pt[128:] * w).astype(BF16)
        for g in range(8):
            at = slice(128 * (g % 2), 128 * (g % 2) + 128)
            y[g // 2, rows16(s), at] = v[16 * g : 16 * g + 16]

    def order(side):
        for g in range(4):
            z = dot(perm, y[g]).astype(BF16)
            e[side, 32 * g : 32 * g + 16] = z[:, :128].reshape(16, 16, 128)
            e[side, 32 * g + 16 : 32 * g + 32] = z[:, 128:].reshape(16, 16, 128)

    def first_edge(s):
        edge(1, s, n[s])

    def send_right(k):
        c = lax.rem(col + k, 16)
        for a in range(1 if k == 0 else 0, 8):
            r = lax.rem(row + a, 8)
            push(e.at[1, 16 * r + c], rx.at[1, me], right_send, right_recv, r, c)

    def send_left(q):
        for k in [4 * (j % 4) + j // 4 for j in range(16)]:
            c = lax.rem(col + k, 16)
            for a in (2 * q, 2 * q + 1):
                if a or k:
                    r = lax.rem(row + 8 - a, 8)
                    push(e.at[0, 16 * r + c], rx.at[0, me], left_send, left_recv.at[a], r, c)

    def first_norm(q):
        rows = jnp.concatenate([tile_of(x_ref, 4 * q + k) for k in range(4)], axis=0)
        n[pl.ds(pl.multiple_of(4 * q, 4), 4)] = norm_last(rows).astype(BF16).reshape(4, 128, 128)

    loop(0, 4, first_norm, 4)
    loop(0, 16, first_edge, 4)
    order(1)
    for copy in fetch[2:]:
        copy.wait()
    pl.semaphore_wait(bar, 127)
    for q in range(4):
        for k in range(4):
            send_right(4 * k + q)
        for s in range(4 * q, 4 * q + 4):
            edge(0, s, n[s])
    rx[1, me] = e[1, me]
    order(0)
    for q in range(4):
        send_left(q)
        for s in range(4 * q, 4 * q + 4):
            gate[s] = jax.nn.sigmoid(dot(n[s], tri_gate_ref[...]))
    rx[0, me] = e[0, me]
    wvt[...] = turned(att_in_ref[:, 256:384])
    wgt[...] = turned(att_in_ref[:, 384:512])

    def assemble(side, r, m, at):
        for cg in range(4):
            tiles = [rx[side, 16 * r + 4 * cg + c] for c in range(4)]
            for b, t in enumerate(block_turn(tiles)):
                m[rows16(at + b), 128 * cg : 128 * cg + 128] = t

    take(rx.at[1, pl.ds(0, 127)], right_recv)
    loop(0, 8, lambda r: assemble(1, r, rm, 4 * r), 4)

    def product(o, first=0):
        r = lax.rem(row + o, 8)
        take(rx.at[0, pl.ds(0, 16 - first)], left_recv.at[o])
        assemble(0, r, lm, 0)
        p = dot(lm[...], rm[...], NT).astype(BF16)
        for cg in range(4):
            tiles = [p[16 * b : 16 * b + 16, 128 * cg : 128 * cg + 128] for b in range(4)]
            for c, t in enumerate(block_turn(tiles)):
                po[16 * r + 4 * cg + c] = t
        for k in [4 * (j % 4) + j // 4 for j in range(first, 16)]:
            c = lax.rem(col + k, 16)
            push(po.at[16 * r + c], px.at[me], prod_send, prod_recv.at[o], r, c)

    product(0, 1)
    loop(1, 8, product)
    px[me] = po[me]

    for o in range(8):
        r = lax.rem(row - o + 8, 8)
        take(px.at[pl.ds(0, 15 if o == 0 else 16)], prod_recv.at[o])
        got = px[rows16(r)]
        np_[:, rows16(r), :] = dot(perm, got.reshape(256, 128)).astype(BF16).reshape(16, 16, 128)
        got = got.astype(F32)
        group_mean = jnp.sum(got, axis=0) * (1.0 / 16)
        got = got - group_mean[None]
        squares = jnp.sum(got * got, axis=0)
        if o == 0:
            mean, spread = group_mean, squares
        else:
            step = group_mean - mean
            mean = mean + step * (1.0 / (o + 1))
            spread = spread + squares + step * step * (16.0 * o / (o + 1))
    stats[0] = mean
    stats[1] = lax.rsqrt(spread * (1.0 / 128) + 1e-5)

    wb = bias_ref[...]

    def send_norm(s):
        @pl.when(s != col)
        def _():
            push(nm.at[s], nx.at[col], norm_send, norm_recv, row, s)

    for half in range(2):
        first = 8 * (lax.rem(z_lo + 1, 2) if half == 0 else z_lo)
        for s in [first + k for k in range(8)]:
            z = (np_[s].astype(F32) - stats[0, pl.ds(s, 1)]) * stats[1, pl.ds(s, 1)]
            u = gate[s] * dot(z.astype(BF16), tri_out_ref[...], TN)
            update[s] = u
            gate[s] = tile_of(x_ref, s) + u
        for q in range(2):
            at = pl.ds(pl.multiple_of(first + 4 * q, 4), 4)
            nb = norm_last(gate[at].reshape(512, 128)).astype(BF16)
            nm[at] = nb.reshape(4, 128, 128)
            z = dot(wb, nb, NT)
            for k in range(4):
                yb[pl.ds(first + 4 * q + k, 4, stride=16), :] = z[:, 128 * k : 128 * k + 128]
        for s in [first + k for k in range(8 if half == 0 else 0)]:
            push(nm.at[s], nx.at[col], norm_send, norm_recv, row, s)

    yt = yb[...].T
    own_keys = lax.broadcasted_iota(jnp.int32, (32, 256), 0) + 32 * col
    yt = jnp.concatenate([yt[32 * b : 32 * b + 32] for b in range(4)], axis=1)
    bm[...] = jnp.where(own_keys < length, yt, -1e9).astype(BF16)
    line_of = 64 * core + 8 * row + 4 * z_lo
    mine = line_of + x_at
    for k in range(1, 4):
        c = 8 * z_lo + 2 * lax.rem(x_at + k, 4) + core
        push(bm, bx.at[mine], line_send, line, row, c)
    loop(8 * z_lo, 8 * z_lo + 8, send_norm)
    nx[col] = nm[col]
    bx[mine] = bm[...]
    take(bx.at[pl.ds(0, 3)], line)
    z_hi = row % 2
    group = bx.at[pl.ds(line_of, 4)]
    for k in range(1, 4):
        z = lax.rem(z_at + k, 4)
        push(group, group, plane_send, plane.at[jnp.where(z // 2 == z_hi, 0, 1)], 2 * y_at + z // 2, 8 * (z % 2) + 2 * x_at + core)
    for k in (1, 3, 2):
        push(group, group, early_send, early.at[k], 2 * lax.rem(y_at + k, 4) + z_hi, col)

    turn = 2 * (x_at % 2)
    shift = x_at // 2 + 2 * z_lo

    def listed(o):
        late = lax.rem(o + shift, 4)
        last = jnp.where(late < 2, 3 - turn, 2)
        back = jnp.where(o < 2, 0, jnp.where(o < 4, 1 + turn, last))
        half = lax.rem(z_hi + jnp.where(o < 4, o, late), 2)
        return 2 * lax.rem(y_at - back + 4, 4) + half, back, half == z_hi

    put_off = jnp.where(chip // 2 == y_at, lax.rem(chip + 4, 8), chip)
    far_back = lax.rem(y_at - put_off // 2 + 4, 4)
    other = jnp.where(put_off % 2 == z_hi, 0, 1)
    place = jnp.where(
        far_back == 1 + turn,
        2 + other,
        4 + lax.rem(other + jnp.where(far_back == 2, 2, 0) - shift + 4, 4),
    )

    def rows_of(o):
        return listed(jnp.where(o == 7, place, o + jnp.where(o < place, 0, 1)))

    def bias_rows(r):
        return bx.at[pl.ds(64 * core + 8 * r, 8)]

    take(bx.at[pl.ds(0, 4)], plane.at[0])
    rest = bx.at[pl.ds(64 * core + 8 * row + 4 - 4 * z_lo, 4)]
    own_row, other_row = bias_rows(row), bias_rows(2 * y_at + 1 - z_hi)
    push(own_row, own_row, far_send, far.at[0], row, mate)
    for k in (1, 3, 2):
        push(rest, rest, near_send, near.at[k], 2 * lax.rem(y_at + k, 4) + z_hi, col)

    take(bx.at[pl.ds(0, 8)], plane.at[1])
    push(other_row, other_row, far_send, far.at[1], row, mate)
    for k in (1, 3, 2):
        push(other_row, other_row, near_send, near.at[4 + k], 2 * lax.rem(y_at + k, 4) + z_hi, col)

    take(nx.at[pl.ds(0, 15)], norm_recv)

    for q in range(4):
        at = slice(4 * q, 4 * q + 4)
        nb = nx[at].reshape(512, 128)
        qk = dot(nb, att_in_ref[:, :256])
        qs[at] = (qk[:, :128] * 32 ** (-0.5)).astype(BF16).reshape(4, 128, 128)
        ks[at] = qk[:, 128:].astype(BF16).reshape(4, 128, 128)
    for q in range(4):
        z = jax.nn.sigmoid(dot(wgt[...], nx[4 * q : 4 * q + 4].reshape(512, 128), NT))
        for k in range(4):
            gt[4 * q + k] = z[:, 128 * k : 128 * k + 128]
    for b in range(4):
        vt[b, :128] = dot(wvt[...], nx[:, 32 * b : 32 * b + 32, :].reshape(512, 128), NT).astype(BF16)
        vt[b, 128:] = jnp.ones((16, 512), BF16)

    tile[...] = jnp.zeros((2, 128, 128), F32)

    def block(o):
        r = rows_of(o)[0]

        @pl.when((o > 0) & (o < 7))
        def _():
            later, back, own_half = rows_of(o + 1)
            rows = bias_rows(later)

            @pl.when(own_half)
            def _():
                take(bx.at[pl.ds(0, 4)], early.at[back])
                take(bx.at[pl.ds(0, 4)], near.at[back])

            @pl.when(jnp.logical_not(own_half))
            def _():
                take(bx.at[pl.ds(0, 8)], near.at[4 + back])

            push(rows, rows, far_send, far.at[o + 1], row, mate)

        take(bx.at[pl.ds(0, 8)], far.at[o])
        for k in range(2):
            got = bx[pl.ds(pl.multiple_of(64 * k + 8 * r, 8), 8)].astype(F32)
            bias[:, k] = got * LOG2E

        def score(b):
            q = qs[pl.ds(2 * r, 2), 32 * b : 32 * b + 32, :].reshape(4, 1, 16, 128)
            hd = lax.broadcasted_iota(jnp.int32, (4, 4, 16, 128), 1)
            ln = lax.broadcasted_iota(jnp.int32, (4, 4, 16, 128), 3)
            qm = jnp.where(
                hd == ln // 32, jnp.broadcast_to(q, (4, 4, 16, 128)).astype(F32), 0.0
            ).astype(BF16)
            keys = ks[:, 32 * b : 32 * b + 32, :].reshape(512, 128)
            st = dot(keys, qm.reshape(256, 128), NT) * LOG2E + bias[...].reshape(512, 256)
            scores[b] = st
            return jnp.max(st, axis=0, keepdims=True)

        top = score(0)
        for b in range(4):
            later_top = score(b + 1) if b < 3 else None
            ot = dot(vt[b], jnp.exp2(scores[b] - top).astype(BF16))
            ot = ot[:128] * (1.0 / ot[128:129])
            for h in range(4):
                part = ot[32 * h : 32 * h + 32]
                for j in range(4):
                    at = 64 * (j % 2) + 16 * h
                    to = 32 * b + 16 * (j % 2)
                    moved = part[:, 128 * (j // 2) : 128 * (j // 2) + 128]
                    if (to - at) % 128:
                        moved = pltpu.roll(moved, (to - at) % 128, 1)
                    here = (lane128 >= to) & (lane128 < to + 16)
                    rows = slice(32 * h, 32 * h + 32)
                    tile[j // 2, rows] = jnp.where(here, moved, tile[j // 2, rows])
            top = later_top
        for k in range(2):
            c = 2 * r + k
            go[c] = (tile[k] * gt[c]).astype(BF16)
        for k in range(2):
            c = 2 * r + k

            @pl.when(c != col)
            def _():
                push(go.at[c], gx.at[col], back_send, back_recv, row, c)

    loop(0, 8, block)
    gx[col] = go[col]
    take(gx.at[pl.ds(0, 15)], back_recv)

    for g in range(4):
        for s in range(4 * g, 4 * g + 4):
            t = update[s] + dot(gx[s], att_out_ref[...], TN)
            for b in range(4):
                out[b, s] = t[32 * b : 32 * b + 32]
    take(rx.at[0, pl.ds(0, 127)], right_send)
    take(rx.at[0, pl.ds(0, 127)], left_send)
    take(px.at[pl.ds(0, 127)], prod_send)
    take(nx.at[pl.ds(0, 15)], norm_send)
    take(bx.at[pl.ds(0, 3)], line_send)
    take(bx.at[pl.ds(0, 12)], plane_send)
    take(bx.at[pl.ds(0, 12)], early_send)
    take(bx.at[pl.ds(0, 36)], near_send)
    take(bx.at[pl.ds(0, 64)], far_send)
    take(go.at[pl.ds(0, 15)], back_send)


SCRATCH = [
    ((64, 32, 128), F32),
    ((128, 512), BF16),
    ((128, 128), BF16),
    ((128, 128), BF16),
    ((4, 128), BF16),
    ((128, 512), BF16),
    ((128, 128), BF16),
    ((16, 128, 128), BF16),
    ((16, 128, 128), F32),
    ((512, 128), BF16),
    ((128, 128), BF16),
    ((128, 128), BF16),
    ((4, 256, 256), BF16),
    ((2, 128, 16, 128), BF16),
    ((2, 128, 16, 128), BF16),
    ((16, 128, 128), BF16),
    ((64, 512), BF16),
    ((512, 512), BF16),
    ((128, 16, 128), BF16),
    ((128, 16, 128), BF16),
    ((16, 128, 128), F32),
    ((16, 128, 128), BF16),
    ((2, 16, 128), F32),
    ((64, 128), F32),
    ((16, 128, 128), BF16),
    ((16, 128, 128), BF16),
    ((32, 256), BF16),
    ((128, 32, 256), BF16),
    ((16, 128, 128), BF16),
    ((16, 128, 128), BF16),
    ((4, 144, 512), BF16),
    ((16, 128, 128), F32),
    ((8, 2, 32, 256), F32),
    ((4, 512, 256), F32),
    ((2, 128, 128), F32),
    ((16, 128, 128), BF16),
]
SEMAPHORES = [
    (7,), (), (), (), (8,), (), (8,), (), (), (), (), (), (2,), (), (4,), (), (8,), (), (8,), (), (),
]


def per_device(pair, valid_length, tri_in, tri_gate, tri_out, att_in, att_bias, att_out):
    vmem = pl.BlockSpec(memory_space=pltpu.VMEM)
    smem = pl.BlockSpec(memory_space=pltpu.SMEM)
    hbm = pl.BlockSpec(memory_space=pltpu.HBM)
    change = pl.pallas_call(
        kernel,
        out_shape=jax.ShapeDtypeStruct((4, 16, 32, 128), F32),
        in_specs=[hbm, smem] + [hbm] * 6,
        out_specs=vmem,
        scratch_shapes=[pltpu.VMEM(*s) for s in SCRATCH]
        + [pltpu.SemaphoreType.DMA(s) for s in SEMAPHORES],
        compiler_params=pltpu.CompilerParams(
            collective_id=0, has_side_effects=True, vmem_limit_bytes=40 * 1024 * 1024
        ),
    )(*[a if n == 1 else pltpu.with_memory_space_constraint(a, pltpu.HBM) for n, a in enumerate((pair, valid_length, tri_in, tri_gate, tri_out, att_bias.T, att_in, att_out))])
    return pair + change.reshape(64, 32, 128)


def solution(mesh):
    placed = (P("row", "col", None), P(), P(), P(), P(), P(), P(), P())
    return jax.shard_map(
        per_device, mesh=mesh, in_specs=placed, out_specs=P("row", "col", None), check_vma=False
    )
```

```python
import jax
import jax.numpy as jnp
from jax import lax
from jax.experimental import pallas as pl
from jax.experimental.pallas import tpu as pltpu
from jax.sharding import PartitionSpec as P

MESH = pl.DeviceIdType.MESH
LOG2E = 1.4426950408889634
F32 = jnp.float32
BF16 = jnp.bfloat16
NT = (((1,), (1,)), ((), ()))
TN = (((0,), (0,)), ((), ()))
NN = (((1,), (0,)), ((), ()))


def dot(a, b, dims=NN):
    return lax.dot_general(a, b, dims, preferred_element_type=F32)


def norm_last(x):
    c = x - jnp.mean(x, axis=-1, keepdims=True)
    return c * lax.rsqrt(jnp.mean(c * c, axis=-1, keepdims=True) + 1e-5)


def turned(w):
    return w.astype(F32).T.astype(BF16)


def swap16():
    p = lax.broadcasted_iota(jnp.int32, (256, 256), 0)
    q = lax.broadcasted_iota(jnp.int32, (256, 256), 1)
    return (q == (p % 16) * 16 + p // 16).astype(F32).astype(BF16)


def block_turn(tiles):
    return [
        jnp.concatenate([t[:, 32 * b : 32 * b + 32] for t in tiles], axis=1) for b in range(4)
    ]


def tile_of(x_ref, s):
    return jnp.concatenate([x_ref[16 * b + s] for b in range(4)], axis=0)


def rows16(start):
    return pl.ds(pl.multiple_of(16 * start, 16), 16)


def loop(low, high, body, unroll=1):
    def step(n, carry):
        body(n)
        return carry

    lax.fori_loop(low, high, step, 0, unroll=unroll)


def push(src, dst, send_sem, recv_sem, row, col):
    pltpu.make_async_remote_copy(src, dst, send_sem, recv_sem, (row, col), MESH).start()


def take(ref, sem):
    pltpu.make_async_copy(ref, ref, sem).wait()


def kernel(
    x_hbm, len_ref, tri_in_hbm, tri_gate_hbm, tri_out_hbm, bias_hbm, att_in_hbm, att_out_hbm, out,
    x_ref, tri_in_ref, tri_gate_ref, tri_out_ref, bias_ref, att_in_ref, att_out_ref, gx, update, wt, wvt, wgt, y, e, rx, n, lm, rm, po, px, gate, np_, stats, yb, nm, nx, bm, bx,
    qs, ks, vt, gt, bias, scores, tile, go,
    load, right_send, right_recv, left_send, left_recv, prod_send, prod_recv, norm_send, norm_recv,
    line_send, line, plane_send, plane, early_send, early, near_send, near, far_send, far, back_send, back_recv,
):
    row, col = lax.axis_index("row"), lax.axis_index("col")
    me = 16 * row + col
    chip, core = col // 2, col % 2
    z_lo, x_at = chip // 4, chip % 4
    y_at, z_at = row // 2, 2 * (row % 2) + z_lo
    mate = col + 1 - 2 * core
    bar = pltpu.get_barrier_semaphore()
    pairs = (
        (tri_in_hbm, tri_in_ref), (x_hbm, x_ref), (tri_gate_hbm, tri_gate_ref), (att_in_hbm, att_in_ref),
        (tri_out_hbm, tri_out_ref), (bias_hbm, bias_ref), (att_out_hbm, att_out_ref),
    )
    fetch = [pltpu.make_async_copy(a, b, load.at[n]) for n, (a, b) in enumerate(pairs)]
    for copy in fetch:
        copy.start()

    def greet(r, first=0):
        for k in range(first, 16):
            c = lax.rem(col + k, 16)
            pl.semaphore_signal(bar, inc=1, device_id=(r, c), device_id_type=MESH)

    loop(2, 9, lambda a: greet(lax.rem(row + lax.rem(a + 2, 8) + jnp.where(a > 5, 1, 0), 8)))
    greet(row, 1)
    fetch[0].wait()
    wt[...] = turned(tri_in_ref[...])
    perm = swap16()
    lane128 = lax.broadcasted_iota(jnp.int32, (1, 128), 1)
    length = len_ref[0]
    keep_k = (32 * col + lane128 % 32) < length
    fetch[1].wait()

    def edge(side, s, nb):
        pt = dot(wt[256 * side : 256 * side + 256], nb, NT)
        w = jnp.where(keep_k & ((64 * row + (lane128 // 32) * 16 + s) < length), 1.0, 0.0)
        v = (jax.nn.sigmoid(pt[:128]) * pt[128:] * w).astype(BF16)
        for g in range(8):
            at = slice(128 * (g % 2), 128 * (g % 2) + 128)
            y[g // 2, rows16(s), at] = v[16 * g : 16 * g + 16]

    def order(side):
        for g in range(4):
            z = dot(perm, y[g]).astype(BF16)
            e[side, 32 * g : 32 * g + 16] = z[:, :128].reshape(16, 16, 128)
            e[side, 32 * g + 16 : 32 * g + 32] = z[:, 128:].reshape(16, 16, 128)

    def first_edge(s):
        edge(1, s, n[s])

    def send_right(k):
        c = lax.rem(col + k, 16)
        for a in range(1 if k == 0 else 0, 8):
            r = lax.rem(row + a, 8)
            push(e.at[1, 16 * r + c], rx.at[1, me], right_send, right_recv, r, c)

    def send_left(q):
        for k in [4 * (j % 4) + j // 4 for j in range(16)]:
            c = lax.rem(col + k, 16)
            for a in (2 * q, 2 * q + 1):
                if a or k:
                    r = lax.rem(row + 8 - a, 8)
                    push(e.at[0, 16 * r + c], rx.at[0, me], left_send, left_recv.at[a], r, c)

    def first_norm(q):
        rows = jnp.concatenate([tile_of(x_ref, 4 * q + k) for k in range(4)], axis=0)
        n[pl.ds(pl.multiple_of(4 * q, 4), 4)] = norm_last(rows).astype(BF16).reshape(4, 128, 128)

    loop(0, 4, first_norm, 4)
    loop(0, 16, first_edge, 4)
    order(1)
    for copy in fetch[2:]:
        copy.wait()
    pl.semaphore_wait(bar, 127)
    for q in range(4):
        for k in range(4):
            send_right(4 * k + q)
        for s in range(4 * q, 4 * q + 4):
            edge(0, s, n[s])
    rx[1, me] = e[1, me]
    order(0)
    for q in range(4):
        send_left(q)
        for s in range(4 * q, 4 * q + 4):
            gate[s] = jax.nn.sigmoid(dot(n[s], tri_gate_ref[...]))
    rx[0, me] = e[0, me]
    wvt[...] = turned(att_in_ref[:, 256:384])
    wgt[...] = turned(att_in_ref[:, 384:512])

    def assemble(side, r, m, at):
        for cg in range(4):
            tiles = [rx[side, 16 * r + 4 * cg + c] for c in range(4)]
            for b, t in enumerate(block_turn(tiles)):
                m[rows16(at + b), 128 * cg : 128 * cg + 128] = t

    take(rx.at[1, pl.ds(0, 127)], right_recv)
    loop(0, 8, lambda r: assemble(1, r, rm, 4 * r), 4)

    def product(o, first=0):
        r = lax.rem(row + o, 8)
        take(rx.at[0, pl.ds(0, 16 - first)], left_recv.at[o])
        assemble(0, r, lm, 0)
        p = dot(lm[...], rm[...], NT).astype(BF16)
        for cg in range(4):
            tiles = [p[16 * b : 16 * b + 16, 128 * cg : 128 * cg + 128] for b in range(4)]
            for c, t in enumerate(block_turn(tiles)):
                po[16 * r + 4 * cg + c] = t
        for k in [4 * (j % 4) + j // 4 for j in range(first, 16)]:
            c = lax.rem(col + k, 16)
            push(po.at[16 * r + c], px.at[me], prod_send, prod_recv.at[o], r, c)

    product(0, 1)
    loop(1, 8, product)
    px[me] = po[me]

    for o in range(8):
        r = lax.rem(row - o + 8, 8)
        take(px.at[pl.ds(0, 15 if o == 0 else 16)], prod_recv.at[o])
        got = px[rows16(r)]
        np_[:, rows16(r), :] = dot(perm, got.reshape(256, 128)).astype(BF16).reshape(16, 16, 128)
        got = got.astype(F32)
        group_mean = jnp.sum(got, axis=0) * (1.0 / 16)
        got = got - group_mean[None]
        squares = jnp.sum(got * got, axis=0)
        if o == 0:
            mean, spread = group_mean, squares
        else:
            step = group_mean - mean
            mean = mean + step * (1.0 / (o + 1))
            spread = spread + squares + step * step * (16.0 * o / (o + 1))
    stats[0] = mean
    stats[1] = lax.rsqrt(spread * (1.0 / 128) + 1e-5)

    wb = bias_ref[...]

    def send_norm(s):
        @pl.when(s != col)
        def _():
            push(nm.at[s], nx.at[col], norm_send, norm_recv, row, s)

    for half in range(2):
        first = 8 * (lax.rem(z_lo + 1, 2) if half == 0 else z_lo)
        for s in [first + k for k in range(8)]:
            z = (np_[s].astype(F32) - stats[0, pl.ds(s, 1)]) * stats[1, pl.ds(s, 1)]
            u = gate[s] * dot(z.astype(BF16), tri_out_ref[...], TN)
            update[s] = u
            gate[s] = tile_of(x_ref, s) + u
        for q in range(2):
            at = pl.ds(pl.multiple_of(first + 4 * q, 4), 4)
            nb = norm_last(gate[at].reshape(512, 128)).astype(BF16)
            nm[at] = nb.reshape(4, 128, 128)
            z = dot(wb, nb, NT)
            for k in range(4):
                yb[pl.ds(first + 4 * q + k, 4, stride=16), :] = z[:, 128 * k : 128 * k + 128]
        for s in [first + k for k in range(8 if half == 0 else 0)]:
            push(nm.at[s], nx.at[col], norm_send, norm_recv, row, s)

    yt = yb[...].T
    own_keys = lax.broadcasted_iota(jnp.int32, (32, 256), 0) + 32 * col
    yt = jnp.concatenate([yt[32 * b : 32 * b + 32] for b in range(4)], axis=1)
    bm[...] = jnp.where(own_keys < length, yt, -1e9).astype(BF16)
    line_of = 64 * core + 8 * row + 4 * z_lo
    mine = line_of + x_at
    for k in range(1, 4):
        c = 8 * z_lo + 2 * lax.rem(x_at + k, 4) + core
        push(bm, bx.at[mine], line_send, line, row, c)
    loop(8 * z_lo, 8 * z_lo + 8, send_norm)
    nx[col] = nm[col]
    bx[mine] = bm[...]
    take(bx.at[pl.ds(0, 3)], line)
    z_hi = row % 2
    group = bx.at[pl.ds(line_of, 4)]
    for k in range(1, 4):
        z = lax.rem(z_at + k, 4)
        push(group, group, plane_send, plane.at[jnp.where(z // 2 == z_hi, 0, 1)], 2 * y_at + z // 2, 8 * (z % 2) + 2 * x_at + core)
    for k in (1, 3, 2):
        push(group, group, early_send, early.at[k], 2 * lax.rem(y_at + k, 4) + z_hi, col)

    turn = 2 * (x_at % 2)
    shift = x_at // 2 + 2 * z_lo

    def listed(o):
        late = lax.rem(o + shift, 4)
        last = jnp.where(late < 2, 3 - turn, 2)
        back = jnp.where(o < 2, 0, jnp.where(o < 4, 1 + turn, last))
        half = lax.rem(z_hi + jnp.where(o < 4, o, late), 2)
        return 2 * lax.rem(y_at - back + 4, 4) + half, back, half == z_hi

    put_off = jnp.where(chip // 2 == y_at, lax.rem(chip + 4, 8), chip)
    far_back = lax.rem(y_at - put_off // 2 + 4, 4)
    other = jnp.where(put_off % 2 == z_hi, 0, 1)
    place = jnp.where(
        far_back == 1 + turn,
        2 + other,
        4 + lax.rem(other + jnp.where(far_back == 2, 2, 0) - shift + 4, 4),
    )

    def rows_of(o):
        return listed(jnp.where(o == 7, place, o + jnp.where(o < place, 0, 1)))

    def bias_rows(r):
        return bx.at[pl.ds(64 * core + 8 * r, 8)]

    take(bx.at[pl.ds(0, 4)], plane.at[0])
    rest = bx.at[pl.ds(64 * core + 8 * row + 4 - 4 * z_lo, 4)]
    own_row, other_row = bias_rows(row), bias_rows(2 * y_at + 1 - z_hi)
    push(own_row, own_row, far_send, far.at[0], row, mate)
    for k in (1, 3, 2):
        push(rest, rest, near_send, near.at[k], 2 * lax.rem(y_at + k, 4) + z_hi, col)

    take(bx.at[pl.ds(0, 8)], plane.at[1])
    push(other_row, other_row, far_send, far.at[1], row, mate)
    for k in (1, 3, 2):
        push(other_row, other_row, near_send, near.at[4 + k], 2 * lax.rem(y_at + k, 4) + z_hi, col)

    take(nx.at[pl.ds(0, 15)], norm_recv)

    for q in range(4):
        at = slice(4 * q, 4 * q + 4)
        nb = nx[at].reshape(512, 128)
        qk = dot(nb, att_in_ref[:, :256])
        qs[at] = (qk[:, :128] * 32 ** (-0.5)).astype(BF16).reshape(4, 128, 128)
        ks[at] = qk[:, 128:].astype(BF16).reshape(4, 128, 128)
    for q in range(4):
        z = jax.nn.sigmoid(dot(wgt[...], nx[4 * q : 4 * q + 4].reshape(512, 128), NT))
        for k in range(4):
            gt[4 * q + k] = z[:, 128 * k : 128 * k + 128]
    for b in range(4):
        vt[b, :128] = dot(wvt[...], nx[:, 32 * b : 32 * b + 32, :].reshape(512, 128), NT).astype(BF16)
        vt[b, 128:] = jnp.ones((16, 512), BF16)

    tile[...] = jnp.zeros((2, 128, 128), F32)

    def block(o):
        r = rows_of(o)[0]

        @pl.when((o > 0) & (o < 7))
        def _():
            later, back, own_half = rows_of(o + 1)
            rows = bias_rows(later)

            @pl.when(own_half)
            def _():
                take(bx.at[pl.ds(0, 4)], early.at[back])
                take(bx.at[pl.ds(0, 4)], near.at[back])

            @pl.when(jnp.logical_not(own_half))
            def _():
                take(bx.at[pl.ds(0, 8)], near.at[4 + back])

            push(rows, rows, far_send, far.at[o + 1], row, mate)

        take(bx.at[pl.ds(0, 8)], far.at[o])
        for k in range(2):
            got = bx[pl.ds(pl.multiple_of(64 * k + 8 * r, 8), 8)].astype(F32)
            bias[:, k] = got * LOG2E

        def score(b):
            q = qs[pl.ds(2 * r, 2), 32 * b : 32 * b + 32, :].reshape(4, 1, 16, 128)
            hd = lax.broadcasted_iota(jnp.int32, (4, 4, 16, 128), 1)
            ln = lax.broadcasted_iota(jnp.int32, (4, 4, 16, 128), 3)
            qm = jnp.where(
                hd == ln // 32, jnp.broadcast_to(q, (4, 4, 16, 128)).astype(F32), 0.0
            ).astype(BF16)
            keys = ks[:, 32 * b : 32 * b + 32, :].reshape(512, 128)
            st = dot(keys, qm.reshape(256, 128), NT) * LOG2E + bias[...].reshape(512, 256)
            scores[b] = st
            return jnp.max(st, axis=0, keepdims=True)

        top = score(0)
        for b in range(4):
            later_top = score(b + 1) if b < 3 else None
            ot = dot(vt[b], jnp.exp2(scores[b] - top).astype(BF16))
            ot = ot[:128] * (1.0 / ot[128:129])
            for h in range(4):
                part = ot[32 * h : 32 * h + 32]
                for j in range(4):
                    at = 64 * (j % 2) + 16 * h
                    to = 32 * b + 16 * (j % 2)
                    moved = part[:, 128 * (j // 2) : 128 * (j // 2) + 128]
                    if (to - at) % 128:
                        moved = pltpu.roll(moved, (to - at) % 128, 1)
                    here = (lane128 >= to) & (lane128 < to + 16)
                    rows = slice(32 * h, 32 * h + 32)
                    tile[j // 2, rows] = jnp.where(here, moved, tile[j // 2, rows])
            top = later_top
        for k in range(2):
            c = 2 * r + k
            go[c] = (tile[k] * gt[c]).astype(BF16)
        for k in range(2):
            c = 2 * r + k

            @pl.when(c != col)
            def _():
                push(go.at[c], gx.at[col], back_send, back_recv, row, c)

    loop(0, 8, block)
    gx[col] = go[col]
    take(gx.at[pl.ds(0, 15)], back_recv)

    for g in range(4):
        for s in range(4 * g, 4 * g + 4):
            t = update[s] + dot(gx[s], att_out_ref[...], TN)
            for b in range(4):
                out[b, s] = t[32 * b : 32 * b + 32]
    take(rx.at[0, pl.ds(0, 127)], right_send)
    take(rx.at[0, pl.ds(0, 127)], left_send)
    take(px.at[pl.ds(0, 127)], prod_send)
    take(nx.at[pl.ds(0, 15)], norm_send)
    take(bx.at[pl.ds(0, 3)], line_send)
    take(bx.at[pl.ds(0, 12)], plane_send)
    take(bx.at[pl.ds(0, 12)], early_send)
    take(bx.at[pl.ds(0, 36)], near_send)
    take(bx.at[pl.ds(0, 64)], far_send)
    take(go.at[pl.ds(0, 15)], back_send)


SCRATCH = [
    ((64, 32, 128), F32),
    ((128, 512), BF16),
    ((128, 128), BF16),
    ((128, 128), BF16),
    ((4, 128), BF16),
    ((128, 512), BF16),
    ((128, 128), BF16),
    ((16, 128, 128), BF16),
    ((16, 128, 128), F32),
    ((512, 128), BF16),
    ((128, 128), BF16),
    ((128, 128), BF16),
    ((4, 256, 256), BF16),
    ((2, 128, 16, 128), BF16),
    ((2, 128, 16, 128), BF16),
    ((16, 128, 128), BF16),
    ((64, 512), BF16),
    ((512, 512), BF16),
    ((128, 16, 128), BF16),
    ((128, 16, 128), BF16),
    ((16, 128, 128), F32),
    ((16, 128, 128), BF16),
    ((2, 16, 128), F32),
    ((64, 128), F32),
    ((16, 128, 128), BF16),
    ((16, 128, 128), BF16),
    ((32, 256), BF16),
    ((128, 32, 256), BF16),
    ((16, 128, 128), BF16),
    ((16, 128, 128), BF16),
    ((4, 144, 512), BF16),
    ((16, 128, 128), F32),
    ((8, 2, 32, 256), F32),
    ((4, 512, 256), F32),
    ((2, 128, 128), F32),
    ((16, 128, 128), BF16),
]
SEMAPHORES = [
    (7,), (), (), (), (8,), (), (8,), (), (), (), (), (), (2,), (), (4,), (), (8,), (), (8,), (), (),
]


def per_device(pair, valid_length, tri_in, tri_gate, tri_out, att_in, att_bias, att_out):
    vmem = pl.BlockSpec(memory_space=pltpu.VMEM)
    smem = pl.BlockSpec(memory_space=pltpu.SMEM)
    hbm = pl.BlockSpec(memory_space=pltpu.HBM)
    change = pl.pallas_call(
        kernel,
        out_shape=jax.ShapeDtypeStruct((4, 16, 32, 128), F32),
        in_specs=[hbm, smem] + [hbm] * 6,
        out_specs=vmem,
        scratch_shapes=[pltpu.VMEM(*s) for s in SCRATCH]
        + [pltpu.SemaphoreType.DMA(s) for s in SEMAPHORES],
        compiler_params=pltpu.CompilerParams(
            collective_id=0, has_side_effects=True, vmem_limit_bytes=40 * 1024 * 1024
        ),
    )(*[a if n == 1 else pltpu.with_memory_space_constraint(a, pltpu.HBM) for n, a in enumerate((pair, valid_length, tri_in, tri_gate, tri_out, att_bias.T, att_in, att_out))])
    return pair + change.reshape(64, 32, 128)


def solution(mesh):
    placed = (P("row", "col", None), P(), P(), P(), P(), P(), P(), P())
    return jax.shard_map(
        per_device, mesh=mesh, in_specs=placed, out_specs=P("row", "col", None), check_vma=False
    )
```
